256 devices in a mesh: section: 2 (over core), tile: 128 (over y, z, x).
Axes of the slice: x: 4, y: 4, z: 8, core: 2. Of those that a mesh axis runs over, the one named last changes fastest.
Arguments:
- object_slices: float32 [2, 4096, 2, 16, 128], P('section', 'tile'), may hold values from -4 to 4
- probe_wave: float32 [2, 256, 256], replicated, may hold values from -4 to 4
- intensities: float32 [256, 256, 256], P('tile'), may hold values from 0 to 2
- send_list: int32 [128, 2, 128, 2], P('tile'), may hold values from -1 to 31, as said below
- cell_slot: int32 [256, 32], P('tile'), may hold values from 0 to 255, as said below
Outputs:
- object_gradient: float32 [2, 4096, 2, 16, 128], P('section', 'tile')
The draws below stay inside these ranges and needn't reach their ends.
Inputs may be any that keep to these rules, and one draw needn't show every extreme that they name: `cell_slot`: the cells of one device's batch name distinct slots; the slots named by a batch are exactly the entries of send_list for that device and batch that are not -1. `send_list`: entry [o, m, d, c] is a patch index of owner o exactly when slot o * 2 + c is named by a cell of device d in batch m, and -1 otherwise. In every batch of every device, some owner has all 2 of its places used.
All inputs are finite; a program needn't handle non-finite values.
Results may differ from the reference program's by a relative error of at most 0.0003.
Values sent between devices are 32-bit elements; how exact they have to be, the bound alone decides.
A program may use at most 64 MiB of HBM per device.

```python
import jax
import jax.numpy as jnp
from jax import lax

W = 256
PW = 128
PR = 16
MB = 2
POS_MB = 1
CELLS = 32
CAP = 2
BLK_DEV = 32
BLOCKS = 4096
POSITIONS = 256
N_SECTION = 2
N_TILE = 128


def request_plan(key):
    slots_all = N_TILE * CAP
    wanted = POS_MB * CELLS
    batch_total = N_TILE * MB

    def one_batch(batch_key):
        branch_keys = jax.random.split(batch_key, 4)
        shuffled = jax.random.permutation(branch_keys[0], slots_all)
        chosen_owner = jax.random.randint(branch_keys[1], (), 0, N_TILE)
        slot_ids = jnp.arange(slots_all, dtype=jnp.int32)
        priority = jnp.where(slot_ids // CAP == chosen_owner, -1, shuffled)
        picked = jnp.argsort(priority, stable=True)[:wanted].astype(jnp.int32)
        picked = jax.random.permutation(branch_keys[2], picked)
        local_ids = jax.random.randint(branch_keys[3], (wanted,), 0, BLK_DEV)
        owner_table = jnp.full((slots_all,), -1, jnp.int32).at[picked].set(local_ids)
        return (picked, owner_table)
    picked_all, tables = jax.vmap(one_batch)(jax.random.split(key, batch_total))
    cell_table = picked_all.reshape(POSITIONS, CELLS).astype(jnp.int32)
    send_table = jnp.transpose(tables.reshape(N_TILE, MB, N_TILE, CAP), (2, 1, 0, 3)).astype(jnp.int32)
    return (send_table, cell_table)


def draw_send_list(key, part):
    return request_plan(jax.random.fold_in(key, 11))[0]


def draw_cell_slot(key, part):
    return request_plan(jax.random.fold_in(key, 11))[1]


def shard_levels(own_key, shape, cuts, low, largest):
    gain = 1.0
    for position, blocks in cuts:
        heights = jax.random.uniform(jax.random.fold_in(jax.random.fold_in(own_key, 6), position), (blocks,), jnp.float32, low / len(cuts), largest / len(cuts))
        gain = gain * jnp.repeat(jnp.exp(heights), shape[position] // blocks).reshape((-1,) + (1,) * (len(shape) - 1 - position))
    return gain


def centred(rng, dims, scale, reach, pieces=(), kind=jnp.bfloat16):
    entries = jax.random.normal(rng, dims, jnp.float32) * scale
    if len(pieces) > 0:
        entries = shard_levels(rng, dims, pieces, -0.22, 0.18) * entries
    return jnp.clip(entries, min=-reach, max=reach).astype(kind)


def setup_inputs(seed: int = 0) -> dict:
    keys = jax.random.split(jax.random.key(seed), 6)
    return {
        "object_slices": centred(keys[0], (N_SECTION, BLOCKS, 2, PR, PW), 0.7, 4.0, ((0, 2), (1, 128)), jnp.float32),
        "probe_wave": centred(keys[1], (2, W, W), 0.7, 4.0, (), jnp.float32),
        "intensities": jnp.clip(2.0 * jax.random.uniform(keys[2], (POSITIONS, W, W), jnp.float32) ** shard_levels(keys[2], (POSITIONS, W, W), ((0, 128),), -0.2, 0.2), 0.0, 2.0),
        "send_list": draw_send_list(jax.random.fold_in(keys[5], 71), 0),
        "cell_slot": draw_cell_slot(jax.random.fold_in(keys[5], 71), 0),
    }


PHASE_SCALE = 20.0


def stitch(cell_patches):
    row_count = cell_patches.shape[0]
    arranged = cell_patches.reshape(row_count, W // PR, W // PW, 2, PR, PW)
    return jnp.transpose(arranged, (3, 0, 1, 4, 2, 5)).reshape(2, row_count, W, W)


def unstitch(wavefield):
    row_count = wavefield.shape[1]
    arranged = wavefield.reshape(2, row_count, W // PR, PR, W // PW, PW)
    return jnp.transpose(arranged, (1, 2, 4, 0, 3, 5)).reshape(row_count, CELLS, 2, PR, PW)


def filter_phase():
    indices = jnp.arange(W, dtype=jnp.int32)
    frequency = jnp.where(indices < W // 2, indices, indices - W)
    squared = frequency[:, None] * frequency[:, None] + frequency[None, :] * frequency[None, :]
    return PHASE_SCALE * squared.astype(jnp.float32) / (W * W)


def forward(wavefield):
    return jnp.fft.fft2(wavefield, norm="ortho")


def inverse(wavefield):
    return jnp.fft.ifft2(wavefield, norm="ortho")


def reference(object_slices, probe_wave, intensities, send_list, cell_slot):
    phases = filter_phase()
    transfer = jnp.cos(phases) - 1j * jnp.sin(phases)
    incident = probe_wave[0] + 1j * probe_wave[1]
    row_count = MB * POS_MB

    def per_device(gradient_sum, device):
        first_row = device * row_count
        slot_ids = lax.dynamic_slice_in_dim(cell_slot, first_row, row_count, 0)
        measured = lax.dynamic_slice_in_dim(intensities, first_row, row_count, 0)
        batch_ids = (jnp.arange(row_count, dtype=jnp.int32) // POS_MB)[:, None]
        owners = slot_ids // CAP
        local_ids = send_list[owners, batch_ids, device, slot_ids % CAP]
        block_ids = owners * BLK_DEV + local_ids

        def window(slice_index):
            wavefield = stitch(object_slices[slice_index][block_ids])
            return wavefield[0] + 1j * wavefield[1]

        first_slice = window(0)
        second_slice = window(1)
        entering = incident[None] * first_slice
        propagated = inverse(transfer[None] * forward(entering))
        far_field = forward(propagated * second_slice)
        misfit = (jnp.real(far_field) ** 2 + jnp.imag(far_field) ** 2 - measured) * far_field
        back_far = inverse(misfit)
        grad_second = jnp.conj(propagated) * back_far
        back_slice = jnp.conj(second_slice) * back_far
        back_first = inverse(jnp.conj(transfer)[None] * forward(back_slice))
        grad_first = jnp.conj(incident)[None] * back_first

        def as_cells(wavefield):
            return unstitch(jnp.stack([jnp.real(wavefield), jnp.imag(wavefield)]))

        gradient_sum = gradient_sum.at[0, block_ids].add(as_cells(grad_first))
        gradient_sum = gradient_sum.at[1, block_ids].add(as_cells(grad_second))
        return gradient_sum, None

    start_sum = jnp.zeros((N_SECTION, BLOCKS, 2, PR, PW), jnp.float32)
    gradient_sum, unused = lax.scan(per_device, start_sum, jnp.arange(N_TILE, dtype=jnp.int32))
    return gradient_sum
```

```python
import functools

import jax
import jax.numpy as jnp
import ml_dtypes
import numpy as np
from jax import lax
from jax.experimental import pallas as pl
from jax.experimental.pallas import tpu as pltpu
from jax.sharding import PartitionSpec as P

W = 256
PW = 128
PR = 16
MB = 2
CELLS = 32
NX, NY, NZ = 4, 4, 8
PLANE = NX * NY
OWN = 32
COLUMN = NZ * OWN
PLACES = 14
ROWS = PLANE * PLACES
CHUNKS = 4
PHASE_SCALE = 20.0
MESH = pl.DeviceIdType.MESH
F32 = jnp.float32
I32 = jnp.int32
BF16 = jnp.bfloat16


def stacked_parts(matrix):
    rows = np.concatenate([matrix.real, matrix.imag], axis=0).astype(np.float32)
    high = rows.astype(ml_dtypes.bfloat16)
    low = (rows - high.astype(np.float32)).astype(ml_dtypes.bfloat16)
    return np.concatenate([high, high, low], axis=1)


def matrix_tables():
    index = np.arange(W)
    product = np.outer(index, index) % W
    dft = np.exp(-2j * np.pi * product / W) / np.sqrt(W)
    frequency = np.where(index < W // 2, index, index - W).astype(np.float64)
    diagonal = np.exp(-1j * PHASE_SCALE * frequency**2 / (W * W))
    move = np.conj(dft) @ (diagonal[:, None] * dft)
    move = (move + move.T) / 2
    return stacked_parts(dft), stacked_parts(move)


def place():
    tile = lax.axis_index("tile")
    core = lax.axis_index("section")
    y = tile // (NZ * NX)
    z = (tile // NX) % NZ
    x = tile % NX
    return core, y, z, x


def plane_tile(q, z):
    return (q // NX) * (NZ * NX) + z * NX + q % NX


def iota(shape, axis):
    return lax.broadcasted_iota(I32, shape, axis)


def to_column(row):
    n = row.shape[1]
    wide = jnp.broadcast_to(row, (n, n))
    return jnp.sum(jnp.where(iota((n, n), 0) == iota((n, n), 1), wide, 0.0), axis=1, keepdims=True)


def quotient(values, divisor, count):
    total = jnp.zeros(values.shape, I32)
    for step in range(1, count):
        total = total + jnp.where(values >= divisor * step, 1, 0)
    return total


def hops(chunk, direction):
    return 4 if (chunk % 2 == 0) == (direction > 0) else 3


def gather_kernel(
    obj,
    meta,
    cells,
    win,
    tab,
    flag,
    ag,
    metas,
    metain,
    tables,
    pick,
    slot,
    pack,
    recv,
    mark,
    marks,
    other,
    ag_send,
    ag_recv,
    meta_send,
    meta_recv,
    mark_send,
    mark_recv,
    xy_send,
    xy_recv,
    pair_send,
    pair_recv,
    local_sem,
):
    core, y, z, x = place()
    mine = y * NX + x
    barrier = pltpu.get_barrier_semaphore()

    def ring_device(zz):
        return (core, y * (NZ * NX) + zz * NX + x)

    def plane_device(q):
        return (core, plane_tile(q, z))

    def greet_ring(step, carry):
        pl.semaphore_signal(
            barrier, inc=1, device_id=ring_device((z + step) % NZ), device_id_type=MESH
        )
        return carry

    def greet_plane(step, carry):
        pl.semaphore_signal(
            barrier, inc=1, device_id=plane_device((mine + step) % PLANE), device_id_type=MESH
        )
        return carry

    partner = (1 - core, y * (NZ * NX) + z * NX + x)
    lax.fori_loop(1, NZ, greet_ring, 0)
    lax.fori_loop(1, PLANE, greet_plane, 0)
    pl.semaphore_signal(barrier, inc=1, device_id=partner, device_id_type=MESH)
    pl.semaphore_wait(barrier, NZ + PLANE - 1)

    def ring_copy(chunk, direction, hop):
        block = (z - direction * (hop - 1) + 2 * NZ) % NZ
        place_of = ag[chunk].at[pl.ds(block * OWN, OWN)]
        side = 0 if direction > 0 else 1
        return pltpu.make_async_remote_copy(
            src_ref=obj.at[:, chunk] if hop == 1 else place_of,
            dst_ref=place_of,
            send_sem=ag_send.at[chunk, side, hop - 1],
            recv_sem=ag_recv.at[chunk, side, hop - 1],
            device_id=ring_device((z + direction + NZ) % NZ),
            device_id_type=MESH,
        )

    def ring_arrival(chunk, direction, hop):
        block = (z - direction * hop + 2 * NZ) % NZ
        place_of = ag[chunk].at[pl.ds(block * OWN, OWN)]
        side = 0 if direction > 0 else 1
        pltpu.make_async_remote_copy(
            src_ref=place_of,
            dst_ref=place_of,
            send_sem=ag_send.at[chunk, side, hop - 1],
            recv_sem=ag_recv.at[chunk, side, hop - 1],
            device_id=ring_device((z + direction + NZ) % NZ),
            device_id_type=MESH,
        ).wait_recv()

    def start_ring(first):
        for chunk in (first, first + 1):
            for direction in (1, -1):
                ring_copy(chunk, direction, 1).start()

    def forward_ring(first, hop):
        for chunk in (first, first + 1):
            for direction in (1, -1):
                ring_arrival(chunk, direction, hop - 1)
                if hop <= hops(chunk, direction):
                    ring_copy(chunk, direction, hop).start()

    start_ring(0)

    row = cells[...]
    owner = row >> 1
    from_q = (owner >> 5) * NX + (owner & 3)
    entry = ((owner >> 2) & 7) * 4 + (iota(row.shape, 1) >> 5) * 2 + (row & 1)
    code_row = (from_q * 32 + entry).astype(F32)
    q_row = from_q.astype(F32)
    code_col = to_column(code_row)
    q_col = to_column(q_row)
    ahead = (q_col == q_row) & (code_col < code_row)
    rank = jnp.sum(jnp.where(ahead, 1.0, 0.0), axis=0, keepdims=True)
    over = jnp.where(jnp.max(rank, axis=1, keepdims=True) >= PLACES, 1, 0)
    at = q_row * PLACES + jnp.minimum(rank, PLACES - 1.0)
    tables[...] = jnp.zeros(tables.shape, I32)
    tables[0:1, 0 : MB * CELLS] = at.astype(I32)
    at_col = to_column(jnp.where(rank < PLACES, at, -1.0))
    spread = jnp.broadcast_to(at_col, (MB * CELLS, 256)) == iota((MB * CELLS, 256), 1).astype(F32)
    number = iota((MB * CELLS, 256), 0).astype(F32)
    back_row = jnp.sum(jnp.where(spread, number, 0.0), axis=0, keepdims=True)

    lane = iota((8, 128), 1)
    for zz in range(NZ):
        metas[zz] = jnp.where(lane == 64, jnp.broadcast_to(over, (8, 128)), meta[zz])
    metain[z] = metas[z]

    def meta_copy(step):
        there = (z + step) % NZ
        return pltpu.make_async_remote_copy(
            src_ref=metas.at[there],
            dst_ref=metain.at[z],
            send_sem=meta_send.at[step],
            recv_sem=meta_recv.at[step],
            device_id=ring_device(there),
            device_id_type=MESH,
        )

    for step in range(1, NZ):
        meta_copy(step).start()

    slots = pltpu.make_async_copy(tables, slot, local_sem.at[0])
    slots.start()

    for chunk in range(CHUNKS):
        ag[chunk][pl.ds(z * OWN, OWN)] = obj[:, chunk]

    forward_ring(0, 2)
    forward_ring(0, 3)
    start_ring(2)

    for step in range(1, NZ):
        meta_copy(step).wait()
    wanted = metain[:, 0, :].astype(F32)
    lanes = iota((NZ, 128), 1)
    column_over = jnp.max(
        jnp.max(jnp.where(lanes == 64, wanted, 0.0), axis=1, keepdims=True), axis=0, keepdims=True
    )
    mark[...] = jnp.broadcast_to(column_over, (8, 128)).astype(I32)
    marks[mine] = mark[...]

    def mark_copy(step):
        return pltpu.make_async_remote_copy(
            src_ref=mark,
            dst_ref=marks.at[mine],
            send_sem=mark_send.at[step],
            recv_sem=mark_recv.at[step],
            device_id=plane_device((mine + step) % PLANE),
            device_id_type=MESH,
        )

    valid = (wanted >= 0.0) & (lanes < 64)
    held = jnp.where(valid, 1.0, 0.0)
    big_row, big_lane = iota((128, 128), 0), iota((128, 128), 1)
    group = jnp.where((big_row >> 2) == (big_lane >> 2), 1.0, 0.0)
    before = jnp.where(((big_row >> 2) == (big_lane >> 2)) & (big_row < big_lane), 1.0, 0.0)
    in_group = jnp.dot(held, group, preferred_element_type=F32)
    order = jnp.dot(held, before, preferred_element_type=F32)
    rows = []
    running = jnp.zeros((1, 128), F32)
    for zz in range(NZ):
        rows.append(order[zz : zz + 1] + running)
        running = running + in_group[zz : zz + 1]
    order = jnp.concatenate(rows, axis=0)
    named = iota((NZ, 128), 0).astype(F32) * OWN + wanted + 1.0
    picks = [
        jnp.sum(jnp.where(valid & (order == float(k)), named, 0.0), axis=0, keepdims=True)
        for k in range(PLACES)
    ]
    picks.append(jnp.zeros((16 - PLACES, 128), F32))
    picks = jnp.dot(jnp.concatenate(picks, axis=0), group, preferred_element_type=F32)
    metas[0] = picks[0:8].astype(I32)
    metas[1] = picks[8:16].astype(I32)
    for half in range(2):
        pltpu.make_async_copy(metas.at[half], pick.at[half], local_sem.at[1 + half]).start()
    target = iota((1, 256), 1)
    target_q = quotient(target, PLACES, PLANE)
    target_k = target - target_q * PLACES
    chosen = jnp.where(
        iota((128, 256), 0) == jnp.broadcast_to(target_q * 4, (128, 256)), 1.0, 0.0
    )
    chosen = jnp.dot(picks, chosen, preferred_element_type=F32)
    here = (iota((16, 256), 0) == jnp.broadcast_to(target_k, (16, 256))) & (
        iota((16, 256), 1) < ROWS
    )
    sums_row = jnp.sum(jnp.where(here, chosen, 0.0), axis=0, keepdims=True)
    tab[...] = jnp.zeros(tab.shape, I32)
    tab[0:1, :] = back_row.astype(I32)
    tab[1:2, :] = sums_row.astype(I32)
    slots.wait()
    for half in range(2):
        pltpu.make_async_copy(metas.at[half], pick.at[half], local_sem.at[1 + half]).wait()
    for step in range(1, PLANE):
        mark_copy(step).start()

    forward_ring(0, 4)
    ring_arrival(0, 1, 4)
    ring_arrival(1, -1, 4)

    def plane_copy(chunk, step):
        q = (mine + step) % PLANE
        return pltpu.make_async_remote_copy(
            src_ref=pack.at[chunk, pl.ds(q * PLACES, PLACES)],
            dst_ref=recv[chunk].at[pl.ds(mine * PLACES, PLACES)],
            send_sem=xy_send.at[chunk, step],
            recv_sem=xy_recv.at[chunk, step],
            device_id=plane_device(q),
            device_id_type=MESH,
        )

    def send_plane(chunk):
        def fill(q, carry):
            for k in range(PLACES):
                index = jnp.clip(pick[k // 8, k % 8, q * 4], 1, COLUMN) - 1
                pack[chunk, q * PLACES + k] = ag[chunk][index]
            return carry

        lax.fori_loop(0, PLANE, fill, 0)

        def send(step, carry):
            plane_copy(chunk, step).start()
            return carry

        lax.fori_loop(1, PLANE, send, 0)
        recv[chunk][pl.ds(mine * PLACES, PLACES)] = pack[chunk, pl.ds(mine * PLACES, PLACES)]

    def pair_copy(part):
        return pltpu.make_async_remote_copy(
            src_ref=other.at[part],
            dst_ref=win.at[core, part],
            send_sem=pair_send.at[part],
            recv_sem=pair_recv.at[part],
            device_id=partner,
            device_id_type=MESH,
        )

    def take_plane(chunk):
        def arrive(step, carry):
            plane_copy(chunk, step).wait_recv()
            return carry

        lax.fori_loop(1, PLANE, arrive, 0)
        part, half = chunk // 2, chunk % 2

        def lay(r, carry):
            start = pl.multiple_of(r * PR + half * 8, 8)
            for column in range(2):
                k = r * 2 + column
                lanes_of = slice(column * PW, column * PW + PW)
                keep = jnp.clip(slot[0, core * CELLS + k], 0, ROWS - 1)
                give = jnp.clip(slot[0, (1 - core) * CELLS + k], 0, ROWS - 1)
                win[core, part, pl.ds(start, 8), lanes_of] = recv[chunk][keep]
                other[part, pl.ds(start, 8), lanes_of] = recv[chunk][give]
            return carry

        lax.fori_loop(0, W // PR, lay, 0)

    send_plane(0)
    send_plane(1)
    forward_ring(2, 2)
    forward_ring(2, 3)
    forward_ring(2, 4)
    ring_arrival(2, 1, 4)
    send_plane(2)
    ring_arrival(3, -1, 4)
    send_plane(3)
    take_plane(0)
    take_plane(1)
    pair_copy(0).start()
    for step in range(1, PLANE):
        mark_copy(step).wait()
    flag[...] = jnp.max(marks[...].astype(F32), axis=0).astype(I32)
    take_plane(2)
    take_plane(3)
    pair_copy(1).start()
    for chunk in range(CHUNKS):
        for direction in (1, -1):
            for hop in range(1, hops(chunk, direction) + 1):
                ring_copy(chunk, direction, hop).wait_send()

    def drain(step, carry):
        for chunk in range(CHUNKS):
            plane_copy(chunk, step).wait_send()
        return carry

    lax.fori_loop(1, PLANE, drain, 0)
    pair_copy(0).wait()
    pair_copy(1).wait()


def fetch_windows(owned, wanted, cells):
    vmem = pl.BlockSpec(memory_space=pltpu.VMEM)
    tile = (8, 128)
    return pl.pallas_call(
        gather_kernel,
        out_shape=(
            jax.ShapeDtypeStruct((2, 2, W, W), F32),
            jax.ShapeDtypeStruct((8, 256), I32),
            jax.ShapeDtypeStruct(tile, I32),
        ),
        in_specs=[vmem] * 3,
        out_specs=(vmem, vmem, vmem),
        scratch_shapes=[
            [pltpu.VMEM((COLUMN,) + tile, F32)] * CHUNKS,
            pltpu.VMEM((NZ,) + tile, I32),
            pltpu.VMEM((NZ,) + tile, I32),
            pltpu.VMEM(tile, I32),
            pltpu.SMEM((2,) + tile, I32),
            pltpu.SMEM(tile, I32),
            pltpu.VMEM((CHUNKS, ROWS) + tile, F32),
            [pltpu.VMEM((ROWS,) + tile, F32)] * CHUNKS,
            pltpu.VMEM(tile, I32),
            pltpu.VMEM((PLANE,) + tile, I32),
            pltpu.VMEM((2, W, W), F32),
            pltpu.SemaphoreType.DMA((CHUNKS, 2, 4)),
            pltpu.SemaphoreType.DMA((CHUNKS, 2, 4)),
            pltpu.SemaphoreType.DMA((NZ,)),
            pltpu.SemaphoreType.DMA((NZ,)),
            pltpu.SemaphoreType.DMA((PLANE,)),
            pltpu.SemaphoreType.DMA((PLANE,)),
            pltpu.SemaphoreType.DMA((CHUNKS, PLANE)),
            pltpu.SemaphoreType.DMA((CHUNKS, PLANE)),
            pltpu.SemaphoreType.DMA((2,)),
            pltpu.SemaphoreType.DMA((2,)),
            pltpu.SemaphoreType.DMA((3,)),
        ],
        compiler_params=pltpu.CompilerParams(collective_id=0, has_side_effects=True),
        name="fetch_windows",
    )(owned, wanted, cells)


def parts(value):
    high = value.astype(BF16)
    return high, (value - high.astype(F32)).astype(BF16)


def from_left(real, imag, table, sign):
    high, low = parts(jnp.concatenate([real, imag], axis=1))
    out = jnp.dot(
        table[...], jnp.concatenate([high, low, high], axis=0), preferred_element_type=F32
    )
    return out[:W, :W] - sign * out[W:, W:], out[:W, W:] + sign * out[W:, :W]


def from_right(real, imag, table, sign):
    high, low = parts(jnp.concatenate([real, imag], axis=0))
    out = lax.dot_general(
        jnp.concatenate([high, low, high], axis=1),
        table[...],
        (((1,), (1,)), ((), ())),
        preferred_element_type=F32,
    )
    return out[:W, :W] - sign * out[W:, W:], sign * out[:W, W:] + out[W:, :W]


def both_sides(real, imag, table, sign):
    real, imag = from_left(real, imag, table, sign)
    return from_right(real, imag, table, sign)


def position_kernel(win, probe, measured, dft, move, grad):
    core = lax.axis_index("section")

    def lay(index, real, imag):
        for k in range(CELLS):
            rows = slice(k // 2 * PR, k // 2 * PR + PR)
            lanes = slice(k % 2 * PW, k % 2 * PW + PW)
            grad[index, k, 0] = real[rows, lanes]
            grad[index, k, 1] = imag[rows, lanes]

    pr, pi = probe[0], probe[1]
    ar, ai = win[0, 0], win[0, 1]
    wave_r, wave_i = both_sides(pr * ar - pi * ai, pr * ai + pi * ar, move, 1.0)
    br, bi = win[1, 0], win[1, 1]
    far_r, far_i = both_sides(
        wave_r * br - wave_i * bi, wave_r * bi + wave_i * br, dft, 1.0
    )
    gap = far_r * far_r + far_i * far_i - measured[core]
    back_r, back_i = both_sides(gap * far_r, gap * far_i, dft, -1.0)
    lay(1, wave_r * back_r + wave_i * back_i, wave_r * back_i - wave_i * back_r)
    br, bi = win[1, 0], win[1, 1]
    low_r, low_i = both_sides(
        br * back_r + bi * back_i, br * back_i - bi * back_r, move, -1.0
    )
    pr, pi = probe[0], probe[1]
    lay(0, pr * low_r + pi * low_i, pr * low_i - pi * low_r)


def position_gradients(windows, probe_wave, intensities, dft, move):
    vmem = pl.BlockSpec(memory_space=pltpu.VMEM)
    return pl.pallas_call(
        position_kernel,
        out_shape=jax.ShapeDtypeStruct((2, CELLS, 2, PR, PW), F32),
        in_specs=[vmem] * 5,
        out_specs=vmem,
        name="position_gradients",
    )(windows, probe_wave, intensities, dft, move)


def return_kernel(
    grad,
    back,
    tab,
    out,
    cells,
    pack,
    recv,
    total,
    ring,
    mix,
    pair_send,
    pair_recv,
    xy_send,
    xy_recv,
    rs_send,
    rs_recv,
):
    core, y, z, x = place()
    mine = y * NX + x
    barrier = pltpu.get_barrier_semaphore()

    def ring_device(zz):
        return (core, y * (NZ * NX) + zz * NX + x)

    def plane_device(q):
        return (core, plane_tile(q, z))

    def greet_plane(step, carry):
        pl.semaphore_signal(
            barrier, inc=1, device_id=plane_device((mine + step) % PLANE), device_id_type=MESH
        )
        return carry

    partner = (1 - core, y * (NZ * NX) + z * NX + x)
    for direction in (1, -1):
        pl.semaphore_signal(
            barrier,
            inc=1,
            device_id=ring_device((z + direction + NZ) % NZ),
            device_id_type=MESH,
        )
    lax.fori_loop(1, PLANE, greet_plane, 0)
    pl.semaphore_signal(barrier, inc=1, device_id=partner, device_id_type=MESH)
    pl.semaphore_wait(barrier, PLANE + 2)

    def pair_copy(chunk):
        return pltpu.make_async_remote_copy(
            src_ref=grad.at[1 - core, :, chunk],
            dst_ref=cells[chunk].at[pl.ds(core * CELLS, CELLS)],
            send_sem=pair_send.at[chunk],
            recv_sem=pair_recv.at[chunk],
            device_id=partner,
            device_id_type=MESH,
        )

    def pair_arrival(chunk):
        pltpu.make_async_remote_copy(
            src_ref=grad.at[1 - core, :, chunk],
            dst_ref=cells[chunk].at[pl.ds((1 - core) * CELLS, CELLS)],
            send_sem=pair_send.at[chunk],
            recv_sem=pair_recv.at[chunk],
            device_id=partner,
            device_id_type=MESH,
        ).wait_recv()

    for chunk in range(CHUNKS):
        pair_copy(chunk).start()
    for chunk in range(CHUNKS):
        cells[chunk][pl.ds(core * CELLS, CELLS)] = grad[core, :, chunk]
        recv[chunk, ROWS * 8 :] = jnp.zeros(((256 - ROWS) * 8, 128), F32)

    mix[...] = jnp.where(
        jnp.broadcast_to(tab[1:2, :], (COLUMN, 256)) == iota((COLUMN, 256), 0) + 1, 1.0, 0.0
    ).astype(BF16)

    def plane_copy(chunk, step):
        q = (mine + step) % PLANE
        return pltpu.make_async_remote_copy(
            src_ref=pack.at[chunk, pl.ds(q * (PLACES * 8), PLACES * 8)],
            dst_ref=recv.at[chunk, pl.ds(mine * (PLACES * 8), PLACES * 8)],
            send_sem=xy_send.at[chunk, step],
            recv_sem=xy_recv.at[chunk, step],
            device_id=plane_device(q),
            device_id_type=MESH,
        )

    for chunk in range(CHUNKS):
        pair_arrival(chunk)

        def fill(q, carry):
            for k in range(PLACES):
                row = q * PLACES + k
                pack[chunk, pl.ds(pl.multiple_of(row * 8, 8), 8)] = cells[chunk][
                    jnp.clip(back[0, row], 0, MB * CELLS - 1)
                ]
            return carry

        lax.fori_loop(0, PLANE, fill, 0)

        def send(step, carry):
            plane_copy(chunk, step).start()
            return carry

        lax.fori_loop(1, PLANE, send, 0)
        own_rows = pl.ds(mine * (PLACES * 8), PLACES * 8)
        recv[chunk, own_rows] = pack[chunk, own_rows]

    def block(zz):
        return pl.ds(((zz + 2 * NZ) % NZ) * (OWN * 8), OWN * 8)

    def ring_copy(chunk, direction, step):
        side = 0 if direction > 0 else 1
        reach = hops(chunk, direction)
        return pltpu.make_async_remote_copy(
            src_ref=total.at[chunk, block(z + direction * reach)]
            if step == 1
            else ring.at[chunk, side, step - 2],
            dst_ref=ring.at[chunk, side, step - 1],
            send_sem=rs_send.at[chunk, side, step - 1],
            recv_sem=rs_recv.at[chunk, side, step - 1],
            device_id=ring_device((z + direction + NZ) % NZ),
            device_id_type=MESH,
        )

    def sum_cells(chunk):
        def arrive(step, carry):
            plane_copy(chunk, step).wait_recv()
            return carry

        lax.fori_loop(1, PLANE, arrive, 0)

        def add(r, carry):
            high, low = parts(recv[chunk, pl.ds(r, 256, stride=8), :])
            both = jnp.dot(
                mix[...], jnp.concatenate([high, low], axis=1), preferred_element_type=F32
            )
            total[chunk, pl.ds(r, COLUMN, stride=8), :] = both[:, :128] + both[:, 128:]
            return carry

        lax.fori_loop(0, 8, add, 0)
        for direction in (1, -1):
            ring_copy(chunk, direction, 1).start()

    def pass_on(chunk, step):
        for direction in (1, -1):
            reach = hops(chunk, direction)
            side = 0 if direction > 0 else 1
            if step <= reach:
                ring_copy(chunk, direction, step - 1).wait_recv()
                ring[chunk, side, step - 2] += total[
                    chunk, block(z + direction * (reach - step + 1))
                ]
                ring_copy(chunk, direction, step).start()

    def finish(chunk):
        value = total[chunk, block(z)]
        for direction in (1, -1):
            reach = hops(chunk, direction)
            side = 0 if direction > 0 else 1
            ring_copy(chunk, direction, reach).wait_recv()
            value = value + ring[chunk, side, reach - 1]
        out[:, chunk] = value.reshape(OWN, 8, 128)

    sum_cells(0)
    sum_cells(1)
    pass_on(0, 2)
    pass_on(1, 2)
    sum_cells(2)
    pass_on(0, 3)
    pass_on(1, 3)
    sum_cells(3)
    pass_on(0, 4)
    pass_on(1, 4)
    pass_on(2, 2)
    pass_on(3, 2)
    finish(0)
    finish(1)
    pass_on(2, 3)
    pass_on(3, 3)
    pass_on(2, 4)
    pass_on(3, 4)
    finish(2)
    finish(3)

    for chunk in range(CHUNKS):
        pair_copy(chunk).wait_send()
        for direction in (1, -1):
            for step in range(1, hops(chunk, direction) + 1):
                ring_copy(chunk, direction, step).wait_send()

    def drain(step, carry):
        for chunk in range(CHUNKS):
            plane_copy(chunk, step).wait_send()
        return carry

    lax.fori_loop(1, PLANE, drain, 0)


def return_gradients(gradients, table):
    vmem = pl.BlockSpec(memory_space=pltpu.VMEM)
    smem = pl.BlockSpec(memory_space=pltpu.SMEM)
    tile = (8, 128)
    return pl.pallas_call(
        return_kernel,
        out_shape=jax.ShapeDtypeStruct((OWN, CHUNKS) + tile, F32),
        in_specs=[vmem, smem, vmem],
        out_specs=vmem,
        scratch_shapes=[
            [pltpu.VMEM((MB * CELLS,) + tile, F32)] * CHUNKS,
            pltpu.VMEM((CHUNKS, ROWS * 8, 128), F32),
            pltpu.VMEM((CHUNKS, 256 * 8, 128), F32),
            pltpu.VMEM((CHUNKS, COLUMN * 8, 128), F32),
            pltpu.VMEM((CHUNKS, 2, 4, OWN * 8, 128), F32),
            pltpu.VMEM((COLUMN, 256), BF16),
            pltpu.SemaphoreType.DMA((CHUNKS,)),
            pltpu.SemaphoreType.DMA((CHUNKS,)),
            pltpu.SemaphoreType.DMA((CHUNKS, PLANE)),
            pltpu.SemaphoreType.DMA((CHUNKS, PLANE)),
            pltpu.SemaphoreType.DMA((CHUNKS, 2, 4)),
            pltpu.SemaphoreType.DMA((CHUNKS, 2, 4)),
        ],
        compiler_params=pltpu.CompilerParams(collective_id=1, has_side_effects=True),
        name="return_gradients",
    )(gradients, table[0:1], table)


def swapped(block):
    return lax.ppermute(block, "section", [(0, 1), (1, 0)])


def full_windows(owned, send_plan, cell_slot):
    core = lax.axis_index("section")
    outbound = jnp.swapaxes(send_plan, 0, 1)
    patches = owned[jnp.maximum(outbound, 0)]
    arrived = lax.all_to_all(patches, "tile", split_axis=0, concat_axis=0, tiled=True)
    windows = []
    for batch in range(MB):
        flat = arrived[:, batch].reshape((-1, 2, PR, PW))
        picked = flat[cell_slot[batch]].reshape(W // PR, W // PW, 2, PR, PW)
        windows.append(jnp.transpose(picked, (2, 0, 3, 1, 4)).reshape(2, W, W))
    windows = jnp.stack(windows)
    passed = swapped(lax.dynamic_index_in_dim(windows, 1 - core, 0, keepdims=False))
    kept = lax.dynamic_index_in_dim(windows, core, 0, keepdims=False)
    first = core == 0
    return jnp.stack([jnp.where(first, kept, passed), jnp.where(first, passed, kept)])


def full_sums(gradients, send_plan, cell_slot):
    core = lax.axis_index("section")
    passed = swapped(lax.dynamic_index_in_dim(gradients, 1 - core, 0, keepdims=False))
    kept = lax.dynamic_index_in_dim(gradients, core, 0, keepdims=False)
    first = core == 0
    batches = [jnp.where(first, kept, passed), jnp.where(first, passed, kept)]
    slots = 2 * NX * NY * NZ
    placed = [
        jnp.zeros((slots, 2, PR, PW), F32)
        .at[cell_slot[batch]]
        .set(batches[batch])
        .reshape(slots // 2, 2, 2, PR, PW)
        for batch in range(MB)
    ]
    returned = lax.all_to_all(
        jnp.stack(placed, axis=1), "tile", split_axis=0, concat_axis=0, tiled=True
    )
    outbound = jnp.swapaxes(send_plan, 0, 1)
    target = jnp.where(outbound < 0, OWN, outbound).reshape(-1)
    sums = jax.ops.segment_sum(
        returned.reshape((-1, 2, PR, PW)), target, num_segments=OWN + 1
    )
    return sums[:OWN]


def body(dft, move, object_slices, probe_wave, intensities, send_list, cell_slot):
    owned = object_slices[0]
    send_plan = send_list[0]
    wanted = jnp.transpose(send_plan.reshape(MB, NY, NZ, NX, 2), (2, 1, 3, 0, 4))
    wanted = jnp.pad(wanted.reshape(NZ, 1, 64), ((0, 0), (0, 0), (0, 64)))
    wanted = jnp.broadcast_to(wanted, (NZ, 8, 128))
    windows, table, flag = fetch_windows(
        owned.reshape(OWN, CHUNKS, 8, 128), wanted, cell_slot.reshape(1, MB * CELLS)
    )
    crowded = flag[0, 0] > 0
    windows = lax.cond(
        crowded,
        lambda: full_windows(owned, send_plan, cell_slot),
        lambda: windows,
    )
    gradients = position_gradients(windows, probe_wave, intensities, dft, move)
    sums = lax.cond(
        crowded,
        lambda: full_sums(gradients, send_plan, cell_slot),
        lambda: return_gradients(
            gradients.reshape(2, CELLS, CHUNKS, 8, 128), table
        ).reshape(OWN, 2, PR, PW),
    )
    return sums[None]


def solution(mesh):
    dft, move = matrix_tables()
    in_specs = (
        P("section", "tile", None, None, None),
        P(),
        P("tile", None, None),
        P("tile", None, None, None),
        P("tile", None),
    )
    out_specs = P("section", "tile", None, None, None)
    step = functools.partial(body, jnp.asarray(dft), jnp.asarray(move))
    return jax.shard_map(step, mesh=mesh, in_specs=in_specs, out_specs=out_specs, check_vma=False)
```

```python
import functools

import jax
import jax.numpy as jnp
import ml_dtypes
import numpy as np
from jax import lax
from jax.experimental import pallas as pl
from jax.experimental.pallas import tpu as pltpu
from jax.sharding import PartitionSpec as P

W = 256
PW = 128
PR = 16
MB = 2
CELLS = 32
NX, NY, NZ = 4, 4, 8
PLANE = NX * NY
OWN = 32
COLUMN = NZ * OWN
PLACES = 32
ROWS = 4 * PLACES
CHUNKS = 4
PHASE_SCALE = 20.0
MESH = pl.DeviceIdType.MESH
F32 = jnp.float32
I32 = jnp.int32
BF16 = jnp.bfloat16


def stacked_parts(matrix):
    rows = np.concatenate([matrix.real, matrix.imag], axis=0).astype(np.float32)
    high = rows.astype(ml_dtypes.bfloat16)
    low = (rows - high.astype(np.float32)).astype(ml_dtypes.bfloat16)
    return np.concatenate([high, high, low], axis=1)


def matrix_tables():
    index = np.arange(W)
    product = np.outer(index, index) % W
    dft = np.exp(-2j * np.pi * product / W) / np.sqrt(W)
    frequency = np.where(index < W // 2, index, index - W).astype(np.float64)
    diagonal = np.exp(-1j * PHASE_SCALE * frequency**2 / (W * W))
    move = np.conj(dft) @ (diagonal[:, None] * dft)
    move = (move + move.T) / 2
    return stacked_parts(dft), stacked_parts(move)


def place():
    tile = lax.axis_index("tile")
    core = lax.axis_index("section")
    y = tile // (NZ * NX)
    z = (tile // NX) % NZ
    x = tile % NX
    return core, y, z, x


def device(core, y, z, x):
    return (core, y * (NZ * NX) + z * NX + x)


def iota(shape, axis):
    return lax.broadcasted_iota(I32, shape, axis)


def to_column(row):
    n = row.shape[1]
    wide = jnp.broadcast_to(row, (n, n))
    return jnp.sum(jnp.where(iota((n, n), 0) == iota((n, n), 1), wide, 0.0), axis=1, keepdims=True)


def exclusive(column):
    rows = [jnp.zeros_like(column[0:1])]
    for step in range(column.shape[0] - 1):
        rows.append(rows[-1] + column[step : step + 1])
    return jnp.concatenate(rows, axis=0)


def send_to(src, dst, send_sem, recv_sem, target):
    return pltpu.make_async_remote_copy(
        src_ref=src,
        dst_ref=dst,
        send_sem=send_sem,
        recv_sem=recv_sem,
        device_id=target,
        device_id_type=MESH,
    )


def greet(barrier, targets):
    for target in targets:
        pl.semaphore_signal(barrier, inc=1, device_id=target, device_id_type=MESH)
    pl.semaphore_wait(barrier, len(targets))


def hops(chunk, direction):
    return 4 if (chunk % 2 == 0) == (direction > 0) else 3


def gather_kernel(
    obj,
    meta,
    cells,
    win,
    tab,
    flag,
    ag,
    metas,
    metain,
    tables,
    pick,
    turn,
    slot,
    x_pack,
    x_recv,
    y_pack,
    y_recv,
    mark,
    marks_x,
    marks_y,
    marks_z,
    other,
    ag_send,
    ag_recv,
    meta_send,
    meta_recv,
    mark_send,
    mark_recv,
    x_send,
    x_sem,
    y_send,
    y_sem,
    pair_send,
    pair_recv,
    local_sem,
):
    core, y, z, x = place()
    partner = device(1 - core, y, z, x)

    def ring_device(step):
        return device(core, y, (z + step) % NZ, x)

    def x_device(step):
        return device(core, y, z, (x + step) % NX)

    def y_device(step):
        return device(core, (y + step) % NY, z, x)

    greet(
        pltpu.get_barrier_semaphore(),
        [ring_device(step) for step in range(1, NZ)]
        + [x_device(step) for step in range(1, NX)]
        + [y_device(step) for step in range(1, NY)]
        + [partner],
    )

    def block(chunk, zz):
        return ag[chunk].at[pl.ds(((zz + 2 * NZ) % NZ) * OWN, OWN)]

    def ring_copy(chunk, direction, hop):
        side = 0 if direction > 0 else 1
        held = block(chunk, z - direction * (hop - 1))
        return send_to(
            obj.at[:, chunk] if hop == 1 else held,
            held,
            ag_send.at[chunk, side, hop - 1],
            ag_recv.at[chunk, side, hop - 1],
            ring_device(direction + NZ),
        )

    def ring_arrival(chunk, direction, hop):
        side = 0 if direction > 0 else 1
        held = block(chunk, z - direction * hop)
        send_to(
            held,
            held,
            ag_send.at[chunk, side, hop - 1],
            ag_recv.at[chunk, side, hop - 1],
            ring_device(direction + NZ),
        ).wait_recv()

    def start_ring(first):
        for chunk in (first, first + 1):
            for direction in (1, -1):
                ring_copy(chunk, direction, 1).start()

    def forward_ring(first, hop):
        for chunk in (first, first + 1):
            for direction in (1, -1):
                ring_arrival(chunk, direction, hop - 1)
                if hop <= hops(chunk, direction):
                    ring_copy(chunk, direction, hop).start()

    start_ring(0)

    row = cells[...]
    owner = row >> 1
    entry = ((owner >> 2) & 7) * 4 + (iota(row.shape, 1) >> 5) * 2 + (row & 1)
    code_row = ((owner >> 5) * 128 + (owner & 3) * 32 + entry).astype(F32)
    y_row = (owner >> 5).astype(F32)
    code_col = to_column(code_row)
    y_col = to_column(y_row)
    ahead = (y_col == y_row) & (code_col < code_row)
    rank = jnp.sum(jnp.where(ahead, 1.0, 0.0), axis=0, keepdims=True)
    over = jnp.where(jnp.max(rank, axis=1, keepdims=True) >= PLACES, 1, 0)
    at = y_row * PLACES + jnp.minimum(rank, PLACES - 1.0)
    tables[0] = jnp.zeros((8, 128), I32)
    tables[0, 0:1, 0 : MB * CELLS] = at.astype(I32)
    at_col = to_column(jnp.where(rank < PLACES, at, -1.0))
    spread = jnp.broadcast_to(at_col, (MB * CELLS, ROWS)) == iota((MB * CELLS, ROWS), 1).astype(
        F32
    )
    number = iota((MB * CELLS, ROWS), 0).astype(F32)
    back_row = jnp.sum(jnp.where(spread, number, 0.0), axis=0, keepdims=True)

    lane = iota((8, 128), 1)
    for zz in range(NZ):
        metas[zz] = jnp.where(lane == 64, jnp.broadcast_to(over, (8, 128)), meta[zz])
    metain[z] = metas[z]

    def meta_copy(step):
        return send_to(
            metas.at[(z + step) % NZ],
            metain.at[z],
            meta_send.at[step],
            meta_recv.at[step],
            ring_device(step),
        )

    for step in range(1, NZ):
        meta_copy(step).start()

    def table_copy(index, target):
        return pltpu.make_async_copy(tables.at[index], target, local_sem.at[index])

    table_copy(0, slot).start()

    for chunk in range(CHUNKS):
        ag[chunk][pl.ds(z * OWN, OWN)] = obj[:, chunk]

    forward_ring(0, 2)
    forward_ring(0, 3)
    start_ring(2)

    for step in range(1, NZ):
        meta_copy(step).wait()
    wanted = metain[:, 0, :].astype(F32)
    lanes = iota((NZ, 128), 1)
    valid = (wanted >= 0.0) & (lanes < 64)
    held = jnp.where(valid, 1.0, 0.0)
    big_row, big_lane = iota((128, 128), 0), iota((128, 128), 1)
    one_device = (big_row >> 2) == (big_lane >> 2)
    one_x = ((big_row >> 2) & 3) == ((big_lane >> 2) & 3)
    group = jnp.where(one_device, 1.0, 0.0)
    before = jnp.where(one_device & (big_row < big_lane), 1.0, 0.0)
    column = jnp.where(one_x & (big_row < 64), 1.0, 0.0)
    above = jnp.where(one_x & ((big_row >> 4) < (big_lane >> 4)), 1.0, 0.0)
    in_group = jnp.dot(held, group, preferred_element_type=F32)
    order = jnp.dot(held, before, preferred_element_type=F32) + exclusive(in_group)
    in_all = jnp.sum(held, axis=0, keepdims=True)
    sums = jnp.concatenate([in_all, jnp.zeros((7, 128), F32)], axis=0)
    count = jnp.dot(sums, group, preferred_element_type=F32)[0:1]
    start = jnp.dot(sums, above, preferred_element_type=F32)[0:1]
    whole = jnp.dot(sums, column, preferred_element_type=F32)[0:1]
    order = order + start
    named = iota((NZ, 128), 0).astype(F32) * OWN + wanted + 1.0
    picks = [
        jnp.sum(jnp.where(valid & (order == float(k)), named, 0.0), axis=0, keepdims=True)
        for k in range(PLACES)
    ]
    picks = jnp.dot(jnp.concatenate(picks, axis=0), column, preferred_element_type=F32)
    for part in range(PLACES // 8):
        tables[1 + part] = picks[part * 8 : part * 8 + 8].astype(I32)
        table_copy(1 + part, pick.at[part]).start()
    over_x = jnp.where(jnp.max(whole, axis=1, keepdims=True) > PLACES, 1.0, 0.0)
    over_z = jnp.max(
        jnp.max(jnp.where(lanes == 64, wanted, 0.0), axis=1, keepdims=True), axis=0, keepdims=True
    )
    over = jnp.broadcast_to(jnp.maximum(over_x, over_z), (1, 128))
    mark[0] = jnp.concatenate([count, start, over, jnp.zeros((5, 128), F32)], axis=0).astype(I32)
    marks_x[x] = mark[0]

    def mark_copy(kind, step):
        targets = (x_device, y_device, ring_device)
        arrays = (marks_x, marks_y, marks_z)
        own = (x, y, z)
        return send_to(
            mark.at[kind],
            arrays[kind].at[own[kind]],
            mark_send.at[kind, step],
            mark_recv.at[kind, step],
            targets[kind](step),
        )

    for step in range(1, NX):
        mark_copy(0, step).start()
    target = iota((128, ROWS), 1)
    chosen = jnp.where(iota((128, ROWS), 0) == (target // PLACES) * 4, 1.0, 0.0)
    chosen = jnp.dot(picks, chosen, preferred_element_type=F32)
    here = iota((PLACES, ROWS), 0) == iota((PLACES, ROWS), 1) % PLACES
    sums_row = jnp.sum(jnp.where(here, chosen, 0.0), axis=0, keepdims=True)
    tab[...] = jnp.zeros(tab.shape, I32)
    tab[0:1, :] = back_row.astype(I32)
    tab[1:2, :] = sums_row.astype(I32)

    table_copy(0, slot).wait()
    for part in range(PLACES // 8):
        table_copy(1 + part, pick.at[part]).wait()

    forward_ring(0, 4)
    ring_arrival(0, 1, 4)
    ring_arrival(1, -1, 4)

    def x_copy(chunk, step):
        return send_to(
            x_pack.at[chunk, pl.ds(((x + step) % NX) * PLACES, PLACES)],
            x_recv[chunk].at[pl.ds(x * PLACES, PLACES)],
            x_send.at[chunk, step],
            x_sem.at[chunk, step],
            x_device(step),
        )

    def y_copy(chunk, step):
        return send_to(
            y_pack.at[chunk, pl.ds(((y + step) % NY) * PLACES, PLACES)],
            y_recv[chunk].at[pl.ds(y * PLACES, PLACES)],
            y_send.at[chunk, step],
            y_sem.at[chunk, step],
            y_device(step),
        )

    def along_x(chunk):
        def fill(to, carry):
            for k in range(PLACES):
                index = jnp.clip(pick[k // 8, k % 8, to * 4], 1, COLUMN) - 1
                x_pack[chunk, to * PLACES + k] = ag[chunk][index]
            return carry

        lax.fori_loop(0, NX, fill, 0)
        for step in range(1, NX):
            x_copy(chunk, step).start()
        own = pl.ds(x * PLACES, PLACES)
        x_recv[chunk][own] = x_pack[chunk, own]

    def along_y(chunk):
        for step in range(1, NX):
            x_copy(chunk, step).wait_recv()

        def fill(to, carry):
            for k in range(PLACES):
                index = jnp.clip(turn[to, k], 1, ROWS) - 1
                y_pack[chunk, to * PLACES + k] = x_recv[chunk][index]
            return carry

        lax.fori_loop(0, NY, fill, 0)
        for step in range(1, NY):
            y_copy(chunk, step).start()
        own = pl.ds(y * PLACES, PLACES)
        y_recv[chunk][own] = y_pack[chunk, own]

    def pair_copy(part):
        return send_to(
            other.at[part],
            win.at[core, part],
            pair_send.at[part],
            pair_recv.at[part],
            partner,
        )

    def take(chunk):
        for step in range(1, NY):
            y_copy(chunk, step).wait_recv()
        part, half = chunk // 2, chunk % 2

        def lay(r, carry):
            first = pl.multiple_of(r * PR + half * 8, 8)
            for side in range(2):
                k = r * 2 + side
                lanes_of = slice(side * PW, side * PW + PW)
                keep = jnp.clip(slot[0, core * CELLS + k], 0, ROWS - 1)
                give = jnp.clip(slot[0, (1 - core) * CELLS + k], 0, ROWS - 1)
                win[core, part, pl.ds(first, 8), lanes_of] = y_recv[chunk][keep]
                other[part, pl.ds(first, 8), lanes_of] = y_recv[chunk][give]
            return carry

        lax.fori_loop(0, W // PR, lay, 0)

    along_x(0)
    along_x(1)

    for step in range(1, NX):
        mark_copy(0, step).wait()
    counts = marks_x[:, 0, :].astype(F32)
    starts = marks_x[:, 1, :].astype(F32)
    four = iota((NX, 128), 1)
    wide = four.astype(F32)
    giver = iota((NX, 128), 0).astype(F32)
    onward = []
    back = jnp.zeros((NX, 128), F32)
    for to in range(NY):
        mine = four == to * 16 + x * 4
        many = jnp.sum(jnp.where(mine, counts, 0.0), axis=1, keepdims=True)
        low = jnp.sum(jnp.where(mine, starts, 0.0), axis=1, keepdims=True)
        first = exclusive(many)
        inside = (wide >= first) & (wide < first + many)
        onward.append(
            jnp.sum(
                jnp.where(inside, giver * PLACES + low + wide - first + 1.0, 0.0),
                axis=0,
                keepdims=True,
            )
        )
        inside = (wide >= low) & (wide < low + many)
        back = back + jnp.where(inside, to * PLACES + first + wide - low + 1.0, 0.0)
    last = 1 + PLACES // 8
    tables[last] = jnp.concatenate(onward + [jnp.zeros((4, 128), F32)], axis=0).astype(I32)
    table_copy(last, turn).start()
    tab[8:12, :] = back.astype(I32)
    mark[1] = jnp.broadcast_to(
        jnp.max(marks_x[:, 2, :].astype(F32), axis=0, keepdims=True), (8, 128)
    ).astype(I32)
    marks_y[y] = mark[1]
    for step in range(1, NY):
        mark_copy(1, step).start()
    table_copy(last, turn).wait()

    forward_ring(2, 2)
    along_y(0)
    forward_ring(2, 3)
    along_y(1)
    for step in range(1, NY):
        mark_copy(1, step).wait()
    mark[2] = jnp.max(marks_y[...].astype(F32), axis=0).astype(I32)
    marks_z[z] = mark[2]
    for step in range(1, NZ):
        mark_copy(2, step).start()
    forward_ring(2, 4)
    ring_arrival(2, 1, 4)
    along_x(2)
    ring_arrival(3, -1, 4)
    along_x(3)
    take(0)
    take(1)
    pair_copy(0).start()
    for step in range(1, NZ):
        mark_copy(2, step).wait()
    flag[...] = jnp.max(marks_z[...].astype(F32), axis=0).astype(I32)
    along_y(2)
    along_y(3)
    take(2)
    take(3)
    pair_copy(1).start()
    for chunk in range(CHUNKS):
        for direction in (1, -1):
            for hop in range(1, hops(chunk, direction) + 1):
                ring_copy(chunk, direction, hop).wait_send()
        for step in range(1, NX):
            x_copy(chunk, step).wait_send()
            y_copy(chunk, step).wait_send()
    pair_copy(0).wait()
    pair_copy(1).wait()


def fetch_windows(owned, wanted, cells):
    vmem = pl.BlockSpec(memory_space=pltpu.VMEM)
    tile = (8, 128)
    dma = pltpu.SemaphoreType.DMA
    return pl.pallas_call(
        gather_kernel,
        out_shape=(
            jax.ShapeDtypeStruct((2, 2, W, W), F32),
            jax.ShapeDtypeStruct((16, 128), I32),
            jax.ShapeDtypeStruct(tile, I32),
        ),
        in_specs=[vmem] * 3,
        out_specs=(vmem, vmem, vmem),
        scratch_shapes=[
            [pltpu.VMEM((COLUMN,) + tile, F32)] * CHUNKS,
            pltpu.VMEM((NZ,) + tile, I32),
            pltpu.VMEM((NZ,) + tile, I32),
            pltpu.VMEM((2 + PLACES // 8,) + tile, I32),
            pltpu.SMEM((PLACES // 8,) + tile, I32),
            pltpu.SMEM(tile, I32),
            pltpu.SMEM(tile, I32),
            pltpu.VMEM((CHUNKS, ROWS) + tile, F32),
            [pltpu.VMEM((ROWS,) + tile, F32)] * CHUNKS,
            pltpu.VMEM((CHUNKS, ROWS) + tile, F32),
            [pltpu.VMEM((ROWS,) + tile, F32)] * CHUNKS,
            pltpu.VMEM((3,) + tile, I32),
            pltpu.VMEM((NX,) + tile, I32),
            pltpu.VMEM((NY,) + tile, I32),
            pltpu.VMEM((NZ,) + tile, I32),
            pltpu.VMEM((2, W, W), F32),
            dma((CHUNKS, 2, 4)),
            dma((CHUNKS, 2, 4)),
            dma((NZ,)),
            dma((NZ,)),
            dma((3, NZ)),
            dma((3, NZ)),
            dma((CHUNKS, NX)),
            dma((CHUNKS, NX)),
            dma((CHUNKS, NY)),
            dma((CHUNKS, NY)),
            dma((2,)),
            dma((2,)),
            dma((2 + PLACES // 8,)),
        ],
        compiler_params=pltpu.CompilerParams(collective_id=0, has_side_effects=True),
        name="fetch_windows",
    )(owned, wanted, cells)


def parts(value):
    high = value.astype(BF16)
    return high, (value - high.astype(F32)).astype(BF16)


def from_left(real, imag, table, sign):
    high, low = parts(jnp.concatenate([real, imag], axis=1))
    out = jnp.dot(
        table[...], jnp.concatenate([high, low, high], axis=0), preferred_element_type=F32
    )
    return out[:W, :W] - sign * out[W:, W:], out[:W, W:] + sign * out[W:, :W]


def from_right(real, imag, table, sign):
    high, low = parts(jnp.concatenate([real, imag], axis=0))
    out = lax.dot_general(
        jnp.concatenate([high, low, high], axis=1),
        table[...],
        (((1,), (1,)), ((), ())),
        preferred_element_type=F32,
    )
    return out[:W, :W] - sign * out[W:, W:], sign * out[:W, W:] + out[W:, :W]


def both_sides(real, imag, table, sign):
    real, imag = from_left(real, imag, table, sign)
    return from_right(real, imag, table, sign)


def position_kernel(win, probe, measured, dft, move, grad):
    core = lax.axis_index("section")

    def lay(index, real, imag):
        for k in range(CELLS):
            rows = slice(k // 2 * PR, k // 2 * PR + PR)
            lanes = slice(k % 2 * PW, k % 2 * PW + PW)
            grad[index, k, 0] = real[rows, lanes]
            grad[index, k, 1] = imag[rows, lanes]

    pr, pi = probe[0], probe[1]
    ar, ai = win[0, 0], win[0, 1]
    wave_r, wave_i = both_sides(pr * ar - pi * ai, pr * ai + pi * ar, move, 1.0)
    br, bi = win[1, 0], win[1, 1]
    far_r, far_i = both_sides(
        wave_r * br - wave_i * bi, wave_r * bi + wave_i * br, dft, 1.0
    )
    gap = far_r * far_r + far_i * far_i - measured[core]
    back_r, back_i = both_sides(gap * far_r, gap * far_i, dft, -1.0)
    lay(1, wave_r * back_r + wave_i * back_i, wave_r * back_i - wave_i * back_r)
    br, bi = win[1, 0], win[1, 1]
    low_r, low_i = both_sides(
        br * back_r + bi * back_i, br * back_i - bi * back_r, move, -1.0
    )
    pr, pi = probe[0], probe[1]
    lay(0, pr * low_r + pi * low_i, pr * low_i - pi * low_r)


def position_gradients(windows, probe_wave, intensities, dft, move):
    vmem = pl.BlockSpec(memory_space=pltpu.VMEM)
    return pl.pallas_call(
        position_kernel,
        out_shape=jax.ShapeDtypeStruct((2, CELLS, 2, PR, PW), F32),
        in_specs=[vmem] * 5,
        out_specs=vmem,
        name="position_gradients",
    )(windows, probe_wave, intensities, dft, move)


def return_kernel(
    grad,
    places,
    tab,
    out,
    cells,
    y_pack,
    y_recv,
    x_pack,
    x_recv,
    total,
    ring,
    mix,
    pair_send,
    pair_recv,
    y_send,
    y_sem,
    x_send,
    x_sem,
    rs_send,
    rs_recv,
):
    core, y, z, x = place()
    partner = device(1 - core, y, z, x)

    def ring_device(step):
        return device(core, y, (z + step) % NZ, x)

    def x_device(step):
        return device(core, y, z, (x + step) % NX)

    def y_device(step):
        return device(core, (y + step) % NY, z, x)

    greet(
        pltpu.get_barrier_semaphore(),
        [ring_device(1), ring_device(NZ - 1)]
        + [x_device(step) for step in range(1, NX)]
        + [y_device(step) for step in range(1, NY)]
        + [partner],
    )

    def pair_copy(chunk):
        return send_to(
            grad.at[1 - core, :, chunk],
            cells[chunk].at[pl.ds(core * CELLS, CELLS)],
            pair_send.at[chunk],
            pair_recv.at[chunk],
            partner,
        )

    for chunk in range(CHUNKS):
        pair_copy(chunk).start()
    for chunk in range(CHUNKS):
        cells[chunk][pl.ds(core * CELLS, CELLS)] = grad[core, :, chunk]

    mix[...] = jnp.where(
        jnp.broadcast_to(tab[1:2, :], (COLUMN, ROWS)) == iota((COLUMN, ROWS), 0) + 1, 1.0, 0.0
    ).astype(BF16)

    def y_copy(chunk, step):
        return send_to(
            y_pack.at[chunk, pl.ds(((y + step) % NY) * PLACES, PLACES)],
            y_recv[chunk].at[pl.ds(y * PLACES, PLACES)],
            y_send.at[chunk, step],
            y_sem.at[chunk, step],
            y_device(step),
        )

    def x_copy(chunk, step):
        return send_to(
            x_pack.at[chunk, pl.ds(((x + step) % NX) * (PLACES * 8), PLACES * 8)],
            x_recv.at[chunk, pl.ds(x * (PLACES * 8), PLACES * 8)],
            x_send.at[chunk, step],
            x_sem.at[chunk, step],
            x_device(step),
        )

    for chunk in range(CHUNKS):
        pair_copy(chunk).wait_recv()

        def fill_y(to, carry):
            for k in range(PLACES):
                index = jnp.clip(places[0, to * PLACES + k], 0, MB * CELLS - 1)
                y_pack[chunk, to * PLACES + k] = cells[chunk][index]
            return carry

        lax.fori_loop(0, NY, fill_y, 0)
        for step in range(1, NY):
            y_copy(chunk, step).start()
        own = pl.ds(y * PLACES, PLACES)
        y_recv[chunk][own] = y_pack[chunk, own]

    def along_x(chunk):
        for step in range(1, NY):
            y_copy(chunk, step).wait_recv()

        def fill_x(to, carry):
            for k in range(PLACES):
                index = jnp.clip(places[8 + to, k], 1, ROWS) - 1
                spot = pl.ds(pl.multiple_of((to * PLACES + k) * 8, 8), 8)
                x_pack[chunk, spot] = y_recv[chunk][index]
            return carry

        lax.fori_loop(0, NX, fill_x, 0)
        for step in range(1, NX):
            x_copy(chunk, step).start()
        own = pl.ds(x * (PLACES * 8), PLACES * 8)
        x_recv[chunk, own] = x_pack[chunk, own]

    def block(zz):
        return pl.ds(((zz + 2 * NZ) % NZ) * (OWN * 8), OWN * 8)

    def ring_copy(chunk, direction, step):
        side = 0 if direction > 0 else 1
        reach = hops(chunk, direction)
        return send_to(
            total.at[chunk, block(z + direction * reach)]
            if step == 1
            else ring.at[chunk, side, step - 2],
            ring.at[chunk, side, step - 1],
            rs_send.at[chunk, side, step - 1],
            rs_recv.at[chunk, side, step - 1],
            ring_device(direction + NZ),
        )

    def sum_cells(chunk):
        for step in range(1, NX):
            x_copy(chunk, step).wait_recv()

        def add(r, carry):
            high, low = parts(x_recv[chunk, pl.ds(r, ROWS, stride=8), :])
            both = jnp.dot(
                mix[...], jnp.concatenate([high, low], axis=1), preferred_element_type=F32
            )
            total[chunk, pl.ds(r, COLUMN, stride=8), :] = both[:, :128] + both[:, 128:]
            return carry

        lax.fori_loop(0, 8, add, 0)
        for direction in (1, -1):
            ring_copy(chunk, direction, 1).start()

    def pass_on(chunk, step):
        for direction in (1, -1):
            reach = hops(chunk, direction)
            side = 0 if direction > 0 else 1
            if step <= reach:
                ring_copy(chunk, direction, step - 1).wait_recv()
                ring[chunk, side, step - 2] += total[
                    chunk, block(z + direction * (reach - step + 1))
                ]
                ring_copy(chunk, direction, step).start()

    def finish(chunk):
        value = total[chunk, block(z)]
        for direction in (1, -1):
            reach = hops(chunk, direction)
            side = 0 if direction > 0 else 1
            ring_copy(chunk, direction, reach).wait_recv()
            value = value + ring[chunk, side, reach - 1]
        out[:, chunk] = value.reshape(OWN, 8, 128)

    along_x(0)
    along_x(1)
    sum_cells(0)
    along_x(2)
    sum_cells(1)
    pass_on(0, 2)
    along_x(3)
    pass_on(1, 2)
    sum_cells(2)
    pass_on(0, 3)
    pass_on(1, 3)
    pass_on(2, 2)
    sum_cells(3)
    pass_on(0, 4)
    pass_on(1, 4)
    pass_on(2, 3)
    pass_on(3, 2)
    finish(0)
    finish(1)
    pass_on(2, 4)
    pass_on(3, 3)
    finish(2)
    pass_on(3, 4)
    finish(3)

    for chunk in range(CHUNKS):
        pair_copy(chunk).wait_send()
        for direction in (1, -1):
            for step in range(1, hops(chunk, direction) + 1):
                ring_copy(chunk, direction, step).wait_send()
        for step in range(1, NX):
            x_copy(chunk, step).wait_send()
            y_copy(chunk, step).wait_send()


def return_gradients(gradients, table):
    vmem = pl.BlockSpec(memory_space=pltpu.VMEM)
    smem = pl.BlockSpec(memory_space=pltpu.SMEM)
    tile = (8, 128)
    dma = pltpu.SemaphoreType.DMA
    return pl.pallas_call(
        return_kernel,
        out_shape=jax.ShapeDtypeStruct((OWN, CHUNKS) + tile, F32),
        in_specs=[vmem, smem, vmem],
        out_specs=vmem,
        scratch_shapes=[
            [pltpu.VMEM((MB * CELLS,) + tile, F32)] * CHUNKS,
            pltpu.VMEM((CHUNKS, ROWS) + tile, F32),
            [pltpu.VMEM((ROWS,) + tile, F32)] * CHUNKS,
            pltpu.VMEM((CHUNKS, ROWS * 8, 128), F32),
            pltpu.VMEM((CHUNKS, ROWS * 8, 128), F32),
            pltpu.VMEM((CHUNKS, COLUMN * 8, 128), F32),
            pltpu.VMEM((CHUNKS, 2, 4, OWN * 8, 128), F32),
            pltpu.VMEM((COLUMN, ROWS), BF16),
            dma((CHUNKS,)),
            dma((CHUNKS,)),
            dma((CHUNKS, NY)),
            dma((CHUNKS, NY)),
            dma((CHUNKS, NX)),
            dma((CHUNKS, NX)),
            dma((CHUNKS, 2, 4)),
            dma((CHUNKS, 2, 4)),
        ],
        compiler_params=pltpu.CompilerParams(collective_id=1, has_side_effects=True),
        name="return_gradients",
    )(gradients, table, table)


def swapped(block):
    return lax.ppermute(block, "section", [(0, 1), (1, 0)])


def full_windows(owned, send_plan, cell_slot):
    core = lax.axis_index("section")
    outbound = jnp.swapaxes(send_plan, 0, 1)
    patches = owned[jnp.maximum(outbound, 0)]
    arrived = lax.all_to_all(patches, "tile", split_axis=0, concat_axis=0, tiled=True)
    windows = []
    for batch in range(MB):
        flat = arrived[:, batch].reshape((-1, 2, PR, PW))
        picked = flat[cell_slot[batch]].reshape(W // PR, W // PW, 2, PR, PW)
        windows.append(jnp.transpose(picked, (2, 0, 3, 1, 4)).reshape(2, W, W))
    windows = jnp.stack(windows)
    passed = swapped(lax.dynamic_index_in_dim(windows, 1 - core, 0, keepdims=False))
    kept = lax.dynamic_index_in_dim(windows, core, 0, keepdims=False)
    first = core == 0
    return jnp.stack([jnp.where(first, kept, passed), jnp.where(first, passed, kept)])


def full_sums(gradients, send_plan, cell_slot):
    core = lax.axis_index("section")
    passed = swapped(lax.dynamic_index_in_dim(gradients, 1 - core, 0, keepdims=False))
    kept = lax.dynamic_index_in_dim(gradients, core, 0, keepdims=False)
    first = core == 0
    batches = [jnp.where(first, kept, passed), jnp.where(first, passed, kept)]
    slots = 2 * NX * NY * NZ
    placed = [
        jnp.zeros((slots, 2, PR, PW), F32)
        .at[cell_slot[batch]]
        .set(batches[batch])
        .reshape(slots // 2, 2, 2, PR, PW)
        for batch in range(MB)
    ]
    returned = lax.all_to_all(
        jnp.stack(placed, axis=1), "tile", split_axis=0, concat_axis=0, tiled=True
    )
    outbound = jnp.swapaxes(send_plan, 0, 1)
    target = jnp.where(outbound < 0, OWN, outbound).reshape(-1)
    sums = jax.ops.segment_sum(
        returned.reshape((-1, 2, PR, PW)), target, num_segments=OWN + 1
    )
    return sums[:OWN]


def body(dft, move, object_slices, probe_wave, intensities, send_list, cell_slot):
    owned = object_slices[0]
    send_plan = send_list[0]
    wanted = jnp.transpose(send_plan.reshape(MB, NY, NZ, NX, 2), (2, 1, 3, 0, 4))
    wanted = jnp.pad(wanted.reshape(NZ, 1, 64), ((0, 0), (0, 0), (0, 64)))
    wanted = jnp.broadcast_to(wanted, (NZ, 8, 128))
    windows, table, flag = fetch_windows(
        owned.reshape(OWN, CHUNKS, 8, 128), wanted, cell_slot.reshape(1, MB * CELLS)
    )
    crowded = flag[0, 0] > 0
    windows = lax.cond(
        crowded,
        lambda: full_windows(owned, send_plan, cell_slot),
        lambda: windows,
    )
    gradients = position_gradients(windows, probe_wave, intensities, dft, move)
    sums = lax.cond(
        crowded,
        lambda: full_sums(gradients, send_plan, cell_slot),
        lambda: return_gradients(
            gradients.reshape(2, CELLS, CHUNKS, 8, 128), table
        ).reshape(OWN, 2, PR, PW),
    )
    return sums[None]


def solution(mesh):
    dft, move = matrix_tables()
    in_specs = (
        P("section", "tile", None, None, None),
        P(),
        P("tile", None, None),
        P("tile", None, None, None),
        P("tile", None),
    )
    out_specs = P("section", "tile", None, None, None)
    step = functools.partial(body, jnp.asarray(dft), jnp.asarray(move))
    return jax.shard_map(step, mesh=mesh, in_specs=in_specs, out_specs=out_specs, check_vma=False)
```

```python
import functools

import jax
import jax.numpy as jnp
import ml_dtypes
import numpy as np
from jax import lax
from jax.experimental import pallas as pl
from jax.experimental.pallas import tpu as pltpu
from jax.sharding import PartitionSpec as P

W = 256
PW = 128
PR = 16
MB = 2
CELLS = 32
NX, NY, NZ = 4, 4, 8
PLANE = NX * NY
OWN = 32
COLUMN = NZ * OWN
PLACES = 32
ROWS = 4 * PLACES
CHUNKS = 8
TALL = 4
PHASE_SCALE = 20.0
MESH = pl.DeviceIdType.MESH
F32 = jnp.float32
I32 = jnp.int32
BF16 = jnp.bfloat16


FETCH = (
    ("s", 0, -1, 1),
    ("s", 0, 1, 1),
    ("s", 1, -1, 1),
    ("s", 1, 1, 1),
    ("s", 2, -1, 1),
    ("s", 2, 1, 1),
    ("s", 0, -1, 2),
    ("s", 0, 1, 2),
    ("s", 1, -1, 2),
    ("s", 1, 1, 2),
    ("s", 2, -1, 2),
    ("s", 2, 1, 2),
    ("s", 0, -1, 3),
    ("s", 0, 1, 3),
    ("s", 1, -1, 3),
    ("s", 1, 1, 3),
    ("s", 2, -1, 3),
    ("s", 2, 1, 3),
    ("s", 0, 1, 4),
    ("s", 3, -1, 1),
    ("s", 1, -1, 4),
    ("s", 3, 1, 1),
    ("s", 2, 1, 4),
    ("s", 4, -1, 1),
    ("s", 3, -1, 2),
    ("x", 0),
    ("s", 4, 1, 1),
    ("x", 1),
    ("s", 3, 1, 2),
    ("s", 5, -1, 1),
    ("s", 4, -1, 2),
    ("x", 2),
    ("s", 5, 1, 1),
    ("s", 3, -1, 3),
    ("s", 4, 1, 2),
    ("s", 5, -1, 2),
    ("s", 3, 1, 3),
    ("y", 0),
    ("s", 4, -1, 3),
    ("s", 5, 1, 2),
    ("s", 3, -1, 4),
    ("s", 4, 1, 3),
    ("y", 1),
    ("s", 5, -1, 3),
    ("s", 6, 1, 1),
    ("s", 5, 1, 3),
    ("y", 2),
    ("s", 6, -1, 1),
    ("x", 3),
    ("s", 4, 1, 4),
    ("s", 7, -1, 1),
    ("s", 5, -1, 4),
    ("s", 6, 1, 2),
    ("t", 0),
    ("s", 6, -1, 2),
    ("s", 7, 1, 1),
    ("x", 4),
    ("s", 7, -1, 2),
    ("y", 3),
    ("s", 6, 1, 3),
    ("x", 5),
    ("s", 7, 1, 2),
    ("s", 6, -1, 3),
    ("s", 7, -1, 3),
    ("s", 6, 1, 4),
    ("y", 4),
    ("s", 7, 1, 3),
    ("t", 1),
    ("s", 7, -1, 4),
    ("y", 5),
    ("x", 6),
    ("x", 7),
    ("t", 2),
    ("y", 6),
    ("y", 7),
    ("t", 3),
)
RETURN = (
    ("x", 0),
    ("x", 1),
    ("a", 0),
    ("x", 2),
    ("a", 1),
    ("x", 3),
    ("p", 0, -1, 2),
    ("p", 0, 1, 2),
    ("x", 4),
    ("a", 2),
    ("p", 1, -1, 2),
    ("p", 1, 1, 2),
    ("p", 0, -1, 3),
    ("p", 0, 1, 3),
    ("x", 5),
    ("a", 3),
    ("p", 2, -1, 2),
    ("p", 2, 1, 2),
    ("x", 6),
    ("a", 4),
    ("p", 1, -1, 3),
    ("p", 1, 1, 3),
    ("p", 0, 1, 4),
    ("x", 7),
    ("p", 3, -1, 2),
    ("p", 3, 1, 2),
    ("a", 5),
    ("p", 2, -1, 3),
    ("p", 2, 1, 3),
    ("p", 4, -1, 2),
    ("p", 4, 1, 2),
    ("a", 6),
    ("p", 1, -1, 4),
    ("p", 3, -1, 3),
    ("f", 0),
    ("a", 7),
    ("p", 3, 1, 3),
    ("p", 5, -1, 2),
    ("p", 5, 1, 2),
    ("p", 2, 1, 4),
    ("p", 4, -1, 3),
    ("p", 4, 1, 3),
    ("p", 6, -1, 2),
    ("p", 6, 1, 2),
    ("f", 1),
    ("p", 3, -1, 4),
    ("p", 7, 1, 2),
    ("p", 7, -1, 2),
    ("p", 5, -1, 3),
    ("p", 5, 1, 3),
    ("f", 2),
    ("p", 4, 1, 4),
    ("p", 6, -1, 3),
    ("p", 6, 1, 3),
    ("f", 3),
    ("p", 7, -1, 3),
    ("p", 7, 1, 3),
    ("p", 5, -1, 4),
    ("f", 4),
    ("p", 6, 1, 4),
    ("p", 7, -1, 4),
    ("f", 5),
    ("f", 6),
    ("f", 7),
)


def stacked_parts(matrix):
    rows = np.concatenate([matrix.real, matrix.imag], axis=0).astype(np.float32)
    high = rows.astype(ml_dtypes.bfloat16)
    low = (rows - high.astype(np.float32)).astype(ml_dtypes.bfloat16)
    return np.concatenate([high, low], axis=1)


def matrix_tables():
    index = np.arange(W)
    product = np.outer(index, index) % W
    dft = np.exp(-2j * np.pi * product / W) / np.sqrt(W)
    frequency = np.where(index < W // 2, index, index - W).astype(np.float64)
    diagonal = np.exp(-1j * PHASE_SCALE * frequency**2 / (W * W))
    move = np.conj(dft) @ (diagonal[:, None] * dft)
    move = (move + move.T) / 2
    return stacked_parts(dft), stacked_parts(move)


def place():
    tile = lax.axis_index("tile")
    core = lax.axis_index("section")
    y = tile // (NZ * NX)
    z = (tile // NX) % NZ
    x = tile % NX
    return core, y, z, x


def device(core, y, z, x):
    return (core, y * (NZ * NX) + z * NX + x)


def iota(shape, axis):
    return lax.broadcasted_iota(I32, shape, axis)


def to_column(row):
    n = row.shape[1]
    wide = jnp.broadcast_to(row, (n, n))
    return jnp.sum(jnp.where(iota((n, n), 0) == iota((n, n), 1), wide, 0.0), axis=1, keepdims=True)


def exclusive(column):
    rows = [jnp.zeros_like(column[0:1])]
    for step in range(column.shape[0] - 1):
        rows.append(rows[-1] + column[step : step + 1])
    return jnp.concatenate(rows, axis=0)


def send_to(src, dst, send_sem, recv_sem, target):
    return pltpu.make_async_remote_copy(
        src_ref=src,
        dst_ref=dst,
        send_sem=send_sem,
        recv_sem=recv_sem,
        device_id=target,
        device_id_type=MESH,
    )


def greet(barrier, targets):
    for target in targets:
        pl.semaphore_signal(barrier, inc=1, device_id=target, device_id_type=MESH)
    pl.semaphore_wait(barrier, len(targets))


def hops(chunk, direction):
    return 4 if (chunk % 2 == 0) == (direction > 0) else 3


def gather_kernel(
    obj,
    meta,
    cells,
    win,
    tab,
    flag,
    ag,
    metas,
    metain,
    tables,
    pick,
    turn,
    slot,
    x_pack,
    x_recv,
    y_pack,
    y_recv,
    mark,
    marks_x,
    marks_y,
    marks_z,
    other,
    ag_send,
    ag_recv,
    meta_send,
    meta_recv,
    mark_send,
    mark_recv,
    x_send,
    x_sem,
    y_send,
    y_sem,
    pair_send,
    pair_recv,
    local_sem,
):
    core, y, z, x = place()
    partner = device(1 - core, y, z, x)

    def ring_device(step):
        return device(core, y, (z + step) % NZ, x)

    def x_device(step):
        return device(core, y, z, (x + step) % NX)

    def y_device(step):
        return device(core, (y + step) % NY, z, x)

    greet(
        pltpu.get_barrier_semaphore(),
        [ring_device(step) for step in range(1, NZ)]
        + [x_device(step) for step in range(1, NX)]
        + [y_device(step) for step in range(1, NY)]
        + [partner],
    )

    def block(chunk, zz):
        return ag[chunk].at[pl.ds(((zz + 2 * NZ) % NZ) * OWN, OWN)]

    def ring_copy(chunk, direction, hop):
        side = 0 if direction > 0 else 1
        held = block(chunk, z - direction * (hop - 1))
        return send_to(
            obj.at[:, chunk] if hop == 1 else held,
            held,
            ag_send.at[chunk, side, hop - 1],
            ag_recv.at[chunk, side, hop - 1],
            ring_device(direction + NZ),
        )

    def ring_arrival(chunk, direction, hop):
        side = 0 if direction > 0 else 1
        held = block(chunk, z - direction * hop)
        send_to(
            held,
            held,
            ag_send.at[chunk, side, hop - 1],
            ag_recv.at[chunk, side, hop - 1],
            ring_device(direction + NZ),
        ).wait_recv()

    def ring_send(chunk, direction, hop):
        if hop > 1:
            ring_arrival(chunk, direction, hop - 1)
        ring_copy(chunk, direction, hop).start()

    first_wait = min(i for i, event in enumerate(FETCH) if event[0] != "s" or event[3] > 1)
    first_x = min(i for i, event in enumerate(FETCH) if event[0] == "x")
    first_y = min(i for i, event in enumerate(FETCH) if event[0] == "y")
    for event in FETCH[:first_wait]:
        ring_send(*event[1:])

    row = cells[...]
    owner = row >> 1
    entry = ((owner >> 2) & 7) * 4 + (iota(row.shape, 1) >> 5) * 2 + (row & 1)
    code_row = ((owner >> 5) * 128 + (owner & 3) * 32 + entry).astype(F32)
    y_row = (owner >> 5).astype(F32)
    code_col = to_column(code_row)
    y_col = to_column(y_row)
    ahead = (y_col == y_row) & (code_col < code_row)
    rank = jnp.sum(jnp.where(ahead, 1.0, 0.0), axis=0, keepdims=True)
    over = jnp.where(jnp.max(rank, axis=1, keepdims=True) >= PLACES, 1, 0)
    at = y_row * PLACES + jnp.minimum(rank, PLACES - 1.0)
    tables[0] = jnp.zeros((8, 128), I32)
    tables[0, 0:1, 0 : MB * CELLS] = at.astype(I32)
    at_col = to_column(jnp.where(rank < PLACES, at, -1.0))
    spread = jnp.broadcast_to(at_col, (MB * CELLS, ROWS)) == iota((MB * CELLS, ROWS), 1).astype(
        F32
    )
    number = iota((MB * CELLS, ROWS), 0).astype(F32)
    back_row = jnp.sum(jnp.where(spread, number, 0.0), axis=0, keepdims=True)

    lane = iota((8, 128), 1)
    for zz in range(NZ):
        metas[zz] = jnp.where(lane == 64, jnp.broadcast_to(over, (8, 128)), meta[zz])
    metain[z] = metas[z]

    def meta_copy(step):
        return send_to(
            metas.at[(z + step) % NZ],
            metain.at[z],
            meta_send.at[step],
            meta_recv.at[step],
            ring_device(step),
        )

    for step in range(1, NZ):
        meta_copy(step).start()

    def table_copy(index, target):
        return pltpu.make_async_copy(tables.at[index], target, local_sem.at[index])

    table_copy(0, slot).start()

    for chunk in range(CHUNKS):
        ag[chunk][pl.ds(z * OWN, OWN)] = obj[:, chunk]

    half_way = (first_wait + first_x) // 2
    for event in FETCH[first_wait:half_way]:
        ring_send(*event[1:])

    for step in range(1, NZ):
        meta_copy(step).wait()
    wanted = metain[:, 0, :].astype(F32)
    lanes = iota((NZ, 128), 1)
    valid = (wanted >= 0.0) & (lanes < 64)
    held = jnp.where(valid, 1.0, 0.0)
    big_row, big_lane = iota((128, 128), 0), iota((128, 128), 1)
    one_device = (big_row >> 2) == (big_lane >> 2)
    one_x = ((big_row >> 2) & 3) == ((big_lane >> 2) & 3)
    group = jnp.where(one_device, 1.0, 0.0)
    before = jnp.where(one_device & (big_row < big_lane), 1.0, 0.0)
    column = jnp.where(one_x & (big_row < 64), 1.0, 0.0)
    above = jnp.where(one_x & ((big_row >> 4) < (big_lane >> 4)), 1.0, 0.0)
    in_group = jnp.dot(held, group, preferred_element_type=F32)
    order = jnp.dot(held, before, preferred_element_type=F32) + exclusive(in_group)
    in_all = jnp.sum(held, axis=0, keepdims=True)
    sums = jnp.concatenate([in_all, jnp.zeros((7, 128), F32)], axis=0)
    count = jnp.dot(sums, group, preferred_element_type=F32)[0:1]
    start = jnp.dot(sums, above, preferred_element_type=F32)[0:1]
    whole = jnp.dot(sums, column, preferred_element_type=F32)[0:1]
    order = order + start
    named = iota((NZ, 128), 0).astype(F32) * OWN + wanted + 1.0
    picks = [
        jnp.sum(jnp.where(valid & (order == float(k)), named, 0.0), axis=0, keepdims=True)
        for k in range(PLACES)
    ]
    picks = jnp.dot(jnp.concatenate(picks, axis=0), column, preferred_element_type=F32)
    for part in range(PLACES // 8):
        tables[1 + part] = picks[part * 8 : part * 8 + 8].astype(I32)
        table_copy(1 + part, pick.at[part]).start()
    over_x = jnp.where(jnp.max(whole, axis=1, keepdims=True) > PLACES, 1.0, 0.0)
    over_z = jnp.max(
        jnp.max(jnp.where(lanes == 64, wanted, 0.0), axis=1, keepdims=True), axis=0, keepdims=True
    )
    over = jnp.broadcast_to(jnp.maximum(over_x, over_z), (1, 128))
    mark[0] = jnp.concatenate([count, start, over, jnp.zeros((5, 128), F32)], axis=0).astype(I32)
    marks_x[x] = mark[0]

    def mark_copy(kind, step):
        targets = (x_device, y_device, ring_device)
        arrays = (marks_x, marks_y, marks_z)
        own = (x, y, z)
        return send_to(
            mark.at[kind],
            arrays[kind].at[own[kind]],
            mark_send.at[kind, step],
            mark_recv.at[kind, step],
            targets[kind](step),
        )

    for step in range(1, NX):
        mark_copy(0, step).start()
    target = iota((128, ROWS), 1)
    chosen = jnp.where(iota((128, ROWS), 0) == (target // PLACES) * 4, 1.0, 0.0)
    chosen = jnp.dot(picks, chosen, preferred_element_type=F32)
    here = iota((PLACES, ROWS), 0) == iota((PLACES, ROWS), 1) % PLACES
    sums_row = jnp.sum(jnp.where(here, chosen, 0.0), axis=0, keepdims=True)
    tab[...] = jnp.zeros(tab.shape, I32)
    tab[0:1, :] = back_row.astype(I32)
    tab[1:2, :] = sums_row.astype(I32)

    table_copy(0, slot).wait()
    for part in range(PLACES // 8):
        table_copy(1 + part, pick.at[part]).wait()

    for event in FETCH[half_way:first_x]:
        ring_send(*event[1:])

    def x_copy(chunk, step):
        return send_to(
            x_pack.at[chunk, pl.ds(((x + step) % NX) * PLACES, PLACES)],
            x_recv[chunk].at[pl.ds(x * PLACES, PLACES)],
            x_send.at[chunk, step],
            x_sem.at[chunk, step],
            x_device(step),
        )

    def y_copy(chunk, step):
        return send_to(
            y_pack.at[chunk, pl.ds(((y + step) % NY) * PLACES, PLACES)],
            y_recv[chunk].at[pl.ds(y * PLACES, PLACES)],
            y_send.at[chunk, step],
            y_sem.at[chunk, step],
            y_device(step),
        )

    def along_x(chunk):
        for direction in (1, -1):
            ring_arrival(chunk, direction, hops(chunk, direction))

        def fill(to, carry):
            for k in range(PLACES):
                index = jnp.clip(pick[k // 8, k % 8, to * 4], 1, COLUMN) - 1
                x_pack[chunk, to * PLACES + k] = ag[chunk][index]
            return carry

        lax.fori_loop(0, NX, fill, 0)
        for step in range(1, NX):
            x_copy(chunk, step).start()
        own = pl.ds(x * PLACES, PLACES)
        x_recv[chunk][own] = x_pack[chunk, own]

    def along_y(chunk):
        for step in range(1, NX):
            x_copy(chunk, step).wait_recv()

        def fill(to, carry):
            for k in range(PLACES):
                index = jnp.clip(turn[to, k], 1, ROWS) - 1
                y_pack[chunk, to * PLACES + k] = x_recv[chunk][index]
            return carry

        lax.fori_loop(0, NY, fill, 0)
        for step in range(1, NY):
            y_copy(chunk, step).start()
        own = pl.ds(y * PLACES, PLACES)
        y_recv[chunk][own] = y_pack[chunk, own]

    def pair_copy(part):
        return send_to(
            other.at[part],
            win.at[core, part],
            pair_send.at[part],
            pair_recv.at[part],
            partner,
        )

    def take(quarter):
        low, high = 2 * quarter, 2 * quarter + 1
        for chunk in (low, high):
            for step in range(1, NY):
                y_copy(chunk, step).wait_recv()
        part, half = quarter // 2, quarter % 2

        def both(index):
            index = jnp.clip(index, 0, ROWS - 1)
            return jnp.concatenate([y_recv[low][index], y_recv[high][index]], axis=0)

        def lay(r, carry):
            first = pl.multiple_of(r * PR + half * 8, 8)
            for side in range(2):
                k = r * 2 + side
                lanes_of = slice(side * PW, side * PW + PW)
                win[core, part, pl.ds(first, 8), lanes_of] = both(slot[0, core * CELLS + k])
                other[part, pl.ds(first, 8), lanes_of] = both(slot[0, (1 - core) * CELLS + k])
            return carry

        lax.fori_loop(0, W // PR, lay, 0)

    def run(events):
        for event in events:
            if event[0] == "s":
                ring_send(*event[1:])
            elif event[0] == "x":
                along_x(event[1])
            elif event[0] == "y":
                along_y(event[1])
            else:
                take(event[1])
                if event[1] % 2 == 1:
                    pair_copy(event[1] // 2).start()

    run(FETCH[first_x:first_y])

    for step in range(1, NX):
        mark_copy(0, step).wait()
    counts = marks_x[:, 0, :].astype(F32)
    starts = marks_x[:, 1, :].astype(F32)
    four = iota((NX, 128), 1)
    wide = four.astype(F32)
    giver = iota((NX, 128), 0).astype(F32)
    onward = []
    back = jnp.zeros((NX, 128), F32)
    for to in range(NY):
        mine = four == to * 16 + x * 4
        many = jnp.sum(jnp.where(mine, counts, 0.0), axis=1, keepdims=True)
        low = jnp.sum(jnp.where(mine, starts, 0.0), axis=1, keepdims=True)
        first = exclusive(many)
        inside = (wide >= first) & (wide < first + many)
        onward.append(
            jnp.sum(
                jnp.where(inside, giver * PLACES + low + wide - first + 1.0, 0.0),
                axis=0,
                keepdims=True,
            )
        )
        inside = (wide >= low) & (wide < low + many)
        back = back + jnp.where(inside, to * PLACES + first + wide - low + 1.0, 0.0)
    last = 1 + PLACES // 8
    tables[last] = jnp.concatenate(onward + [jnp.zeros((4, 128), F32)], axis=0).astype(I32)
    table_copy(last, turn).start()
    tab[8:12, :] = back.astype(I32)
    mark[1] = jnp.broadcast_to(
        jnp.max(marks_x[:, 2, :].astype(F32), axis=0, keepdims=True), (8, 128)
    ).astype(I32)
    marks_y[y] = mark[1]
    for step in range(1, NY):
        mark_copy(1, step).start()
    table_copy(last, turn).wait()

    next_y = [i for i, event in enumerate(FETCH) if event[0] == "y"]
    run(FETCH[first_y : next_y[2]])
    for step in range(1, NY):
        mark_copy(1, step).wait()
    mark[2] = jnp.max(marks_y[...].astype(F32), axis=0).astype(I32)
    marks_z[z] = mark[2]
    for step in range(1, NZ):
        mark_copy(2, step).start()
    run(FETCH[next_y[2] : next_y[5]])
    for step in range(1, NZ):
        mark_copy(2, step).wait()
    flag[...] = jnp.max(marks_z[...].astype(F32), axis=0).astype(I32)
    run(FETCH[next_y[5] :])
    for chunk in range(CHUNKS):
        for direction in (1, -1):
            for hop in range(1, hops(chunk, direction) + 1):
                ring_copy(chunk, direction, hop).wait_send()
        for step in range(1, NX):
            x_copy(chunk, step).wait_send()
            y_copy(chunk, step).wait_send()
    pair_copy(0).wait()
    pair_copy(1).wait()


def fetch_windows(owned, wanted, cells):
    vmem = pl.BlockSpec(memory_space=pltpu.VMEM)
    tile, strip = (8, PW), (TALL, PW)
    dma = pltpu.SemaphoreType.DMA
    return pl.pallas_call(
        gather_kernel,
        out_shape=(
            jax.ShapeDtypeStruct((2, 2, W, W), F32),
            jax.ShapeDtypeStruct((16, 128), I32),
            jax.ShapeDtypeStruct(tile, I32),
        ),
        in_specs=[vmem] * 3,
        out_specs=(vmem, vmem, vmem),
        scratch_shapes=[
            [pltpu.VMEM((COLUMN,) + strip, F32)] * CHUNKS,
            pltpu.VMEM((NZ,) + tile, I32),
            pltpu.VMEM((NZ,) + tile, I32),
            pltpu.VMEM((2 + PLACES // 8,) + tile, I32),
            pltpu.SMEM((PLACES // 8,) + tile, I32),
            pltpu.SMEM(tile, I32),
            pltpu.SMEM(tile, I32),
            pltpu.VMEM((CHUNKS, ROWS) + strip, F32),
            [pltpu.VMEM((ROWS,) + strip, F32)] * CHUNKS,
            pltpu.VMEM((CHUNKS, ROWS) + strip, F32),
            [pltpu.VMEM((ROWS,) + strip, F32)] * CHUNKS,
            pltpu.VMEM((3,) + tile, I32),
            pltpu.VMEM((NX,) + tile, I32),
            pltpu.VMEM((NY,) + tile, I32),
            pltpu.VMEM((NZ,) + tile, I32),
            pltpu.VMEM((2, W, W), F32),
            dma((CHUNKS, 2, 4)),
            dma((CHUNKS, 2, 4)),
            dma((NZ,)),
            dma((NZ,)),
            dma((3, NZ)),
            dma((3, NZ)),
            dma((CHUNKS, NX)),
            dma((CHUNKS, NX)),
            dma((CHUNKS, NY)),
            dma((CHUNKS, NY)),
            dma((2,)),
            dma((2,)),
            dma((2 + PLACES // 8,)),
        ],
        compiler_params=pltpu.CompilerParams(collective_id=0, has_side_effects=True),
        name="fetch_windows",
    )(owned, wanted, cells)


def parts(value):
    high = value.astype(BF16)
    return high, (value - high.astype(F32)).astype(BF16)


def from_left(real, imag, table, sign):
    high, low = parts(jnp.concatenate([real, imag], axis=1))
    out = jnp.dot(
        table[...], jnp.concatenate([high, high], axis=0), preferred_element_type=F32
    ) + jnp.dot(table[:, :W], low, preferred_element_type=F32)
    return out[:W, :W] - sign * out[W:, W:], out[:W, W:] + sign * out[W:, :W]


def from_right(real, imag, table, sign):
    high, low = parts(jnp.concatenate([real, imag], axis=0))
    across = (((1,), (1,)), ((), ()))
    out = lax.dot_general(
        jnp.concatenate([high, high], axis=1), table[...], across, preferred_element_type=F32
    ) + lax.dot_general(low, table[:, :W], across, preferred_element_type=F32)
    return out[:W, :W] - sign * out[W:, W:], sign * out[:W, W:] + out[W:, :W]


def both_sides(real, imag, table, sign):
    real, imag = from_left(real, imag, table, sign)
    return from_right(real, imag, table, sign)


def position_kernel(win, probe, measured, dft, move, grad):
    core = lax.axis_index("section")

    def lay(index, real, imag):
        for k in range(CELLS):
            rows = slice(k // 2 * PR, k // 2 * PR + PR)
            lanes = slice(k % 2 * PW, k % 2 * PW + PW)
            grad[index, k, 0] = real[rows, lanes]
            grad[index, k, 1] = imag[rows, lanes]

    pr, pi = probe[0], probe[1]
    ar, ai = win[0, 0], win[0, 1]
    wave_r, wave_i = both_sides(pr * ar - pi * ai, pr * ai + pi * ar, move, 1.0)
    br, bi = win[1, 0], win[1, 1]
    far_r, far_i = both_sides(
        wave_r * br - wave_i * bi, wave_r * bi + wave_i * br, dft, 1.0
    )
    gap = far_r * far_r + far_i * far_i - measured[core]
    back_r, back_i = both_sides(gap * far_r, gap * far_i, dft, -1.0)
    lay(1, wave_r * back_r + wave_i * back_i, wave_r * back_i - wave_i * back_r)
    br, bi = win[1, 0], win[1, 1]
    low_r, low_i = both_sides(
        br * back_r + bi * back_i, br * back_i - bi * back_r, move, -1.0
    )
    pr, pi = probe[0], probe[1]
    lay(0, pr * low_r + pi * low_i, pr * low_i - pi * low_r)


def position_gradients(windows, probe_wave, intensities, dft, move):
    vmem = pl.BlockSpec(memory_space=pltpu.VMEM)
    return pl.pallas_call(
        position_kernel,
        out_shape=jax.ShapeDtypeStruct((2, CELLS, 2, PR, PW), F32),
        in_specs=[vmem] * 5,
        out_specs=vmem,
        name="position_gradients",
    )(windows, probe_wave, intensities, dft, move)


def return_kernel(
    grad,
    places,
    tab,
    out,
    cells,
    y_pack,
    y_recv,
    x_pack,
    x_recv,
    total,
    ring,
    mix,
    pair_send,
    pair_recv,
    y_send,
    y_sem,
    x_send,
    x_sem,
    rs_send,
    rs_recv,
):
    core, y, z, x = place()
    partner = device(1 - core, y, z, x)

    def ring_device(step):
        return device(core, y, (z + step) % NZ, x)

    def x_device(step):
        return device(core, y, z, (x + step) % NX)

    def y_device(step):
        return device(core, (y + step) % NY, z, x)

    greet(
        pltpu.get_barrier_semaphore(),
        [ring_device(1), ring_device(NZ - 1)]
        + [x_device(step) for step in range(1, NX)]
        + [y_device(step) for step in range(1, NY)]
        + [partner],
    )

    def pair_copy(chunk):
        return send_to(
            grad.at[1 - core, :, chunk],
            cells[chunk].at[pl.ds(core * CELLS, CELLS)],
            pair_send.at[chunk],
            pair_recv.at[chunk],
            partner,
        )

    for chunk in range(CHUNKS):
        pair_copy(chunk).start()
    for chunk in range(CHUNKS):
        cells[chunk][pl.ds(core * CELLS, CELLS)] = grad[core, :, chunk]

    mix[...] = jnp.where(
        jnp.broadcast_to(tab[1:2, :], (COLUMN, ROWS)) == iota((COLUMN, ROWS), 0) + 1, 1.0, 0.0
    ).astype(BF16)

    def y_copy(chunk, step):
        return send_to(
            y_pack.at[chunk, pl.ds(((y + step) % NY) * PLACES, PLACES)],
            y_recv[chunk].at[pl.ds(y * PLACES, PLACES)],
            y_send.at[chunk, step],
            y_sem.at[chunk, step],
            y_device(step),
        )

    def x_copy(chunk, step):
        return send_to(
            x_pack.at[chunk, pl.ds(((x + step) % NX) * (PLACES * TALL), PLACES * TALL)],
            x_recv.at[chunk, pl.ds(x * (PLACES * TALL), PLACES * TALL)],
            x_send.at[chunk, step],
            x_sem.at[chunk, step],
            x_device(step),
        )

    for chunk in range(CHUNKS):
        pair_copy(chunk).wait_recv()

        def fill_y(to, carry):
            for k in range(PLACES):
                index = jnp.clip(places[0, to * PLACES + k], 0, MB * CELLS - 1)
                y_pack[chunk, to * PLACES + k] = cells[chunk][index]
            return carry

        lax.fori_loop(0, NY, fill_y, 0)
        for step in range(1, NY):
            y_copy(chunk, step).start()
        own = pl.ds(y * PLACES, PLACES)
        y_recv[chunk][own] = y_pack[chunk, own]

    def along_x(chunk):
        for step in range(1, NY):
            y_copy(chunk, step).wait_recv()

        def fill_x(to, carry):
            for k in range(0, PLACES, 2):
                two = [jnp.clip(places[8 + to, k + i], 1, ROWS) - 1 for i in range(2)]
                spot = pl.ds(pl.multiple_of((to * PLACES + k) * TALL, 8), 2 * TALL)
                x_pack[chunk, spot] = jnp.concatenate([y_recv[chunk][i] for i in two], axis=0)
            return carry

        lax.fori_loop(0, NX, fill_x, 0)
        for step in range(1, NX):
            x_copy(chunk, step).start()
        own = pl.ds(x * (PLACES * TALL), PLACES * TALL)
        x_recv[chunk, own] = x_pack[chunk, own]

    def block(zz):
        return pl.ds(((zz + 2 * NZ) % NZ) * (OWN * TALL), OWN * TALL)

    def ring_copy(chunk, direction, step):
        side = 0 if direction > 0 else 1
        reach = hops(chunk, direction)
        return send_to(
            total.at[chunk, block(z + direction * reach)]
            if step == 1
            else ring.at[chunk, side, step - 2],
            ring.at[chunk, side, step - 1],
            rs_send.at[chunk, side, step - 1],
            rs_recv.at[chunk, side, step - 1],
            ring_device(direction + NZ),
        )

    def sum_cells(chunk):
        for step in range(1, NX):
            x_copy(chunk, step).wait_recv()

        def add(r, carry):
            high, low = parts(x_recv[chunk, pl.ds(r, ROWS, stride=TALL), :])
            both = jnp.dot(
                mix[...], jnp.concatenate([high, low], axis=1), preferred_element_type=F32
            )
            total[chunk, pl.ds(r, COLUMN, stride=TALL), :] = both[:, :128] + both[:, 128:]
            return carry

        lax.fori_loop(0, TALL, add, 0)
        for direction in (1, -1):
            ring_copy(chunk, direction, 1).start()

    def pass_on(chunk, direction, step):
        reach = hops(chunk, direction)
        side = 0 if direction > 0 else 1
        ring_copy(chunk, direction, step - 1).wait_recv()
        ring[chunk, side, step - 2] += total[chunk, block(z + direction * (reach - step + 1))]
        ring_copy(chunk, direction, step).start()

    def last(chunk):
        value = total[chunk, block(z)]
        for direction in (1, -1):
            reach = hops(chunk, direction)
            side = 0 if direction > 0 else 1
            ring_copy(chunk, direction, reach).wait_recv()
            value = value + ring[chunk, side, reach - 1]
        return value

    def finish(quarter):
        low, high = last(2 * quarter), last(2 * quarter + 1)
        for p in range(OWN):
            rows = slice(p * TALL, p * TALL + TALL)
            spot = p * CHUNKS * TALL + quarter * 8
            out[spot : spot + 8] = jnp.concatenate([low[rows], high[rows]], axis=0)

    ended = set()
    for event in RETURN:
        if event[0] == "x":
            along_x(event[1])
        elif event[0] == "a":
            sum_cells(event[1])
        elif event[0] == "p":
            pass_on(*event[1:])
        else:
            ended.add(event[1])
            if event[1] ^ 1 in ended:
                finish(event[1] // 2)

    for chunk in range(CHUNKS):
        pair_copy(chunk).wait_send()
        for direction in (1, -1):
            for step in range(1, hops(chunk, direction) + 1):
                ring_copy(chunk, direction, step).wait_send()
        for step in range(1, NX):
            x_copy(chunk, step).wait_send()
            y_copy(chunk, step).wait_send()


def return_gradients(gradients, table):
    vmem = pl.BlockSpec(memory_space=pltpu.VMEM)
    smem = pl.BlockSpec(memory_space=pltpu.SMEM)
    tile, strip = (8, PW), (TALL, PW)
    dma = pltpu.SemaphoreType.DMA
    return pl.pallas_call(
        return_kernel,
        out_shape=jax.ShapeDtypeStruct((OWN * CHUNKS * TALL, PW), F32),
        in_specs=[vmem, smem, vmem],
        out_specs=vmem,
        scratch_shapes=[
            [pltpu.VMEM((MB * CELLS,) + strip, F32)] * CHUNKS,
            pltpu.VMEM((CHUNKS, ROWS) + strip, F32),
            [pltpu.VMEM((ROWS,) + strip, F32)] * CHUNKS,
            pltpu.VMEM((CHUNKS, ROWS * TALL, 128), F32),
            pltpu.VMEM((CHUNKS, ROWS * TALL, 128), F32),
            pltpu.VMEM((CHUNKS, COLUMN * TALL, 128), F32),
            pltpu.VMEM((CHUNKS, 2, 4, OWN * TALL, 128), F32),
            pltpu.VMEM((COLUMN, ROWS), BF16),
            dma((CHUNKS,)),
            dma((CHUNKS,)),
            dma((CHUNKS, NY)),
            dma((CHUNKS, NY)),
            dma((CHUNKS, NX)),
            dma((CHUNKS, NX)),
            dma((CHUNKS, 2, 4)),
            dma((CHUNKS, 2, 4)),
        ],
        compiler_params=pltpu.CompilerParams(collective_id=1, has_side_effects=True),
        name="return_gradients",
    )(gradients, table, table)


def swapped(block):
    return lax.ppermute(block, "section", [(0, 1), (1, 0)])


def full_windows(owned, send_plan, cell_slot):
    core = lax.axis_index("section")
    outbound = jnp.swapaxes(send_plan, 0, 1)
    patches = owned[jnp.maximum(outbound, 0)]
    arrived = lax.all_to_all(patches, "tile", split_axis=0, concat_axis=0, tiled=True)
    windows = []
    for batch in range(MB):
        flat = arrived[:, batch].reshape((-1, 2, PR, PW))
        picked = flat[cell_slot[batch]].reshape(W // PR, W // PW, 2, PR, PW)
        windows.append(jnp.transpose(picked, (2, 0, 3, 1, 4)).reshape(2, W, W))
    windows = jnp.stack(windows)
    passed = swapped(lax.dynamic_index_in_dim(windows, 1 - core, 0, keepdims=False))
    kept = lax.dynamic_index_in_dim(windows, core, 0, keepdims=False)
    first = core == 0
    return jnp.stack([jnp.where(first, kept, passed), jnp.where(first, passed, kept)])


def full_sums(gradients, send_plan, cell_slot):
    core = lax.axis_index("section")
    passed = swapped(lax.dynamic_index_in_dim(gradients, 1 - core, 0, keepdims=False))
    kept = lax.dynamic_index_in_dim(gradients, core, 0, keepdims=False)
    first = core == 0
    batches = [jnp.where(first, kept, passed), jnp.where(first, passed, kept)]
    slots = 2 * NX * NY * NZ
    placed = [
        jnp.zeros((slots, 2, PR, PW), F32)
        .at[cell_slot[batch]]
        .set(batches[batch])
        .reshape(slots // 2, 2, 2, PR, PW)
        for batch in range(MB)
    ]
    returned = lax.all_to_all(
        jnp.stack(placed, axis=1), "tile", split_axis=0, concat_axis=0, tiled=True
    )
    outbound = jnp.swapaxes(send_plan, 0, 1)
    target = jnp.where(outbound < 0, OWN, outbound).reshape(-1)
    sums = jax.ops.segment_sum(
        returned.reshape((-1, 2, PR, PW)), target, num_segments=OWN + 1
    )
    return sums[:OWN]


def body(dft, move, object_slices, probe_wave, intensities, send_list, cell_slot):
    owned = object_slices[0]
    send_plan = send_list[0]
    wanted = jnp.transpose(send_plan.reshape(MB, NY, NZ, NX, 2), (2, 1, 3, 0, 4))
    wanted = jnp.pad(wanted.reshape(NZ, 1, 64), ((0, 0), (0, 0), (0, 64)))
    wanted = jnp.broadcast_to(wanted, (NZ, 8, 128))
    windows, table, flag = fetch_windows(
        owned.reshape(OWN, CHUNKS, TALL, PW), wanted, cell_slot.reshape(1, MB * CELLS)
    )
    crowded = flag[0, 0] > 0
    windows = lax.cond(
        crowded,
        lambda: full_windows(owned, send_plan, cell_slot),
        lambda: windows,
    )
    gradients = position_gradients(windows, probe_wave, intensities, dft, move)
    sums = lax.cond(
        crowded,
        lambda: full_sums(gradients, send_plan, cell_slot),
        lambda: return_gradients(
            gradients.reshape(2, CELLS, CHUNKS, TALL, PW), table
        ).reshape(OWN, 2, PR, PW),
    )
    return sums[None]


def solution(mesh):
    dft, move = matrix_tables()
    in_specs = (
        P("section", "tile", None, None, None),
        P(),
        P("tile", None, None),
        P("tile", None, None, None),
        P("tile", None),
    )
    out_specs = P("section", "tile", None, None, None)
    step = functools.partial(body, jnp.asarray(dft), jnp.asarray(move))
    return jax.shard_map(step, mesh=mesh, in_specs=in_specs, out_specs=out_specs, check_vma=False)
```

```python
import functools

import jax
import jax.numpy as jnp
import ml_dtypes
import numpy as np
from jax import lax
from jax.experimental import pallas as pl
from jax.experimental.pallas import tpu as pltpu
from jax.sharding import PartitionSpec as P

W = 256
PW = 128
PR = 16
MB = 2
CELLS = 32
NX, NY, NZ = 4, 4, 8
PLANE = NX * NY
OWN = 32
COLUMN = NZ * OWN
PLACES = 32
ROWS = 4 * PLACES
CHUNKS = 8
TALL = 4
PHASE_SCALE = 20.0
MESH = pl.DeviceIdType.MESH
F32 = jnp.float32
I32 = jnp.int32
BF16 = jnp.bfloat16


FETCH = (
    ("s", 0, -1, 1),
    ("s", 0, 1, 1),
    ("s", 1, -1, 1),
    ("s", 1, 1, 1),
    ("s", 2, -1, 1),
    ("s", 2, 1, 1),
    ("s", 0, -1, 2),
    ("s", 0, 1, 2),
    ("s", 1, -1, 2),
    ("s", 1, 1, 2),
    ("s", 2, -1, 2),
    ("s", 2, 1, 2),
    ("s", 0, -1, 3),
    ("s", 0, 1, 3),
    ("s", 1, -1, 3),
    ("s", 1, 1, 3),
    ("s", 2, -1, 3),
    ("s", 2, 1, 3),
    ("s", 0, 1, 4),
    ("s", 3, -1, 1),
    ("s", 1, -1, 4),
    ("s", 3, 1, 1),
    ("s", 2, 1, 4),
    ("s", 4, -1, 1),
    ("s", 3, -1, 2),
    ("x", 0),
    ("s", 4, 1, 1),
    ("x", 1),
    ("s", 3, 1, 2),
    ("s", 5, -1, 1),
    ("s", 4, -1, 2),
    ("x", 2),
    ("s", 5, 1, 1),
    ("s", 3, -1, 3),
    ("s", 4, 1, 2),
    ("s", 5, -1, 2),
    ("s", 3, 1, 3),
    ("y", 0),
    ("s", 4, -1, 3),
    ("s", 5, 1, 2),
    ("s", 3, -1, 4),
    ("s", 4, 1, 3),
    ("y", 1),
    ("s", 5, -1, 3),
    ("s", 6, 1, 1),
    ("s", 5, 1, 3),
    ("y", 2),
    ("s", 6, -1, 1),
    ("x", 3),
    ("s", 4, 1, 4),
    ("s", 7, -1, 1),
    ("s", 5, -1, 4),
    ("s", 6, 1, 2),
    ("t", 0),
    ("s", 6, -1, 2),
    ("s", 7, 1, 1),
    ("x", 4),
    ("s", 7, -1, 2),
    ("y", 3),
    ("s", 6, 1, 3),
    ("x", 5),
    ("s", 7, 1, 2),
    ("s", 6, -1, 3),
    ("s", 7, -1, 3),
    ("s", 6, 1, 4),
    ("y", 4),
    ("s", 7, 1, 3),
    ("t", 1),
    ("s", 7, -1, 4),
    ("y", 5),
    ("x", 6),
    ("x", 7),
    ("t", 2),
    ("y", 6),
    ("y", 7),
    ("t", 3),
)
RETURN = (
    ("x", 0),
    ("x", 1),
    ("a", 0),
    ("x", 2),
    ("a", 1),
    ("x", 3),
    ("p", 0, -1, 2),
    ("p", 0, 1, 2),
    ("x", 4),
    ("a", 2),
    ("p", 1, -1, 2),
    ("p", 1, 1, 2),
    ("p", 0, -1, 3),
    ("p", 0, 1, 3),
    ("x", 5),
    ("a", 3),
    ("p", 2, -1, 2),
    ("p", 2, 1, 2),
    ("x", 6),
    ("a", 4),
    ("p", 1, -1, 3),
    ("p", 1, 1, 3),
    ("p", 0, 1, 4),
    ("x", 7),
    ("p", 3, -1, 2),
    ("p", 3, 1, 2),
    ("a", 5),
    ("p", 2, -1, 3),
    ("p", 2, 1, 3),
    ("p", 4, -1, 2),
    ("p", 4, 1, 2),
    ("a", 6),
    ("p", 1, -1, 4),
    ("p", 3, -1, 3),
    ("f", 0),
    ("a", 7),
    ("p", 3, 1, 3),
    ("p", 5, -1, 2),
    ("p", 5, 1, 2),
    ("p", 2, 1, 4),
    ("p", 4, -1, 3),
    ("p", 4, 1, 3),
    ("p", 6, -1, 2),
    ("p", 6, 1, 2),
    ("f", 1),
    ("p", 3, -1, 4),
    ("p", 7, 1, 2),
    ("p", 7, -1, 2),
    ("p", 5, -1, 3),
    ("p", 5, 1, 3),
    ("f", 2),
    ("p", 4, 1, 4),
    ("p", 6, -1, 3),
    ("p", 6, 1, 3),
    ("f", 3),
    ("p", 7, -1, 3),
    ("p", 7, 1, 3),
    ("p", 5, -1, 4),
    ("f", 4),
    ("p", 6, 1, 4),
    ("p", 7, -1, 4),
    ("f", 5),
    ("f", 6),
    ("f", 7),
)


def stacked_parts(matrix):
    rows = np.concatenate([matrix.real, matrix.imag], axis=0).astype(np.float32)
    high = rows.astype(ml_dtypes.bfloat16)
    low = (rows - high.astype(np.float32)).astype(ml_dtypes.bfloat16)
    return np.concatenate([high, low], axis=1)


def matrix_tables():
    index = np.arange(W)
    product = np.outer(index, index) % W
    dft = np.exp(-2j * np.pi * product / W) / np.sqrt(W)
    frequency = np.where(index < W // 2, index, index - W).astype(np.float64)
    diagonal = np.exp(-1j * PHASE_SCALE * frequency**2 / (W * W))
    move = np.conj(dft) @ (diagonal[:, None] * dft)
    move = (move + move.T) / 2
    return stacked_parts(dft), stacked_parts(move)


def place():
    tile = lax.axis_index("tile")
    core = lax.axis_index("section")
    y = tile // (NZ * NX)
    z = (tile // NX) % NZ
    x = tile % NX
    return core, y, z, x


def device(core, y, z, x):
    return (core, y * (NZ * NX) + z * NX + x)


def iota(shape, axis):
    return lax.broadcasted_iota(I32, shape, axis)


def to_column(row):
    n = row.shape[1]
    wide = jnp.broadcast_to(row, (n, n))
    return jnp.sum(jnp.where(iota((n, n), 0) == iota((n, n), 1), wide, 0.0), axis=1, keepdims=True)


def exclusive(column):
    rows = [jnp.zeros_like(column[0:1])]
    for step in range(column.shape[0] - 1):
        rows.append(rows[-1] + column[step : step + 1])
    return jnp.concatenate(rows, axis=0)


def send_to(src, dst, send_sem, recv_sem, target):
    return pltpu.make_async_remote_copy(
        src_ref=src,
        dst_ref=dst,
        send_sem=send_sem,
        recv_sem=recv_sem,
        device_id=target,
        device_id_type=MESH,
    )


def greet(barrier, targets):
    for target in targets:
        pl.semaphore_signal(barrier, inc=1, device_id=target, device_id_type=MESH)
    pl.semaphore_wait(barrier, len(targets))


def hops(chunk, direction):
    return 4 if (chunk % 2 == 0) == (direction > 0) else 3


def fill_rows(count, move):
    def some(part, carry):
        for k in range(8):
            move(part * 8 + k)
        return carry

    lax.fori_loop(0, count // 8, some, 0)


def fetch(
    obj,
    meta,
    cells,
    win,
    tab,
    flag,
    ag,
    metas,
    metain,
    tables,
    pick,
    turn,
    turned,
    slot,
    places,
    x_pack,
    x_recv,
    y_pack,
    y_recv,
    mark,
    marks_x,
    marks_y,
    marks_z,
    other,
    ag_send,
    ag_recv,
    meta_send,
    meta_recv,
    mark_send,
    mark_recv,
    x_send,
    x_sem,
    y_send,
    y_sem,
    pair_send,
    pair_recv,
    local_sem,
    loads,
):
    core, y, z, x = place()
    partner = device(1 - core, y, z, x)

    def ring_device(step):
        return device(core, y, (z + step) % NZ, x)

    def x_device(step):
        return device(core, y, z, (x + step) % NX)

    def y_device(step):
        return device(core, (y + step) % NY, z, x)

    greet(
        pltpu.get_barrier_semaphore(),
        [ring_device(step) for step in range(1, NZ)]
        + [x_device(step) for step in range(1, NX)]
        + [y_device(step) for step in range(1, NY)]
        + [partner],
    )

    def block(chunk, zz):
        return ag[chunk].at[pl.ds(((zz + 2 * NZ) % NZ) * OWN, OWN)]

    def ring_copy(chunk, direction, hop):
        side = 0 if direction > 0 else 1
        held = block(chunk, z - direction * (hop - 1))
        return send_to(
            obj.at[:, chunk] if hop == 1 else held,
            held,
            ag_send.at[chunk, side, hop - 1],
            ag_recv.at[chunk, side, hop - 1],
            ring_device(direction + NZ),
        )

    def ring_arrival(chunk, direction, hop):
        side = 0 if direction > 0 else 1
        held = block(chunk, z - direction * hop)
        send_to(
            held,
            held,
            ag_send.at[chunk, side, hop - 1],
            ag_recv.at[chunk, side, hop - 1],
            ring_device(direction + NZ),
        ).wait_recv()

    def ring_send(chunk, direction, hop):
        if hop > 1:
            ring_arrival(chunk, direction, hop - 1)
        ring_copy(chunk, direction, hop).start()

    first_wait = min(i for i, event in enumerate(FETCH) if event[0] != "s" or event[3] > 1)
    first_x = min(i for i, event in enumerate(FETCH) if event[0] == "x")
    first_y = min(i for i, event in enumerate(FETCH) if event[0] == "y")
    for event in FETCH[:first_wait]:
        ring_send(*event[1:])

    for load in loads:
        load.start()

    row = jnp.concatenate([cells[0:1, :], cells[1:2, :]], axis=1)
    owner = row >> 1
    entry = ((owner >> 2) & 7) * 4 + (iota(row.shape, 1) >> 5) * 2 + (row & 1)
    code_row = ((owner >> 5) * 128 + (owner & 3) * 32 + entry).astype(F32)
    y_row = (owner >> 5).astype(F32)
    code_col = to_column(code_row)
    y_col = to_column(y_row)
    ahead = (y_col == y_row) & (code_col < code_row)
    rank = jnp.sum(jnp.where(ahead, 1.0, 0.0), axis=0, keepdims=True)
    over = jnp.where(jnp.max(rank, axis=1, keepdims=True) >= PLACES, 1, 0)
    at = y_row * PLACES + jnp.minimum(rank, PLACES - 1.0)
    tables[0] = jnp.zeros((8, 128), I32)
    tables[0, 0:1, 0 : MB * CELLS] = at.astype(I32)
    at_col = to_column(jnp.where(rank < PLACES, at, -1.0))
    spread = jnp.broadcast_to(at_col, (MB * CELLS, ROWS)) == iota((MB * CELLS, ROWS), 1).astype(
        F32
    )
    number = iota((MB * CELLS, ROWS), 0).astype(F32)
    back_row = jnp.sum(jnp.where(spread, number, 0.0), axis=0, keepdims=True)

    metas[...] = jnp.concatenate(
        [meta[...], jnp.broadcast_to(over, (1, 128)), jnp.zeros((3, 128), I32)], axis=0
    )
    metain[z] = metas[...]

    def meta_copy(step):
        return send_to(
            metas,
            metain.at[z],
            meta_send.at[step],
            meta_recv.at[step],
            ring_device(step),
        )

    for step in range(1, NZ):
        meta_copy(step).start()

    last = 1 + PLACES // 8

    def table_copy(index, target):
        source = tab if index > last else tables.at[index]
        return pltpu.make_async_copy(source, target, local_sem.at[index])

    table_copy(0, slot).start()

    for chunk in range(CHUNKS):
        ag[chunk][pl.ds(z * OWN, OWN)] = obj[:, chunk]

    half_way = (first_wait + first_x) // 2
    for event in FETCH[first_wait:half_way]:
        ring_send(*event[1:])

    for step in range(1, NZ):
        meta_copy(step).wait()
    wanted = jnp.concatenate([metain[zz][0:4] for zz in range(NZ)], axis=0).astype(F32)
    lanes = iota((4 * NZ, 128), 1)
    valid = (wanted >= 0.0) & (((lanes >> 2) & 7) == z)
    held = jnp.where(valid, 1.0, 0.0)
    big_row, big_lane = iota((128, 128), 0), iota((128, 128), 1)
    one_x = (big_row & 31) == (big_lane & 31)
    column = jnp.where(one_x, 1.0, 0.0)
    above = jnp.where(one_x & ((big_row >> 5) < (big_lane >> 5)), 1.0, 0.0)
    earlier = jnp.where(iota((4 * NZ, 4 * NZ), 1) < iota((4 * NZ, 4 * NZ), 0), 1.0, 0.0)
    count = jnp.sum(held, axis=0, keepdims=True)
    sums = jnp.concatenate([count, jnp.zeros((7, 128), F32)], axis=0)
    start = jnp.dot(sums, above, preferred_element_type=F32)[0:1]
    whole = jnp.dot(sums, column, preferred_element_type=F32)[0:1]
    order = jnp.dot(earlier, held, preferred_element_type=F32) + start
    named = (iota((4 * NZ, 128), 0) >> 2).astype(F32) * OWN + wanted + 1.0
    picks = [
        jnp.sum(jnp.where(valid & (order == float(k)), named, 0.0), axis=0, keepdims=True)
        for k in range(PLACES)
    ]
    picks = jnp.dot(jnp.concatenate(picks, axis=0), column, preferred_element_type=F32)
    for part in range(PLACES // 8):
        tables[1 + part] = picks[part * 8 : part * 8 + 8].astype(I32)
        table_copy(1 + part, pick.at[part]).start()
    over_x = jnp.where(jnp.max(whole, axis=1, keepdims=True) > PLACES, 1.0, 0.0)
    over_z = jnp.max(
        jnp.max(metain[:, 4, :].astype(F32), axis=1, keepdims=True), axis=0, keepdims=True
    )
    over = jnp.broadcast_to(jnp.maximum(over_x, over_z), (1, 128))
    mark[0] = jnp.concatenate([count, start, over, jnp.zeros((5, 128), F32)], axis=0).astype(I32)
    marks_x[x] = mark[0]

    def mark_copy(kind, step):
        targets = (x_device, y_device, ring_device)
        arrays = (marks_x, marks_y, marks_z)
        own = (x, y, z)
        return send_to(
            mark.at[kind],
            arrays[kind].at[own[kind]],
            mark_send.at[kind, step],
            mark_recv.at[kind, step],
            targets[kind](step),
        )

    for step in range(1, NX):
        mark_copy(0, step).start()
    target = iota((128, ROWS), 1)
    chosen = jnp.where(iota((128, ROWS), 0) == (target // PLACES) + z * 4, 1.0, 0.0)
    chosen = jnp.dot(picks, chosen, preferred_element_type=F32)
    here = iota((PLACES, ROWS), 0) == iota((PLACES, ROWS), 1) % PLACES
    sums_row = jnp.sum(jnp.where(here, chosen, 0.0), axis=0, keepdims=True)
    tab[...] = jnp.zeros(tab.shape, I32)
    tab[0:1, :] = back_row.astype(I32)
    tab[1:2, :] = sums_row.astype(I32)

    table_copy(0, slot).wait()
    for part in range(PLACES // 8):
        table_copy(1 + part, pick.at[part]).wait()

    for event in FETCH[half_way:first_x]:
        ring_send(*event[1:])

    def x_copy(chunk, step):
        return send_to(
            x_pack.at[chunk, pl.ds(((x + step) % NX) * PLACES, PLACES)],
            x_recv[chunk].at[pl.ds(x * PLACES, PLACES)],
            x_send.at[chunk, step],
            x_sem.at[chunk, step],
            x_device(step),
        )

    def y_copy(chunk, step):
        return send_to(
            y_pack.at[chunk, pl.ds(((y + step) % NY) * PLACES, PLACES)],
            y_recv[chunk].at[pl.ds(y * PLACES, PLACES)],
            y_send.at[chunk, step],
            y_sem.at[chunk, step],
            y_device(step),
        )

    def along_x(chunk):
        for direction in (1, -1):
            ring_arrival(chunk, direction, hops(chunk, direction))

        def fill(part, carry):
            for k in range(8):
                for to in range(NX):
                    index = jnp.clip(pick[part, k, z * 4 + to], 1, COLUMN) - 1
                    x_pack[chunk, to * PLACES + part * 8 + k] = ag[chunk][index]
            return carry

        lax.fori_loop(0, PLACES // 8, fill, 0)
        for step in range(1, NX):
            x_copy(chunk, step).start()
        own = pl.ds(x * PLACES, PLACES)
        x_recv[chunk][own] = x_pack[chunk, own]

    def along_y(chunk):
        for step in range(1, NX):
            x_copy(chunk, step).wait_recv()

        def fill(part, carry):
            for k in range(8):
                for to in range(NY):
                    index = jnp.clip(turn[to, part * 8 + k], 1, ROWS) - 1
                    y_pack[chunk, to * PLACES + part * 8 + k] = x_recv[chunk][index]
            return carry

        lax.fori_loop(0, PLACES // 8, fill, 0)
        for step in range(1, NY):
            y_copy(chunk, step).start()
        own = pl.ds(y * PLACES, PLACES)
        y_recv[chunk][own] = y_pack[chunk, own]

    def pair_copy(part):
        return send_to(
            other.at[part],
            win.at[core, part],
            pair_send.at[part],
            pair_recv.at[part],
            partner,
        )

    def take(quarter):
        low, high = 2 * quarter, 2 * quarter + 1
        for chunk in (low, high):
            for step in range(1, NY):
                y_copy(chunk, step).wait_recv()
        part, half = quarter // 2, quarter % 2

        def both(index):
            index = jnp.clip(index, 0, ROWS - 1)
            return jnp.concatenate([y_recv[low][index], y_recv[high][index]], axis=0)

        def lay(r, carry):
            first = pl.multiple_of(r * PR + half * 8, 8)
            for side in range(2):
                k = r * 2 + side
                lanes_of = slice(side * PW, side * PW + PW)
                win[core, part, pl.ds(first, 8), lanes_of] = both(slot[0, core * CELLS + k])
                other[part, pl.ds(first, 8), lanes_of] = both(slot[0, (1 - core) * CELLS + k])
            return carry

        lax.fori_loop(0, W // PR, lay, 0)

    def run(events):
        for event in events:
            if event[0] == "s":
                ring_send(*event[1:])
            elif event[0] == "x":
                along_x(event[1])
            elif event[0] == "y":
                along_y(event[1])
            else:
                take(event[1])
                if event[1] % 2 == 1:
                    pair_copy(event[1] // 2).start()

    run(FETCH[first_x:first_y])

    for step in range(1, NX):
        mark_copy(0, step).wait()
    counts = marks_x[:, 0, :].astype(F32)
    starts = marks_x[:, 1, :].astype(F32)
    four = iota((NX, 128), 1)
    wide = four.astype(F32)
    giver = iota((NX, 128), 0).astype(F32)
    onward = []
    back = jnp.zeros((NX, 128), F32)
    for to in range(NY):
        mine = four == to * 32 + z * 4 + x
        many = jnp.sum(jnp.where(mine, counts, 0.0), axis=1, keepdims=True)
        low = jnp.sum(jnp.where(mine, starts, 0.0), axis=1, keepdims=True)
        first = exclusive(many)
        inside = (wide >= first) & (wide < first + many)
        onward.append(
            jnp.sum(
                jnp.where(inside, giver * PLACES + low + wide - first + 1.0, 0.0),
                axis=0,
                keepdims=True,
            )
        )
        inside = (wide >= low) & (wide < low + many)
        back = back + jnp.where(inside, to * PLACES + first + wide - low + 1.0, 0.0)
    tables[last] = jnp.concatenate(onward + [jnp.zeros((4, 128), F32)], axis=0).astype(I32)
    table_copy(last, turn).start()
    tab[8:12, :] = back.astype(I32)
    table_copy(last + 1, places).start()
    mark[1] = jnp.broadcast_to(
        jnp.max(marks_x[:, 2, :].astype(F32), axis=0, keepdims=True), (8, 128)
    ).astype(I32)
    marks_y[y] = mark[1]
    for step in range(1, NY):
        mark_copy(1, step).start()
    table_copy(last, turn).wait()
    table_copy(last + 1, places).wait()

    next_y = [i for i, event in enumerate(FETCH) if event[0] == "y"]
    run(FETCH[first_y : next_y[2]])
    for step in range(1, NY):
        mark_copy(1, step).wait()
    mark[2] = jnp.max(marks_y[...].astype(F32), axis=0).astype(I32)
    marks_z[z] = mark[2]
    for step in range(1, NZ):
        mark_copy(2, step).start()
    run(FETCH[next_y[2] : next_y[5]])
    for step in range(1, NZ):
        mark_copy(2, step).wait()
    mark[0] = jnp.max(marks_z[...].astype(F32), axis=0).astype(I32)
    crowded = pltpu.make_async_copy(mark.at[0], turned, local_sem.at[0])
    crowded.start()
    run(FETCH[next_y[5] :])
    for chunk in range(CHUNKS):
        for direction in (1, -1):
            for hop in range(1, hops(chunk, direction) + 1):
                ring_copy(chunk, direction, hop).wait_send()
        for step in range(1, NX):
            x_copy(chunk, step).wait_send()
            y_copy(chunk, step).wait_send()
    crowded.wait()
    flag[0, 0] = turned[0, 0]
    pair_copy(0).wait()
    pair_copy(1).wait()


def parts(value):
    high = value.astype(BF16)
    return high, (value - high.astype(F32)).astype(BF16)


def from_left(real, imag, table, sign):
    high, low = parts(jnp.concatenate([real, imag], axis=1))
    out = jnp.dot(
        table[...], jnp.concatenate([high, high], axis=0), preferred_element_type=F32
    ) + jnp.dot(table[:, :W], low, preferred_element_type=F32)
    return out[:W, :W] - sign * out[W:, W:], out[:W, W:] + sign * out[W:, :W]


def from_right(real, imag, table, sign):
    high, low = parts(jnp.concatenate([real, imag], axis=0))
    across = (((1,), (1,)), ((), ()))
    out = lax.dot_general(
        jnp.concatenate([high, high], axis=1), table[...], across, preferred_element_type=F32
    ) + lax.dot_general(low, table[:, :W], across, preferred_element_type=F32)
    return out[:W, :W] - sign * out[W:, W:], sign * out[:W, W:] + out[W:, :W]


def both_sides(real, imag, table, sign):
    real, imag = from_left(real, imag, table, sign)
    return from_right(real, imag, table, sign)


def position(win, probe, measured, dft, move, lay):
    pr, pi = probe[0], probe[1]
    ar, ai = win[0, 0], win[0, 1]
    wave_r, wave_i = both_sides(pr * ar - pi * ai, pr * ai + pi * ar, move, 1.0)
    br, bi = win[1, 0], win[1, 1]
    far_r, far_i = both_sides(
        wave_r * br - wave_i * bi, wave_r * bi + wave_i * br, dft, 1.0
    )
    gap = far_r * far_r + far_i * far_i - measured[...]
    back_r, back_i = both_sides(gap * far_r, gap * far_i, dft, -1.0)
    lay(1, wave_r * back_r + wave_i * back_i, wave_r * back_i - wave_i * back_r)
    br, bi = win[1, 0], win[1, 1]
    low_r, low_i = both_sides(
        br * back_r + bi * back_i, br * back_i - bi * back_r, move, -1.0
    )
    pr, pi = probe[0], probe[1]
    lay(0, pr * low_r + pi * low_i, pr * low_i - pi * low_r)


def lay_cells(grad):
    def lay(index, real, imag):
        for k in range(CELLS):
            rows = slice(k // 2 * PR, k // 2 * PR + PR)
            lanes = slice(k % 2 * PW, k % 2 * PW + PW)
            for part, value in enumerate((real, imag)):
                value = value[rows, lanes]
                for strip in range(4):
                    grad[index, k, part * 4 + strip] = value[strip * TALL : strip * TALL + TALL]

    return lay


def position_kernel(win, probe, measured, dft, move, grad):
    core = lax.axis_index("section")
    position(win, probe, measured.at[core], dft, move, lay_cells(grad))


def position_gradients(windows, probe_wave, intensities, dft, move):
    vmem = pl.BlockSpec(memory_space=pltpu.VMEM)
    return pl.pallas_call(
        position_kernel,
        out_shape=jax.ShapeDtypeStruct((2, CELLS, CHUNKS, TALL, PW), F32),
        in_specs=[vmem] * 5,
        out_specs=vmem,
        name="position_gradients",
    )(windows, probe_wave, intensities, dft, move)


def give_back(
    grad,
    places,
    tab,
    out,
    cells,
    y_pack,
    y_recv,
    x_pack,
    x_recv,
    total,
    ring,
    mix,
    pair_send,
    pair_recv,
    y_send,
    y_sem,
    x_send,
    x_sem,
    rs_send,
    rs_recv,
):
    core, y, z, x = place()
    partner = device(1 - core, y, z, x)

    def ring_device(step):
        return device(core, y, (z + step) % NZ, x)

    def x_device(step):
        return device(core, y, z, (x + step) % NX)

    def y_device(step):
        return device(core, (y + step) % NY, z, x)

    def pair_copy(chunk):
        return send_to(
            grad.at[1 - core, :, chunk],
            cells[chunk].at[pl.ds(core * CELLS, CELLS)],
            pair_send.at[chunk],
            pair_recv.at[chunk],
            partner,
        )

    for chunk in range(CHUNKS):
        cells[chunk][pl.ds(core * CELLS, CELLS)] = grad[core, :, chunk]
    for chunk in range(CHUNKS):
        pair_copy(chunk).start()

    mix[...] = jnp.where(
        jnp.broadcast_to(tab[1:2, :], (COLUMN, ROWS)) == iota((COLUMN, ROWS), 0) + 1, 1.0, 0.0
    ).astype(BF16)

    def y_copy(chunk, step):
        return send_to(
            y_pack.at[chunk, pl.ds(((y + step) % NY) * PLACES, PLACES)],
            y_recv[chunk].at[pl.ds(y * PLACES, PLACES)],
            y_send.at[chunk, step],
            y_sem.at[chunk, step],
            y_device(step),
        )

    def x_copy(chunk, step):
        return send_to(
            x_pack.at[chunk, pl.ds(((x + step) % NX) * (PLACES * TALL), PLACES * TALL)],
            x_recv.at[chunk, pl.ds(x * (PLACES * TALL), PLACES * TALL)],
            x_send.at[chunk, step],
            x_sem.at[chunk, step],
            x_device(step),
        )

    for chunk in range(CHUNKS):
        pair_copy(chunk).wait_recv()

        def fill_y(row):
            index = jnp.clip(places[0, row], 0, MB * CELLS - 1)
            y_pack[chunk, row] = cells[chunk][index]

        fill_rows(ROWS, fill_y)
        for step in range(1, NY):
            y_copy(chunk, step).start()
        own = pl.ds(y * PLACES, PLACES)
        y_recv[chunk][own] = y_pack[chunk, own]

    def along_x(chunk):
        for step in range(1, NY):
            y_copy(chunk, step).wait_recv()

        def fill_x(pair):
            to, k = pair // (PLACES // 2), pair % (PLACES // 2) * 2
            two = [jnp.clip(places[8 + to, k + i], 1, ROWS) - 1 for i in range(2)]
            spot = pl.ds(pl.multiple_of(pair * 2 * TALL, 8), 2 * TALL)
            x_pack[chunk, spot] = jnp.concatenate([y_recv[chunk][i] for i in two], axis=0)

        fill_rows(ROWS // 2, fill_x)
        for step in range(1, NX):
            x_copy(chunk, step).start()
        own = pl.ds(x * (PLACES * TALL), PLACES * TALL)
        x_recv[chunk, own] = x_pack[chunk, own]

    def block(zz):
        return pl.ds(((zz + 2 * NZ) % NZ) * (OWN * TALL), OWN * TALL)

    def ring_copy(chunk, direction, step):
        side = 0 if direction > 0 else 1
        reach = hops(chunk, direction)
        return send_to(
            total.at[chunk, block(z + direction * reach)]
            if step == 1
            else ring.at[chunk, side, step - 2],
            ring.at[chunk, side, step - 1],
            rs_send.at[chunk, side, step - 1],
            rs_recv.at[chunk, side, step - 1],
            ring_device(direction + NZ),
        )

    def sum_cells(chunk):
        for step in range(1, NX):
            x_copy(chunk, step).wait_recv()

        def add(r, carry):
            high, low = parts(x_recv[chunk, pl.ds(r, ROWS, stride=TALL), :])
            both = jnp.dot(
                mix[...], jnp.concatenate([high, low], axis=1), preferred_element_type=F32
            )
            total[chunk, pl.ds(r, COLUMN, stride=TALL), :] = both[:, :128] + both[:, 128:]
            return carry

        lax.fori_loop(0, TALL, add, 0)
        for direction in (1, -1):
            ring_copy(chunk, direction, 1).start()

    def pass_on(chunk, direction, step):
        reach = hops(chunk, direction)
        side = 0 if direction > 0 else 1
        ring_copy(chunk, direction, step - 1).wait_recv()
        ring[chunk, side, step - 2] += total[chunk, block(z + direction * (reach - step + 1))]
        ring_copy(chunk, direction, step).start()

    def last(chunk):
        value = total[chunk, block(z)]
        for direction in (1, -1):
            reach = hops(chunk, direction)
            side = 0 if direction > 0 else 1
            ring_copy(chunk, direction, reach).wait_recv()
            value = value + ring[chunk, side, reach - 1]
        return value

    def finish(quarter):
        low, high = last(2 * quarter), last(2 * quarter + 1)
        for p in range(OWN):
            rows = slice(p * TALL, p * TALL + TALL)
            spot = p * CHUNKS * TALL + quarter * 8
            out[spot : spot + 8] = jnp.concatenate([low[rows], high[rows]], axis=0)

    ended = set()
    for event in RETURN:
        if event[0] == "x":
            along_x(event[1])
        elif event[0] == "a":
            sum_cells(event[1])
        elif event[0] == "p":
            pass_on(*event[1:])
        else:
            ended.add(event[1])
            if event[1] ^ 1 in ended:
                finish(event[1] // 2)

    for chunk in range(CHUNKS):
        pair_copy(chunk).wait_send()
        for direction in (1, -1):
            for step in range(1, hops(chunk, direction) + 1):
                ring_copy(chunk, direction, step).wait_send()
        for step in range(1, NX):
            x_copy(chunk, step).wait_send()
            y_copy(chunk, step).wait_send()


def whole_kernel(obj, meta, cells, probe, measured, dft, move, out, flag, *scratch):
    fetching, giving, (grad, probe_in, measured_in, dft_in, move_in, load_sem) = scratch
    win, tab, places = fetching["win"], fetching["tab"], fetching["places"]
    core = lax.axis_index("section")
    loads = [
        pltpu.make_async_copy(source, target, load_sem.at[index])
        for index, (source, target) in enumerate(
            (
                (probe, probe_in),
                (measured.at[core], measured_in),
                (dft, dft_in),
                (move, move_in),
            )
        )
    ]
    fetch(obj, meta, cells, flag=flag, loads=loads, **fetching)
    for load in loads:
        load.wait()
    position(win, probe_in, measured_in, dft_in, move_in, lay_cells(grad))
    del win
    give_back(grad, places, tab, out, **giving)


def object_sums(owned, meta, cells, probe_wave, intensities, dft, move):
    vmem = pl.BlockSpec(memory_space=pltpu.VMEM)
    anywhere = pl.BlockSpec(memory_space=pltpu.HBM)
    tile, strip = (8, PW), (TALL, PW)
    dma = pltpu.SemaphoreType.DMA
    many, one = pltpu.VMEM((CHUNKS, ROWS) + strip, F32), pltpu.VMEM((ROWS,) + strip, F32)
    fetching = dict(
        win=pltpu.VMEM((2, 2, W, W), F32),
        tab=pltpu.VMEM((16, 128), I32),
        ag=[pltpu.VMEM((COLUMN,) + strip, F32)] * CHUNKS,
        metas=pltpu.VMEM(tile, I32),
        metain=pltpu.VMEM((NZ,) + tile, I32),
        tables=pltpu.VMEM((2 + PLACES // 8,) + tile, I32),
        pick=pltpu.SMEM((PLACES // 8,) + tile, I32),
        turn=pltpu.SMEM(tile, I32),
        turned=pltpu.SMEM(tile, I32),
        slot=pltpu.SMEM(tile, I32),
        places=pltpu.SMEM((16, 128), I32),
        x_pack=many,
        x_recv=[one] * CHUNKS,
        y_pack=many,
        y_recv=[one] * CHUNKS,
        mark=pltpu.VMEM((3,) + tile, I32),
        marks_x=pltpu.VMEM((NX,) + tile, I32),
        marks_y=pltpu.VMEM((NY,) + tile, I32),
        marks_z=pltpu.VMEM((NZ,) + tile, I32),
        other=pltpu.VMEM((2, W, W), F32),
        ag_send=dma((CHUNKS, 2, 4)),
        ag_recv=dma((CHUNKS, 2, 4)),
        meta_send=dma((NZ,)),
        meta_recv=dma((NZ,)),
        mark_send=dma((3, NZ)),
        mark_recv=dma((3, NZ)),
        x_send=dma((CHUNKS, NX)),
        x_sem=dma((CHUNKS, NX)),
        y_send=dma((CHUNKS, NY)),
        y_sem=dma((CHUNKS, NY)),
        pair_send=dma((2,)),
        pair_recv=dma((2,)),
        local_sem=dma((3 + PLACES // 8,)),
    )
    giving = dict(
        cells=[pltpu.VMEM((MB * CELLS,) + strip, F32)] * CHUNKS,
        y_pack=many,
        y_recv=[one] * CHUNKS,
        x_pack=pltpu.VMEM((CHUNKS, ROWS * TALL, PW), F32),
        x_recv=pltpu.VMEM((CHUNKS, ROWS * TALL, PW), F32),
        total=pltpu.VMEM((CHUNKS, COLUMN * TALL, PW), F32),
        ring=pltpu.VMEM((CHUNKS, 2, 4, OWN * TALL, PW), F32),
        mix=pltpu.VMEM((COLUMN, ROWS), BF16),
        pair_send=dma((CHUNKS,)),
        pair_recv=dma((CHUNKS,)),
        y_send=dma((CHUNKS, NY)),
        y_sem=dma((CHUNKS, NY)),
        x_send=dma((CHUNKS, NX)),
        x_sem=dma((CHUNKS, NX)),
        rs_send=dma((CHUNKS, 2, 4)),
        rs_recv=dma((CHUNKS, 2, 4)),
    )
    rest = [
        pltpu.VMEM((2, CELLS, CHUNKS) + strip, F32),
        pltpu.VMEM((2, W, W), F32),
        pltpu.VMEM((W, W), F32),
        pltpu.VMEM((2 * W, 2 * W), BF16),
        pltpu.VMEM((2 * W, 2 * W), BF16),
        dma((4,)),
    ]
    return pl.pallas_call(
        whole_kernel,
        out_shape=(
            jax.ShapeDtypeStruct((OWN * CHUNKS * TALL, PW), F32),
            jax.ShapeDtypeStruct((1, 1), I32),
        ),
        in_specs=[vmem] * 3 + [anywhere] * 4,
        out_specs=(vmem, pl.BlockSpec(memory_space=pltpu.SMEM)),
        scratch_shapes=[fetching, giving, rest],
        compiler_params=pltpu.CompilerParams(
            collective_id=0, has_side_effects=True, vmem_limit_bytes=46 << 20
        ),
        name="object_sums",
    )(owned, meta, cells, probe_wave, intensities, dft, move)


def swapped(block):
    return lax.ppermute(block, "section", [(0, 1), (1, 0)])


def place_in_all(cell_slot):
    batch = iota(cell_slot.shape, 0)
    return ((cell_slot >> 1) * (2 * MB) + batch * 2 + (cell_slot & 1)).reshape(-1)


def full_windows(owned, send_plan, cell_slot):
    core = lax.axis_index("section")
    outbound = jnp.swapaxes(send_plan, 0, 1)
    patches = owned[jnp.maximum(outbound, 0)]
    arrived = lax.all_to_all(patches, "tile", split_axis=0, concat_axis=0, tiled=True)
    picked = arrived.reshape((-1, 2, PR, PW))[place_in_all(cell_slot)]
    picked = picked.reshape(MB, W // PR, W // PW, 2, PR, PW)
    windows = jnp.transpose(picked, (0, 3, 1, 4, 2, 5)).reshape(MB, 2, W, W)
    passed = swapped(lax.dynamic_index_in_dim(windows, 1 - core, 0, keepdims=False))
    kept = lax.dynamic_index_in_dim(windows, core, 0, keepdims=False)
    first = core == 0
    return jnp.stack([jnp.where(first, kept, passed), jnp.where(first, passed, kept)])


def full_sums(gradients, send_plan, cell_slot):
    core = lax.axis_index("section")
    passed = swapped(lax.dynamic_index_in_dim(gradients, 1 - core, 0, keepdims=False))
    kept = lax.dynamic_index_in_dim(gradients, core, 0, keepdims=False)
    first = core == 0
    batches = jnp.stack([jnp.where(first, kept, passed), jnp.where(first, passed, kept)])
    owners = NX * NY * NZ
    placed = (
        jnp.zeros((owners * MB * 2, 2, PR, PW), F32)
        .at[place_in_all(cell_slot)]
        .set(batches.reshape(-1, 2, PR, PW))
    )
    returned = lax.all_to_all(
        placed.reshape(owners, MB, 2, 2, PR, PW), "tile", split_axis=0, concat_axis=0, tiled=True
    )
    outbound = jnp.swapaxes(send_plan, 0, 1)
    target = jnp.where(outbound < 0, OWN, outbound).reshape(-1)
    sums = jax.ops.segment_sum(
        returned.reshape((-1, 2, PR, PW)), target, num_segments=OWN + 1
    )
    return sums[:OWN]


def body(dft, move, object_slices, probe_wave, intensities, send_list, cell_slot):
    owned = object_slices[0]
    send_plan = send_list[0]
    meta = jnp.transpose(send_plan, (0, 2, 1)).reshape(MB * 2, NX * NY * NZ)
    meta = lax.optimization_barrier(meta)
    sums, flag = object_sums(
        owned.reshape(OWN, CHUNKS, TALL, PW),
        meta,
        cell_slot,
        probe_wave,
        intensities,
        dft,
        move,
    )

    def full():
        plan = jnp.transpose(meta.reshape(MB, 2, NX * NY * NZ), (0, 2, 1))
        windows = full_windows(owned, plan, cell_slot)
        gradients = position_gradients(windows, probe_wave, intensities, dft, move)
        return full_sums(gradients.reshape(2, CELLS, 2, PR, PW), plan, cell_slot)

    sums = lax.cond(flag[0, 0] > 0, full, lambda: sums.reshape(OWN, 2, PR, PW))
    return sums[None]


def solution(mesh):
    dft, move = matrix_tables()
    in_specs = (
        P("section", "tile", None, None, None),
        P(),
        P("tile", None, None),
        P("tile", None, None, None),
        P("tile", None),
    )
    out_specs = P("section", "tile", None, None, None)
    step = functools.partial(body, jnp.asarray(dft), jnp.asarray(move))
    return jax.shard_map(step, mesh=mesh, in_specs=in_specs, out_specs=out_specs, check_vma=False)
```

```python
import functools

import jax
import jax.numpy as jnp
import ml_dtypes
import numpy as np
from jax import lax
from jax.experimental import pallas as pl
from jax.experimental.pallas import tpu as pltpu
from jax.sharding import PartitionSpec as P

W = 256
PW = 128
PR = 16
MB = 2
CELLS = 32
NX, NY, NZ = 4, 4, 8
PLANE = NX * NY
OWN = 32
COLUMN = NZ * OWN
PLACES = 32
ROWS = 4 * PLACES
CHUNKS = 8
TALL = 4
PHASE_SCALE = 20.0
MESH = pl.DeviceIdType.MESH
F32 = jnp.float32
I32 = jnp.int32
BF16 = jnp.bfloat16


FETCH = (
    ("s", 0, -1, 1),
    ("s", 0, 1, 1),
    ("s", 1, -1, 1),
    ("s", 1, 1, 1),
    ("s", 2, -1, 1),
    ("s", 2, 1, 1),
    ("s", 3, -1, 1),
    ("s", 3, 1, 1),
    ("s", 4, -1, 1),
    ("s", 4, 1, 1),
    ("s", 0, -1, 2),
    ("s", 0, 1, 2),
    ("s", 1, -1, 2),
    ("s", 1, 1, 2),
    ("s", 2, -1, 2),
    ("s", 2, 1, 2),
    ("s", 3, -1, 2),
    ("s", 3, 1, 2),
    ("s", 4, -1, 2),
    ("s", 4, 1, 2),
    ("s", 0, -1, 3),
    ("s", 0, 1, 3),
    ("s", 1, -1, 3),
    ("s", 1, 1, 3),
    ("s", 2, -1, 3),
    ("s", 2, 1, 3),
    ("s", 3, -1, 3),
    ("s", 3, 1, 3),
    ("s", 4, -1, 3),
    ("s", 4, 1, 3),
    ("s", 0, 1, 4),
    ("s", 5, -1, 1),
    ("s", 1, -1, 4),
    ("s", 5, 1, 1),
    ("s", 2, 1, 4),
    ("s", 6, -1, 1),
    ("s", 3, -1, 4),
    ("s", 6, 1, 1),
    ("s", 4, 1, 4),
    ("s", 7, -1, 1),
    ("s", 5, -1, 2),
    ("x", 0),
    ("s", 7, 1, 1),
    ("x", 1),
    ("s", 5, 1, 2),
    ("s", 6, -1, 2),
    ("x", 2),
    ("x", 3),
    ("s", 6, 1, 2),
    ("s", 7, -1, 2),
    ("x", 4),
    ("y", 0),
    ("s", 5, -1, 3),
    ("s", 7, 1, 2),
    ("s", 6, -1, 3),
    ("s", 5, 1, 3),
    ("y", 1),
    ("s", 6, 1, 3),
    ("s", 7, -1, 3),
    ("s", 5, -1, 4),
    ("s", 7, 1, 3),
    ("y", 2),
    ("s", 6, 1, 4),
    ("s", 7, -1, 4),
    ("y", 3),
    ("t", 0),
    ("x", 5),
    ("y", 4),
    ("x", 6),
    ("x", 7),
    ("t", 1),
    ("y", 5),
    ("y", 6),
    ("y", 7),
    ("t", 2),
    ("t", 3),
)
RETURN = (
    ("x", 0),
    ("x", 1),
    ("x", 2),
    ("a", 0),
    ("x", 3),
    ("a", 1),
    ("x", 4),
    ("p", 0, -1, 2),
    ("p", 0, 1, 2),
    ("a", 2),
    ("x", 5),
    ("p", 1, -1, 2),
    ("p", 1, 1, 2),
    ("a", 3),
    ("p", 0, -1, 3),
    ("p", 0, 1, 3),
    ("x", 6),
    ("a", 4),
    ("p", 2, -1, 2),
    ("p", 2, 1, 2),
    ("p", 1, -1, 3),
    ("p", 1, 1, 3),
    ("x", 7),
    ("a", 5),
    ("p", 3, -1, 2),
    ("p", 3, 1, 2),
    ("p", 0, 1, 4),
    ("p", 4, -1, 2),
    ("p", 4, 1, 2),
    ("a", 6),
    ("p", 2, -1, 3),
    ("p", 2, 1, 3),
    ("p", 1, -1, 4),
    ("a", 7),
    ("p", 5, -1, 2),
    ("p", 5, 1, 2),
    ("p", 3, -1, 3),
    ("p", 3, 1, 3),
    ("p", 4, -1, 3),
    ("f", 0),
    ("p", 6, -1, 2),
    ("p", 4, 1, 3),
    ("p", 6, 1, 2),
    ("f", 1),
    ("p", 2, 1, 4),
    ("p", 7, -1, 2),
    ("p", 7, 1, 2),
    ("p", 5, -1, 3),
    ("p", 5, 1, 3),
    ("p", 3, -1, 4),
    ("p", 4, 1, 4),
    ("p", 6, -1, 3),
    ("p", 6, 1, 3),
    ("p", 7, -1, 3),
    ("f", 2),
    ("p", 5, -1, 4),
    ("p", 7, 1, 3),
    ("f", 3),
    ("f", 4),
    ("p", 7, -1, 4),
    ("p", 6, 1, 4),
    ("f", 5),
    ("f", 7),
    ("f", 6),
)


def stacked_parts(matrix):
    rows = np.concatenate([matrix.real, matrix.imag], axis=0).astype(np.float32)
    high = rows.astype(ml_dtypes.bfloat16)
    low = (rows - high.astype(np.float32)).astype(ml_dtypes.bfloat16)
    return np.concatenate([high, low], axis=1)


def matrix_tables():
    index = np.arange(W)
    product = np.outer(index, index) % W
    dft = np.exp(-2j * np.pi * product / W) / np.sqrt(W)
    frequency = np.where(index < W // 2, index, index - W).astype(np.float64)
    diagonal = np.exp(-1j * PHASE_SCALE * frequency**2 / (W * W))
    move = np.conj(dft) @ (diagonal[:, None] * dft)
    move = (move + move.T) / 2
    return stacked_parts(dft), stacked_parts(move)


def place():
    tile = lax.axis_index("tile")
    core = lax.axis_index("section")
    y = tile // (NZ * NX)
    z = (tile // NX) % NZ
    x = tile % NX
    return core, y, z, x


def device(core, y, z, x):
    return (core, y * (NZ * NX) + z * NX + x)


def iota(shape, axis):
    return lax.broadcasted_iota(I32, shape, axis)


def to_column(row):
    n = row.shape[1]
    wide = jnp.broadcast_to(row, (n, n))
    return jnp.sum(jnp.where(iota((n, n), 0) == iota((n, n), 1), wide, 0.0), axis=1, keepdims=True)


def exclusive(column):
    rows = [jnp.zeros_like(column[0:1])]
    for step in range(column.shape[0] - 1):
        rows.append(rows[-1] + column[step : step + 1])
    return jnp.concatenate(rows, axis=0)


def send_to(src, dst, send_sem, recv_sem, target):
    return pltpu.make_async_remote_copy(
        src_ref=src,
        dst_ref=dst,
        send_sem=send_sem,
        recv_sem=recv_sem,
        device_id=target,
        device_id_type=MESH,
    )


def greet(barrier, targets):
    for target in targets:
        pl.semaphore_signal(barrier, inc=1, device_id=target, device_id_type=MESH)
    pl.semaphore_wait(barrier, len(targets))


def hops(chunk, direction):
    return 4 if (chunk % 2 == 0) == (direction > 0) else 3


def fill_rows(count, move):
    def some(part, carry):
        for k in range(8):
            move(part * 8 + k)
        return carry

    lax.fori_loop(0, count // 8, some, 0)


def fetch(
    obj,
    meta,
    cells,
    win,
    tab,
    flag,
    ag,
    metas,
    metain,
    tables,
    pick,
    turn,
    turned,
    slot,
    places,
    x_pack,
    x_recv,
    y_pack,
    y_recv,
    mark,
    marks_x,
    marks_y,
    marks_z,
    other,
    ag_send,
    ag_recv,
    meta_send,
    meta_recv,
    mark_send,
    mark_recv,
    x_send,
    x_sem,
    y_send,
    y_sem,
    pair_send,
    pair_recv,
    local_sem,
    loads,
):
    core, y, z, x = place()
    partner = device(1 - core, y, z, x)

    def ring_device(step):
        return device(core, y, (z + step) % NZ, x)

    def x_device(step):
        return device(core, y, z, (x + step) % NX)

    def y_device(step):
        return device(core, (y + step) % NY, z, x)

    greet(
        pltpu.get_barrier_semaphore(),
        [ring_device(step) for step in range(1, NZ)]
        + [x_device(step) for step in range(1, NX)]
        + [y_device(step) for step in range(1, NY)]
        + [partner],
    )

    def block(chunk, zz):
        return ag[chunk].at[pl.ds(((zz + 2 * NZ) % NZ) * OWN, OWN)]

    def ring_copy(chunk, direction, hop):
        side = 0 if direction > 0 else 1
        held = block(chunk, z - direction * (hop - 1))
        return send_to(
            obj.at[:, chunk] if hop == 1 else held,
            held,
            ag_send.at[chunk, side, hop - 1],
            ag_recv.at[chunk, side, hop - 1],
            ring_device(direction + NZ),
        )

    def ring_arrival(chunk, direction, hop):
        side = 0 if direction > 0 else 1
        held = block(chunk, z - direction * hop)
        send_to(
            held,
            held,
            ag_send.at[chunk, side, hop - 1],
            ag_recv.at[chunk, side, hop - 1],
            ring_device(direction + NZ),
        ).wait_recv()

    def ring_send(chunk, direction, hop):
        if hop > 1:
            ring_arrival(chunk, direction, hop - 1)
        ring_copy(chunk, direction, hop).start()

    first_wait = min(i for i, event in enumerate(FETCH) if event[0] != "s" or event[3] > 1)
    first_x = min(i for i, event in enumerate(FETCH) if event[0] == "x")
    first_y = min(i for i, event in enumerate(FETCH) if event[0] == "y")
    for event in FETCH[:first_wait]:
        ring_send(*event[1:])

    for load in loads:
        load.start()

    row = jnp.concatenate([cells[0:1, :], cells[1:2, :]], axis=1)
    owner = row >> 1
    entry = ((owner >> 2) & 7) * 4 + (iota(row.shape, 1) >> 5) * 2 + (row & 1)
    code_row = ((owner >> 5) * 128 + (owner & 3) * 32 + entry).astype(F32)
    y_row = (owner >> 5).astype(F32)
    code_col = to_column(code_row)
    y_col = to_column(y_row)
    ahead = (y_col == y_row) & (code_col < code_row)
    rank = jnp.sum(jnp.where(ahead, 1.0, 0.0), axis=0, keepdims=True)
    over = jnp.where(jnp.max(rank, axis=1, keepdims=True) >= PLACES, 1, 0)
    at = y_row * PLACES + jnp.minimum(rank, PLACES - 1.0)
    tables[0] = jnp.zeros((8, 128), I32)
    tables[0, 0:1, 0 : MB * CELLS] = at.astype(I32)
    at_col = to_column(jnp.where(rank < PLACES, at, -1.0))
    spread = jnp.broadcast_to(at_col, (MB * CELLS, ROWS)) == iota((MB * CELLS, ROWS), 1).astype(
        F32
    )
    number = iota((MB * CELLS, ROWS), 0).astype(F32)
    back_row = jnp.sum(jnp.where(spread, number, 0.0), axis=0, keepdims=True)

    metas[...] = jnp.concatenate(
        [meta[...], jnp.broadcast_to(over, (1, 128)), jnp.zeros((3, 128), I32)], axis=0
    )
    metain[z] = metas[...]

    def meta_copy(step):
        return send_to(
            metas,
            metain.at[z],
            meta_send.at[step],
            meta_recv.at[step],
            ring_device(step),
        )

    for step in range(1, NZ):
        meta_copy(step).start()

    last = 1 + PLACES // 8

    def table_copy(index, target):
        source = tab if index > last else tables.at[index]
        return pltpu.make_async_copy(source, target, local_sem.at[index])

    table_copy(0, slot).start()

    for chunk in range(CHUNKS):
        ag[chunk][pl.ds(z * OWN, OWN)] = obj[:, chunk]

    half_way = (first_wait + first_x) // 2
    for event in FETCH[first_wait:half_way]:
        ring_send(*event[1:])

    for step in range(1, NZ):
        meta_copy(step).wait()
    wanted = jnp.concatenate([metain[zz][0:4] for zz in range(NZ)], axis=0).astype(F32)
    lanes = iota((4 * NZ, 128), 1)
    valid = (wanted >= 0.0) & (((lanes >> 2) & 7) == z)
    held = jnp.where(valid, 1.0, 0.0)
    big_row, big_lane = iota((128, 128), 0), iota((128, 128), 1)
    one_x = (big_row & 31) == (big_lane & 31)
    column = jnp.where(one_x, 1.0, 0.0)
    above = jnp.where(one_x & ((big_row >> 5) < (big_lane >> 5)), 1.0, 0.0)
    earlier = jnp.where(iota((4 * NZ, 4 * NZ), 1) < iota((4 * NZ, 4 * NZ), 0), 1.0, 0.0)
    count = jnp.sum(held, axis=0, keepdims=True)
    sums = jnp.concatenate([count, jnp.zeros((7, 128), F32)], axis=0)
    start = jnp.dot(sums, above, preferred_element_type=F32)[0:1]
    whole = jnp.dot(sums, column, preferred_element_type=F32)[0:1]
    order = jnp.dot(earlier, held, preferred_element_type=F32) + start
    named = (iota((4 * NZ, 128), 0) >> 2).astype(F32) * OWN + wanted + 1.0
    picks = [
        jnp.sum(jnp.where(valid & (order == float(k)), named, 0.0), axis=0, keepdims=True)
        for k in range(PLACES)
    ]
    picks = jnp.dot(jnp.concatenate(picks, axis=0), column, preferred_element_type=F32)
    for part in range(PLACES // 8):
        tables[1 + part] = picks[part * 8 : part * 8 + 8].astype(I32) - 1
        table_copy(1 + part, pick.at[part]).start()
    over_x = jnp.where(jnp.max(whole, axis=1, keepdims=True) > PLACES, 1.0, 0.0)
    over_z = jnp.max(
        jnp.max(metain[:, 4, :].astype(F32), axis=1, keepdims=True), axis=0, keepdims=True
    )
    over = jnp.broadcast_to(jnp.maximum(over_x, over_z), (1, 128))
    mark[0] = jnp.concatenate([count, start, over, jnp.zeros((5, 128), F32)], axis=0).astype(I32)
    marks_x[x] = mark[0]

    def mark_copy(kind, step):
        targets = (x_device, y_device, ring_device)
        arrays = (marks_x, marks_y, marks_z)
        own = (x, y, z)
        return send_to(
            mark.at[kind],
            arrays[kind].at[own[kind]],
            mark_send.at[kind, step],
            mark_recv.at[kind, step],
            targets[kind](step),
        )

    for step in range(1, NX):
        mark_copy(0, step).start()
    target = iota((128, ROWS), 1)
    chosen = jnp.where(iota((128, ROWS), 0) == (target // PLACES) + z * 4, 1.0, 0.0)
    chosen = jnp.dot(picks, chosen, preferred_element_type=F32)
    here = iota((PLACES, ROWS), 0) == iota((PLACES, ROWS), 1) % PLACES
    sums_row = jnp.sum(jnp.where(here, chosen, 0.0), axis=0, keepdims=True)
    tab[...] = jnp.zeros(tab.shape, I32)
    tab[0:1, :] = back_row.astype(I32)
    tab[1:2, :] = sums_row.astype(I32)

    table_copy(0, slot).wait()
    for part in range(PLACES // 8):
        table_copy(1 + part, pick.at[part]).wait()

    for event in FETCH[half_way:first_x]:
        ring_send(*event[1:])

    def x_copy(chunk, step):
        return send_to(
            x_pack.at[chunk, pl.ds(((x + step) % NX) * PLACES, PLACES)],
            x_recv[chunk].at[pl.ds(x * PLACES, PLACES)],
            x_send.at[chunk, step],
            x_sem.at[chunk, step],
            x_device(step),
        )

    def y_copy(chunk, step):
        return send_to(
            y_pack.at[chunk, pl.ds(((y + step) % NY) * PLACES, PLACES)],
            y_recv[chunk].at[pl.ds(y * PLACES, PLACES)],
            y_send.at[chunk, step],
            y_sem.at[chunk, step],
            y_device(step),
        )

    def along_x(chunk):
        for direction in (1, -1):
            ring_arrival(chunk, direction, hops(chunk, direction))

        def fill(part, carry):
            for k in range(8):
                for to in range(NX):
                    index = pick[part, k, z * 4 + to] & (COLUMN - 1)
                    x_pack[chunk, to * PLACES + part * 8 + k] = ag[chunk][index]
            return carry

        lax.fori_loop(0, PLACES // 8, fill, 0)
        for step in range(1, NX):
            x_copy(chunk, step).start()
        own = pl.ds(x * PLACES, PLACES)
        x_recv[chunk][own] = x_pack[chunk, own]

    def along_y(chunk):
        for step in range(1, NX):
            x_copy(chunk, step).wait_recv()

        def fill(part, carry):
            for k in range(8):
                for to in range(NY):
                    index = turn[to, part * 8 + k] & (ROWS - 1)
                    y_pack[chunk, to * PLACES + part * 8 + k] = x_recv[chunk][index]
            return carry

        lax.fori_loop(0, PLACES // 8, fill, 0)
        for step in range(1, NY):
            y_copy(chunk, step).start()
        own = pl.ds(y * PLACES, PLACES)
        y_recv[chunk][own] = y_pack[chunk, own]

    def pair_copy(part):
        return send_to(
            other.at[part],
            win.at[core, part],
            pair_send.at[part],
            pair_recv.at[part],
            partner,
        )

    def take(quarter):
        low, high = 2 * quarter, 2 * quarter + 1
        for chunk in (low, high):
            for step in range(1, NY):
                y_copy(chunk, step).wait_recv()
        part, half = quarter // 2, quarter % 2

        def both(index):
            index = index & (ROWS - 1)
            return jnp.concatenate([y_recv[low][index], y_recv[high][index]], axis=0)

        def lay(r, carry):
            first = pl.multiple_of(r * PR + half * 8, 8)
            for side in range(2):
                k = r * 2 + side
                lanes_of = slice(side * PW, side * PW + PW)
                win[core, part, pl.ds(first, 8), lanes_of] = both(slot[0, core * CELLS + k])
                other[part, pl.ds(first, 8), lanes_of] = both(slot[0, (1 - core) * CELLS + k])
            return carry

        lax.fori_loop(0, W // PR, lay, 0)

    def run(events):
        for event in events:
            if event[0] == "s":
                ring_send(*event[1:])
            elif event[0] == "x":
                along_x(event[1])
            elif event[0] == "y":
                along_y(event[1])
            else:
                take(event[1])
                if event[1] % 2 == 1:
                    pair_copy(event[1] // 2).start()

    run(FETCH[first_x:first_y])

    for step in range(1, NX):
        mark_copy(0, step).wait()
    counts = marks_x[:, 0, :].astype(F32)
    starts = marks_x[:, 1, :].astype(F32)
    four = iota((NX, 128), 1)
    wide = four.astype(F32)
    giver = iota((NX, 128), 0).astype(F32)
    onward = []
    back = jnp.zeros((NX, 128), F32)
    for to in range(NY):
        mine = four == to * 32 + z * 4 + x
        many = jnp.sum(jnp.where(mine, counts, 0.0), axis=1, keepdims=True)
        low = jnp.sum(jnp.where(mine, starts, 0.0), axis=1, keepdims=True)
        first = exclusive(many)
        inside = (wide >= first) & (wide < first + many)
        onward.append(
            jnp.sum(
                jnp.where(inside, giver * PLACES + low + wide - first, 0.0),
                axis=0,
                keepdims=True,
            )
        )
        inside = (wide >= low) & (wide < low + many)
        back = back + jnp.where(inside, to * PLACES + first + wide - low, 0.0)
    tables[last] = jnp.concatenate(onward + [jnp.zeros((4, 128), F32)], axis=0).astype(I32)
    table_copy(last, turn).start()
    tab[8:12, :] = back.astype(I32)
    table_copy(last + 1, places).start()
    mark[1] = jnp.broadcast_to(
        jnp.max(marks_x[:, 2, :].astype(F32), axis=0, keepdims=True), (8, 128)
    ).astype(I32)
    marks_y[y] = mark[1]
    for step in range(1, NY):
        mark_copy(1, step).start()
    table_copy(last, turn).wait()
    table_copy(last + 1, places).wait()

    next_y = [i for i, event in enumerate(FETCH) if event[0] == "y"]
    run(FETCH[first_y : next_y[2]])
    for step in range(1, NY):
        mark_copy(1, step).wait()
    mark[2] = jnp.max(marks_y[...].astype(F32), axis=0).astype(I32)
    marks_z[z] = mark[2]
    for step in range(1, NZ):
        mark_copy(2, step).start()
    run(FETCH[next_y[2] : next_y[5]])
    for step in range(1, NZ):
        mark_copy(2, step).wait()
    mark[0] = jnp.max(marks_z[...].astype(F32), axis=0).astype(I32)
    crowded = pltpu.make_async_copy(mark.at[0], turned, local_sem.at[0])
    crowded.start()
    run(FETCH[next_y[5] :])
    for chunk in range(CHUNKS):
        for direction in (1, -1):
            for hop in range(1, hops(chunk, direction) + 1):
                ring_copy(chunk, direction, hop).wait_send()
        for step in range(1, NX):
            x_copy(chunk, step).wait_send()
            y_copy(chunk, step).wait_send()
    crowded.wait()
    flag[0, 0] = turned[0, 0]
    pair_copy(0).wait()
    pair_copy(1).wait()


def parts(value):
    high = value.astype(BF16)
    return high, (value - high.astype(F32)).astype(BF16)


def from_left(real, imag, table, sign):
    high, low = parts(jnp.concatenate([real, imag], axis=1))
    out = jnp.dot(
        table[...], jnp.concatenate([high, high], axis=0), preferred_element_type=F32
    ) + jnp.dot(table[:, :W], low, preferred_element_type=F32)
    return out[:W, :W] - sign * out[W:, W:], out[:W, W:] + sign * out[W:, :W]


def from_right(real, imag, table, sign):
    high, low = parts(jnp.concatenate([real, imag], axis=0))
    across = (((1,), (1,)), ((), ()))
    out = lax.dot_general(
        jnp.concatenate([high, high], axis=1), table[...], across, preferred_element_type=F32
    ) + lax.dot_general(low, table[:, :W], across, preferred_element_type=F32)
    return out[:W, :W] - sign * out[W:, W:], sign * out[:W, W:] + out[W:, :W]


def both_sides(real, imag, table, sign):
    real, imag = from_left(real, imag, table, sign)
    return from_right(real, imag, table, sign)


def position(win, probe, measured, dft, move, lay):
    pr, pi = probe[0], probe[1]
    ar, ai = win[0, 0], win[0, 1]
    wave_r, wave_i = both_sides(pr * ar - pi * ai, pr * ai + pi * ar, move, 1.0)
    br, bi = win[1, 0], win[1, 1]
    far_r, far_i = both_sides(
        wave_r * br - wave_i * bi, wave_r * bi + wave_i * br, dft, 1.0
    )
    gap = far_r * far_r + far_i * far_i - measured[...]
    back_r, back_i = both_sides(gap * far_r, gap * far_i, dft, -1.0)
    lay(1, wave_r * back_r + wave_i * back_i, wave_r * back_i - wave_i * back_r)
    br, bi = win[1, 0], win[1, 1]
    low_r, low_i = both_sides(
        br * back_r + bi * back_i, br * back_i - bi * back_r, move, -1.0
    )
    pr, pi = probe[0], probe[1]
    lay(0, pr * low_r + pi * low_i, pr * low_i - pi * low_r)


def lay_cells(grad):
    def lay(index, real, imag):
        for k in range(CELLS):
            rows = slice(k // 2 * PR, k // 2 * PR + PR)
            lanes = slice(k % 2 * PW, k % 2 * PW + PW)
            for part, value in enumerate((real, imag)):
                value = value[rows, lanes]
                for strip in range(4):
                    grad[index, k, part * 4 + strip] = value[strip * TALL : strip * TALL + TALL]

    return lay


def position_kernel(win, probe, measured, dft, move, grad):
    core = lax.axis_index("section")
    position(win, probe, measured.at[core], dft, move, lay_cells(grad))


def position_gradients(windows, probe_wave, intensities, dft, move):
    vmem = pl.BlockSpec(memory_space=pltpu.VMEM)
    return pl.pallas_call(
        position_kernel,
        out_shape=jax.ShapeDtypeStruct((2, CELLS, CHUNKS, TALL, PW), F32),
        in_specs=[vmem] * 5,
        out_specs=vmem,
        name="position_gradients",
    )(windows, probe_wave, intensities, dft, move)


def give_back(
    grad,
    places,
    tab,
    out,
    cells,
    y_pack,
    y_recv,
    x_pack,
    x_recv,
    total,
    ring,
    mix,
    pair_send,
    pair_recv,
    y_send,
    y_sem,
    x_send,
    x_sem,
    rs_send,
    rs_recv,
):
    core, y, z, x = place()
    partner = device(1 - core, y, z, x)

    def ring_device(step):
        return device(core, y, (z + step) % NZ, x)

    def x_device(step):
        return device(core, y, z, (x + step) % NX)

    def y_device(step):
        return device(core, (y + step) % NY, z, x)

    def pair_copy(chunk):
        return send_to(
            grad.at[1 - core, :, chunk],
            cells[chunk].at[pl.ds(core * CELLS, CELLS)],
            pair_send.at[chunk],
            pair_recv.at[chunk],
            partner,
        )

    for chunk in range(CHUNKS):
        cells[chunk][pl.ds(core * CELLS, CELLS)] = grad[core, :, chunk]
    for chunk in range(CHUNKS):
        pair_copy(chunk).start()

    mix[...] = jnp.where(
        jnp.broadcast_to(tab[1:2, :], (COLUMN, ROWS)) == iota((COLUMN, ROWS), 0) + 1, 1.0, 0.0
    ).astype(BF16)

    def y_copy(chunk, step):
        return send_to(
            y_pack.at[chunk, pl.ds(((y + step) % NY) * PLACES, PLACES)],
            y_recv[chunk].at[pl.ds(y * PLACES, PLACES)],
            y_send.at[chunk, step],
            y_sem.at[chunk, step],
            y_device(step),
        )

    def x_copy(chunk, step):
        return send_to(
            x_pack.at[chunk, pl.ds(((x + step) % NX) * (PLACES * TALL), PLACES * TALL)],
            x_recv.at[chunk, pl.ds(x * (PLACES * TALL), PLACES * TALL)],
            x_send.at[chunk, step],
            x_sem.at[chunk, step],
            x_device(step),
        )

    for chunk in range(CHUNKS):
        pair_copy(chunk).wait_recv()

        def fill_y(row):
            index = places[0, row] & (MB * CELLS - 1)
            y_pack[chunk, row] = cells[chunk][index]

        fill_rows(ROWS, fill_y)
        for step in range(1, NY):
            y_copy(chunk, step).start()
        own = pl.ds(y * PLACES, PLACES)
        y_recv[chunk][own] = y_pack[chunk, own]

    def along_x(chunk):
        for step in range(1, NY):
            y_copy(chunk, step).wait_recv()

        def fill_x(pair):
            to, k = pair // (PLACES // 2), pair % (PLACES // 2) * 2
            two = [places[8 + to, k + i] & (ROWS - 1) for i in range(2)]
            spot = pl.ds(pl.multiple_of(pair * 2 * TALL, 8), 2 * TALL)
            x_pack[chunk, spot] = jnp.concatenate([y_recv[chunk][i] for i in two], axis=0)

        fill_rows(ROWS // 2, fill_x)
        for step in range(1, NX):
            x_copy(chunk, step).start()
        own = pl.ds(x * (PLACES * TALL), PLACES * TALL)
        x_recv[chunk, own] = x_pack[chunk, own]

    def block(zz):
        return pl.ds(((zz + 2 * NZ) % NZ) * (OWN * TALL), OWN * TALL)

    def ring_copy(chunk, direction, step):
        side = 0 if direction > 0 else 1
        reach = hops(chunk, direction)
        return send_to(
            total.at[chunk, block(z + direction * reach)]
            if step == 1
            else ring.at[chunk, side, step - 2],
            ring.at[chunk, side, step - 1],
            rs_send.at[chunk, side, step - 1],
            rs_recv.at[chunk, side, step - 1],
            ring_device(direction + NZ),
        )

    def sum_cells(chunk):
        for step in range(1, NX):
            x_copy(chunk, step).wait_recv()

        def add(r, carry):
            high, low = parts(x_recv[chunk, pl.ds(r, ROWS, stride=TALL), :])
            both = jnp.dot(
                mix[...], jnp.concatenate([high, low], axis=1), preferred_element_type=F32
            )
            total[chunk, pl.ds(r, COLUMN, stride=TALL), :] = both[:, :128] + both[:, 128:]
            return carry

        lax.fori_loop(0, TALL, add, 0)
        for direction in (1, -1):
            ring_copy(chunk, direction, 1).start()

    def pass_on(chunk, direction, step):
        reach = hops(chunk, direction)
        side = 0 if direction > 0 else 1
        ring_copy(chunk, direction, step - 1).wait_recv()
        ring[chunk, side, step - 2] += total[chunk, block(z + direction * (reach - step + 1))]
        ring_copy(chunk, direction, step).start()

    def last(chunk):
        value = total[chunk, block(z)]
        for direction in (1, -1):
            reach = hops(chunk, direction)
            side = 0 if direction > 0 else 1
            ring_copy(chunk, direction, reach).wait_recv()
            value = value + ring[chunk, side, reach - 1]
        return value

    def finish(quarter):
        low, high = last(2 * quarter), last(2 * quarter + 1)
        for p in range(OWN):
            rows = slice(p * TALL, p * TALL + TALL)
            spot = p * CHUNKS * TALL + quarter * 8
            out[spot : spot + 8] = jnp.concatenate([low[rows], high[rows]], axis=0)

    ended = set()
    for event in RETURN:
        if event[0] == "x":
            along_x(event[1])
        elif event[0] == "a":
            sum_cells(event[1])
        elif event[0] == "p":
            pass_on(*event[1:])
        else:
            ended.add(event[1])
            if event[1] ^ 1 in ended:
                finish(event[1] // 2)

    for chunk in range(CHUNKS):
        pair_copy(chunk).wait_send()
        for direction in (1, -1):
            for step in range(1, hops(chunk, direction) + 1):
                ring_copy(chunk, direction, step).wait_send()
        for step in range(1, NX):
            x_copy(chunk, step).wait_send()
            y_copy(chunk, step).wait_send()


def whole_kernel(obj, meta, cells, probe, measured, dft, move, out, flag, *scratch):
    fetching, giving, (grad, probe_in, measured_in, dft_in, move_in, load_sem) = scratch
    win, tab, places = fetching["win"], fetching["tab"], fetching["places"]
    core = lax.axis_index("section")
    loads = [
        pltpu.make_async_copy(source, target, load_sem.at[index])
        for index, (source, target) in enumerate(
            (
                (probe, probe_in),
                (measured.at[core], measured_in),
                (dft, dft_in),
                (move, move_in),
            )
        )
    ]
    fetch(obj, meta, cells, flag=flag, loads=loads, **fetching)
    for load in loads:
        load.wait()
    position(win, probe_in, measured_in, dft_in, move_in, lay_cells(grad))
    del win
    give_back(grad, places, tab, out, **giving)


def object_sums(owned, meta, cells, probe_wave, intensities, dft, move):
    vmem = pl.BlockSpec(memory_space=pltpu.VMEM)
    anywhere = pl.BlockSpec(memory_space=pltpu.HBM)
    tile, strip = (8, PW), (TALL, PW)
    dma = pltpu.SemaphoreType.DMA
    many, one = pltpu.VMEM((CHUNKS, ROWS) + strip, F32), pltpu.VMEM((ROWS,) + strip, F32)
    fetching = dict(
        win=pltpu.VMEM((2, 2, W, W), F32),
        tab=pltpu.VMEM((16, 128), I32),
        ag=[pltpu.VMEM((COLUMN,) + strip, F32)] * CHUNKS,
        metas=pltpu.VMEM(tile, I32),
        metain=pltpu.VMEM((NZ,) + tile, I32),
        tables=pltpu.VMEM((2 + PLACES // 8,) + tile, I32),
        pick=pltpu.SMEM((PLACES // 8,) + tile, I32),
        turn=pltpu.SMEM(tile, I32),
        turned=pltpu.SMEM(tile, I32),
        slot=pltpu.SMEM(tile, I32),
        places=pltpu.SMEM((16, 128), I32),
        x_pack=many,
        x_recv=[one] * CHUNKS,
        y_pack=many,
        y_recv=[one] * CHUNKS,
        mark=pltpu.VMEM((3,) + tile, I32),
        marks_x=pltpu.VMEM((NX,) + tile, I32),
        marks_y=pltpu.VMEM((NY,) + tile, I32),
        marks_z=pltpu.VMEM((NZ,) + tile, I32),
        other=pltpu.VMEM((2, W, W), F32),
        ag_send=dma((CHUNKS, 2, 4)),
        ag_recv=dma((CHUNKS, 2, 4)),
        meta_send=dma((NZ,)),
        meta_recv=dma((NZ,)),
        mark_send=dma((3, NZ)),
        mark_recv=dma((3, NZ)),
        x_send=dma((CHUNKS, NX)),
        x_sem=dma((CHUNKS, NX)),
        y_send=dma((CHUNKS, NY)),
        y_sem=dma((CHUNKS, NY)),
        pair_send=dma((2,)),
        pair_recv=dma((2,)),
        local_sem=dma((3 + PLACES // 8,)),
    )
    giving = dict(
        cells=[pltpu.VMEM((MB * CELLS,) + strip, F32)] * CHUNKS,
        y_pack=many,
        y_recv=[one] * CHUNKS,
        x_pack=pltpu.VMEM((CHUNKS, ROWS * TALL, PW), F32),
        x_recv=pltpu.VMEM((CHUNKS, ROWS * TALL, PW), F32),
        total=pltpu.VMEM((CHUNKS, COLUMN * TALL, PW), F32),
        ring=pltpu.VMEM((CHUNKS, 2, 4, OWN * TALL, PW), F32),
        mix=pltpu.VMEM((COLUMN, ROWS), BF16),
        pair_send=dma((CHUNKS,)),
        pair_recv=dma((CHUNKS,)),
        y_send=dma((CHUNKS, NY)),
        y_sem=dma((CHUNKS, NY)),
        x_send=dma((CHUNKS, NX)),
        x_sem=dma((CHUNKS, NX)),
        rs_send=dma((CHUNKS, 2, 4)),
        rs_recv=dma((CHUNKS, 2, 4)),
    )
    rest = [
        pltpu.VMEM((2, CELLS, CHUNKS) + strip, F32),
        pltpu.VMEM((2, W, W), F32),
        pltpu.VMEM((W, W), F32),
        pltpu.VMEM((2 * W, 2 * W), BF16),
        pltpu.VMEM((2 * W, 2 * W), BF16),
        dma((4,)),
    ]
    return pl.pallas_call(
        whole_kernel,
        out_shape=(
            jax.ShapeDtypeStruct((OWN * CHUNKS * TALL, PW), F32),
            jax.ShapeDtypeStruct((1, 1), I32),
        ),
        in_specs=[vmem] * 3 + [anywhere] * 4,
        out_specs=(vmem, pl.BlockSpec(memory_space=pltpu.SMEM)),
        scratch_shapes=[fetching, giving, rest],
        compiler_params=pltpu.CompilerParams(
            collective_id=0, has_side_effects=True, vmem_limit_bytes=46 << 20
        ),
        name="object_sums",
    )(owned, meta, cells, probe_wave, intensities, dft, move)


def swapped(block):
    return lax.ppermute(block, "section", [(0, 1), (1, 0)])


def place_in_all(cell_slot):
    batch = iota(cell_slot.shape, 0)
    return ((cell_slot >> 1) * (2 * MB) + batch * 2 + (cell_slot & 1)).reshape(-1)


def full_windows(owned, send_plan, cell_slot):
    core = lax.axis_index("section")
    outbound = jnp.swapaxes(send_plan, 0, 1)
    patches = owned[jnp.maximum(outbound, 0)]
    arrived = lax.all_to_all(patches, "tile", split_axis=0, concat_axis=0, tiled=True)
    picked = arrived.reshape((-1, 2, PR, PW))[place_in_all(cell_slot)]
    picked = picked.reshape(MB, W // PR, W // PW, 2, PR, PW)
    windows = jnp.transpose(picked, (0, 3, 1, 4, 2, 5)).reshape(MB, 2, W, W)
    passed = swapped(lax.dynamic_index_in_dim(windows, 1 - core, 0, keepdims=False))
    kept = lax.dynamic_index_in_dim(windows, core, 0, keepdims=False)
    first = core == 0
    return jnp.stack([jnp.where(first, kept, passed), jnp.where(first, passed, kept)])


def full_sums(gradients, send_plan, cell_slot):
    core = lax.axis_index("section")
    passed = swapped(lax.dynamic_index_in_dim(gradients, 1 - core, 0, keepdims=False))
    kept = lax.dynamic_index_in_dim(gradients, core, 0, keepdims=False)
    first = core == 0
    batches = jnp.stack([jnp.where(first, kept, passed), jnp.where(first, passed, kept)])
    owners = NX * NY * NZ
    placed = (
        jnp.zeros((owners * MB * 2, 2, PR, PW), F32)
        .at[place_in_all(cell_slot)]
        .set(batches.reshape(-1, 2, PR, PW))
    )
    returned = lax.all_to_all(
        placed.reshape(owners, MB, 2, 2, PR, PW), "tile", split_axis=0, concat_axis=0, tiled=True
    )
    outbound = jnp.swapaxes(send_plan, 0, 1)
    target = jnp.where(outbound < 0, OWN, outbound).reshape(-1)
    sums = jax.ops.segment_sum(
        returned.reshape((-1, 2, PR, PW)), target, num_segments=OWN + 1
    )
    return sums[:OWN]


def body(dft, move, object_slices, probe_wave, intensities, send_list, cell_slot):
    owned = object_slices[0]
    send_plan = send_list[0]
    meta = jnp.transpose(send_plan, (0, 2, 1)).reshape(MB * 2, NX * NY * NZ)
    meta = lax.optimization_barrier(meta)
    sums, flag = object_sums(
        owned.reshape(OWN, CHUNKS, TALL, PW),
        meta,
        cell_slot,
        probe_wave,
        intensities,
        dft,
        move,
    )

    def full():
        plan = jnp.transpose(meta.reshape(MB, 2, NX * NY * NZ), (0, 2, 1))
        windows = full_windows(owned, plan, cell_slot)
        gradients = position_gradients(windows, probe_wave, intensities, dft, move)
        return full_sums(gradients.reshape(2, CELLS, 2, PR, PW), plan, cell_slot)

    sums = lax.cond(flag[0, 0] > 0, full, lambda: sums.reshape(OWN, 2, PR, PW))
    return sums[None]


def solution(mesh):
    dft, move = matrix_tables()
    in_specs = (
        P("section", "tile", None, None, None),
        P(),
        P("tile", None, None),
        P("tile", None, None, None),
        P("tile", None),
    )
    out_specs = P("section", "tile", None, None, None)
    step = functools.partial(body, jnp.asarray(dft), jnp.asarray(move))
    return jax.shard_map(step, mesh=mesh, in_specs=in_specs, out_specs=out_specs, check_vma=False)
```

```python
import functools

import jax
import jax.numpy as jnp
import ml_dtypes
import numpy as np
from jax import lax
from jax.experimental import pallas as pl
from jax.experimental.pallas import tpu as pltpu
from jax.sharding import PartitionSpec as P

W = 256
PW = 128
PR = 16
MB = 2
CELLS = 32
NX, NY, NZ = 4, 4, 8
PLANE = NX * NY
OWN = 32
COLUMN = NZ * OWN
PLACES = 32
ROWS = 4 * PLACES
CHUNKS = 8
TALL = 4
PHASE_SCALE = 20.0
MESH = pl.DeviceIdType.MESH
F32 = jnp.float32
I32 = jnp.int32
BF16 = jnp.bfloat16


FETCH = (
    ("s", 0, -1, 1),
    ("s", 0, 1, 1),
    ("s", 1, -1, 1),
    ("s", 1, 1, 1),
    ("s", 2, -1, 1),
    ("s", 2, 1, 1),
    ("s", 3, -1, 1),
    ("s", 3, 1, 1),
    ("s", 4, -1, 1),
    ("s", 4, 1, 1),
    ("s", 0, -1, 2),
    ("s", 0, 1, 2),
    ("s", 1, -1, 2),
    ("s", 1, 1, 2),
    ("s", 2, -1, 2),
    ("s", 2, 1, 2),
    ("s", 3, -1, 2),
    ("s", 3, 1, 2),
    ("s", 4, -1, 2),
    ("s", 4, 1, 2),
    ("s", 0, -1, 3),
    ("s", 0, 1, 3),
    ("s", 1, -1, 3),
    ("s", 1, 1, 3),
    ("s", 2, -1, 3),
    ("s", 2, 1, 3),
    ("s", 3, -1, 3),
    ("s", 3, 1, 3),
    ("s", 4, -1, 3),
    ("s", 4, 1, 3),
    ("s", 0, 1, 4),
    ("s", 5, -1, 1),
    ("s", 1, -1, 4),
    ("s", 5, 1, 1),
    ("s", 2, 1, 4),
    ("s", 6, -1, 1),
    ("s", 3, -1, 4),
    ("s", 6, 1, 1),
    ("s", 4, 1, 4),
    ("s", 7, -1, 1),
    ("s", 5, -1, 2),
    ("x", 0),
    ("s", 7, 1, 1),
    ("x", 1),
    ("s", 5, 1, 2),
    ("s", 6, -1, 2),
    ("x", 2),
    ("x", 3),
    ("s", 6, 1, 2),
    ("s", 7, -1, 2),
    ("x", 4),
    ("y", 0),
    ("s", 5, -1, 3),
    ("s", 7, 1, 2),
    ("s", 6, -1, 3),
    ("s", 5, 1, 3),
    ("y", 1),
    ("s", 6, 1, 3),
    ("s", 7, -1, 3),
    ("s", 5, -1, 4),
    ("s", 7, 1, 3),
    ("y", 2),
    ("s", 6, 1, 4),
    ("s", 7, -1, 4),
    ("y", 3),
    ("t", 0),
    ("x", 5),
    ("y", 4),
    ("x", 6),
    ("x", 7),
    ("t", 1),
    ("y", 5),
    ("y", 6),
    ("y", 7),
    ("t", 2),
    ("t", 3),
)
RETURN = (
    ("x", 0),
    ("x", 1),
    ("x", 2),
    ("a", 0),
    ("x", 3),
    ("a", 1),
    ("x", 4),
    ("p", 0, -1, 2),
    ("p", 0, 1, 2),
    ("a", 2),
    ("x", 5),
    ("p", 1, -1, 2),
    ("p", 1, 1, 2),
    ("a", 3),
    ("p", 0, -1, 3),
    ("p", 0, 1, 3),
    ("x", 6),
    ("a", 4),
    ("p", 2, -1, 2),
    ("p", 2, 1, 2),
    ("p", 1, -1, 3),
    ("p", 1, 1, 3),
    ("x", 7),
    ("a", 5),
    ("p", 3, -1, 2),
    ("p", 3, 1, 2),
    ("p", 0, 1, 4),
    ("p", 4, -1, 2),
    ("p", 4, 1, 2),
    ("a", 6),
    ("p", 2, -1, 3),
    ("p", 2, 1, 3),
    ("p", 1, -1, 4),
    ("a", 7),
    ("p", 5, -1, 2),
    ("p", 5, 1, 2),
    ("p", 3, -1, 3),
    ("p", 3, 1, 3),
    ("p", 4, -1, 3),
    ("f", 0),
    ("p", 6, -1, 2),
    ("p", 4, 1, 3),
    ("p", 6, 1, 2),
    ("f", 1),
    ("p", 2, 1, 4),
    ("p", 7, -1, 2),
    ("p", 7, 1, 2),
    ("p", 5, -1, 3),
    ("p", 5, 1, 3),
    ("p", 3, -1, 4),
    ("p", 4, 1, 4),
    ("p", 6, -1, 3),
    ("p", 6, 1, 3),
    ("p", 7, -1, 3),
    ("f", 2),
    ("p", 5, -1, 4),
    ("p", 7, 1, 3),
    ("f", 3),
    ("f", 4),
    ("p", 7, -1, 4),
    ("p", 6, 1, 4),
    ("f", 5),
    ("f", 7),
    ("f", 6),
)


def stacked_parts(matrix):
    rows = np.concatenate([matrix.real, matrix.imag], axis=0).astype(np.float32)
    high = rows.astype(ml_dtypes.bfloat16)
    low = (rows - high.astype(np.float32)).astype(ml_dtypes.bfloat16)
    return np.concatenate([high, low], axis=1)


def matrix_tables():
    index = np.arange(W)
    product = np.outer(index, index) % W
    dft = np.exp(-2j * np.pi * product / W) / np.sqrt(W)
    frequency = np.where(index < W // 2, index, index - W).astype(np.float64)
    diagonal = np.exp(-1j * PHASE_SCALE * frequency**2 / (W * W))
    move = np.conj(dft) @ (diagonal[:, None] * dft)
    move = (move + move.T) / 2
    return stacked_parts(dft), stacked_parts(move)


def place():
    tile = lax.axis_index("tile")
    core = lax.axis_index("section")
    y = tile // (NZ * NX)
    z = (tile // NX) % NZ
    x = tile % NX
    return core, y, z, x


def device(core, y, z, x):
    return (core, y * (NZ * NX) + z * NX + x)


def iota(shape, axis):
    return lax.broadcasted_iota(I32, shape, axis)


def to_column(row):
    n = row.shape[1]
    wide = jnp.broadcast_to(row, (n, n))
    return jnp.sum(jnp.where(iota((n, n), 0) == iota((n, n), 1), wide, 0.0), axis=1, keepdims=True)


def exclusive(column):
    rows = [jnp.zeros_like(column[0:1])]
    for step in range(column.shape[0] - 1):
        rows.append(rows[-1] + column[step : step + 1])
    return jnp.concatenate(rows, axis=0)


def send_to(src, dst, send_sem, recv_sem, target):
    return pltpu.make_async_remote_copy(
        src_ref=src,
        dst_ref=dst,
        send_sem=send_sem,
        recv_sem=recv_sem,
        device_id=target,
        device_id_type=MESH,
    )


def greet(barrier, targets):
    for target in targets:
        pl.semaphore_signal(barrier, inc=1, device_id=target, device_id_type=MESH)
    pl.semaphore_wait(barrier, len(targets))


def hops(chunk, direction):
    return 4 if (chunk % 2 == 0) == (direction > 0) else 3


def fill_rows(count, move):
    def some(part, carry):
        for k in range(8):
            move(part * 8 + k)
        return carry

    lax.fori_loop(0, count // 8, some, 0)


def fetch(
    obj,
    meta,
    cells,
    win,
    tab,
    flag,
    ag,
    metas,
    metain,
    tables,
    pick,
    turn,
    turned,
    slot,
    places,
    x_pack,
    x_recv,
    y_pack,
    y_recv,
    mark,
    marks_x,
    marks_y,
    marks_z,
    other,
    ag_send,
    ag_recv,
    meta_send,
    meta_recv,
    mark_send,
    mark_recv,
    x_send,
    x_sem,
    y_send,
    y_sem,
    pair_send,
    pair_recv,
    local_sem,
    loads,
):
    core, y, z, x = place()
    partner = device(1 - core, y, z, x)

    def ring_device(step):
        return device(core, y, (z + step) % NZ, x)

    def x_device(step):
        return device(core, y, z, (x + step) % NX)

    def y_device(step):
        return device(core, (y + step) % NY, z, x)

    greet(
        pltpu.get_barrier_semaphore(),
        [ring_device(step) for step in range(1, NZ)]
        + [x_device(step) for step in range(1, NX)]
        + [y_device(step) for step in range(1, NY)]
        + [partner],
    )

    def block(chunk, zz):
        return ag[chunk].at[pl.ds(((zz + 2 * NZ) % NZ) * OWN, OWN)]

    def ring_copy(chunk, direction, hop):
        side = 0 if direction > 0 else 1
        held = block(chunk, z - direction * (hop - 1))
        return send_to(
            obj.at[:, chunk] if hop == 1 else held,
            held,
            ag_send.at[chunk, side, hop - 1],
            ag_recv.at[chunk, side, hop - 1],
            ring_device(direction + NZ),
        )

    def ring_arrival(chunk, direction, hop):
        side = 0 if direction > 0 else 1
        held = block(chunk, z - direction * hop)
        send_to(
            held,
            held,
            ag_send.at[chunk, side, hop - 1],
            ag_recv.at[chunk, side, hop - 1],
            ring_device(direction + NZ),
        ).wait_recv()

    def ring_send(chunk, direction, hop):
        if hop > 1:
            ring_arrival(chunk, direction, hop - 1)
        ring_copy(chunk, direction, hop).start()

    first_wait = min(i for i, event in enumerate(FETCH) if event[0] != "s" or event[3] > 1)
    first_x = min(i for i, event in enumerate(FETCH) if event[0] == "x")
    first_y = min(i for i, event in enumerate(FETCH) if event[0] == "y")
    for event in FETCH[:first_wait]:
        ring_send(*event[1:])

    for load in loads:
        load.start()

    row = jnp.concatenate([cells[0:1, :], cells[1:2, :]], axis=1)
    owner = row >> 1
    entry = ((owner >> 2) & 7) * 4 + (iota(row.shape, 1) >> 5) * 2 + (row & 1)
    code_row = ((owner >> 5) * 128 + (owner & 3) * 32 + entry).astype(F32)
    y_row = (owner >> 5).astype(F32)
    code_col = to_column(code_row)
    y_col = to_column(y_row)
    ahead = (y_col == y_row) & (code_col < code_row)
    rank = jnp.sum(jnp.where(ahead, 1.0, 0.0), axis=0, keepdims=True)
    over = jnp.where(jnp.max(rank, axis=1, keepdims=True) >= PLACES, 1, 0)
    at = y_row * PLACES + jnp.minimum(rank, PLACES - 1.0)
    tables[0] = jnp.zeros((8, 128), I32)
    tables[0, 0:1, 0 : MB * CELLS] = at.astype(I32)
    at_col = to_column(jnp.where(rank < PLACES, at, -1.0))
    spread = jnp.broadcast_to(at_col, (MB * CELLS, ROWS)) == iota((MB * CELLS, ROWS), 1).astype(
        F32
    )
    number = iota((MB * CELLS, ROWS), 0).astype(F32)
    back_row = jnp.sum(jnp.where(spread, number, 0.0), axis=0, keepdims=True)

    metas[...] = jnp.concatenate(
        [meta[...], jnp.broadcast_to(over, (1, 128)), jnp.zeros((3, 128), I32)], axis=0
    )
    metain[z] = metas[...]

    def meta_copy(step):
        return send_to(
            metas,
            metain.at[z],
            meta_send.at[step],
            meta_recv.at[step],
            ring_device(step),
        )

    for step in range(1, NZ):
        meta_copy(step).start()

    last = 1 + PLACES // 8

    def table_copy(index, target):
        source = tab if index > last else tables.at[index]
        return pltpu.make_async_copy(source, target, local_sem.at[index])

    table_copy(0, slot).start()

    for chunk in range(CHUNKS):
        ag[chunk][pl.ds(z * OWN, OWN)] = obj[:, chunk]

    half_way = (first_wait + first_x) // 2
    for event in FETCH[first_wait:half_way]:
        ring_send(*event[1:])

    for step in range(1, NZ):
        meta_copy(step).wait()
    wanted = jnp.concatenate([metain[zz][0:4] for zz in range(NZ)], axis=0).astype(F32)
    lanes = iota((4 * NZ, 128), 1)
    valid = (wanted >= 0.0) & (((lanes >> 2) & 7) == z)
    held = jnp.where(valid, 1.0, 0.0)
    big_row, big_lane = iota((128, 128), 0), iota((128, 128), 1)
    one_x = (big_row & 31) == (big_lane & 31)
    column = jnp.where(one_x, 1.0, 0.0)
    above = jnp.where(one_x & ((big_row >> 5) < (big_lane >> 5)), 1.0, 0.0)
    earlier = jnp.where(iota((4 * NZ, 4 * NZ), 1) < iota((4 * NZ, 4 * NZ), 0), 1.0, 0.0)
    count = jnp.sum(held, axis=0, keepdims=True)
    sums = jnp.concatenate([count, jnp.zeros((7, 128), F32)], axis=0)
    start = jnp.dot(sums, above, preferred_element_type=F32)[0:1]
    whole = jnp.dot(sums, column, preferred_element_type=F32)[0:1]
    order = jnp.dot(earlier, held, preferred_element_type=F32) + start
    named = (iota((4 * NZ, 128), 0) >> 2).astype(F32) * OWN + wanted + 1.0
    picks = [
        jnp.sum(jnp.where(valid & (order == float(k)), named, 0.0), axis=0, keepdims=True)
        for k in range(PLACES)
    ]
    picks = jnp.dot(jnp.concatenate(picks, axis=0), column, preferred_element_type=F32)
    for part in range(PLACES // 8):
        tables[1 + part] = picks[part * 8 : part * 8 + 8].astype(I32) - 1
        table_copy(1 + part, pick.at[part]).start()
    over_x = jnp.where(jnp.max(whole, axis=1, keepdims=True) > PLACES, 1.0, 0.0)
    over_z = jnp.max(
        jnp.max(metain[:, 4, :].astype(F32), axis=1, keepdims=True), axis=0, keepdims=True
    )
    over = jnp.broadcast_to(jnp.maximum(over_x, over_z), (1, 128))
    mark[0] = jnp.concatenate([count, start, over, jnp.zeros((5, 128), F32)], axis=0).astype(I32)
    marks_x[x] = mark[0]

    def mark_copy(kind, step):
        targets = (x_device, y_device, ring_device)
        arrays = (marks_x, marks_y, marks_z)
        own = (x, y, z)
        return send_to(
            mark.at[kind],
            arrays[kind].at[own[kind]],
            mark_send.at[kind, step],
            mark_recv.at[kind, step],
            targets[kind](step),
        )

    for step in range(1, NX):
        mark_copy(0, step).start()
    target = iota((128, ROWS), 1)
    chosen = jnp.where(iota((128, ROWS), 0) == (target // PLACES) + z * 4, 1.0, 0.0)
    chosen = jnp.dot(picks, chosen, preferred_element_type=F32)
    here = iota((PLACES, ROWS), 0) == iota((PLACES, ROWS), 1) % PLACES
    sums_row = jnp.sum(jnp.where(here, chosen, 0.0), axis=0, keepdims=True)
    tab[...] = jnp.zeros(tab.shape, I32)
    tab[0:1, :] = back_row.astype(I32)
    tab[1:2, :] = sums_row.astype(I32)

    table_copy(0, slot).wait()
    for part in range(PLACES // 8):
        table_copy(1 + part, pick.at[part]).wait()

    for event in FETCH[half_way:first_x]:
        ring_send(*event[1:])

    def x_copy(chunk, step):
        return send_to(
            x_pack.at[chunk, pl.ds(((x + step) % NX) * PLACES, PLACES)],
            x_recv[chunk].at[pl.ds(x * PLACES, PLACES)],
            x_send.at[chunk, step],
            x_sem.at[chunk, step],
            x_device(step),
        )

    def y_copy(chunk, step):
        return send_to(
            y_pack.at[chunk, pl.ds(((y + step) % NY) * PLACES, PLACES)],
            y_recv[chunk].at[pl.ds(y * PLACES, PLACES)],
            y_send.at[chunk, step],
            y_sem.at[chunk, step],
            y_device(step),
        )

    def along_x(chunk):
        for direction in (1, -1):
            ring_arrival(chunk, direction, hops(chunk, direction))

        def fill(part, carry):
            for k in range(8):
                for to in range(NX):
                    index = pick[part, k, z * 4 + to] & (COLUMN - 1)
                    x_pack[chunk, to * PLACES + part * 8 + k] = ag[chunk][index]
            return carry

        lax.fori_loop(0, PLACES // 8, fill, 0)
        for step in range(1, NX):
            x_copy(chunk, step).start()
        own = pl.ds(x * PLACES, PLACES)
        x_recv[chunk][own] = x_pack[chunk, own]

    def along_y(chunk):
        for step in range(1, NX):
            x_copy(chunk, step).wait_recv()

        def fill(part, carry):
            for k in range(8):
                for to in range(NY):
                    index = turn[to, part * 8 + k] & (ROWS - 1)
                    y_pack[chunk, to * PLACES + part * 8 + k] = x_recv[chunk][index]
            return carry

        lax.fori_loop(0, PLACES // 8, fill, 0)
        for step in range(1, NY):
            y_copy(chunk, step).start()
        own = pl.ds(y * PLACES, PLACES)
        y_recv[chunk][own] = y_pack[chunk, own]

    def pair_copy(quarter):
        return send_to(
            other.at[quarter // 2, quarter % 2],
            win.at[core, quarter // 2, quarter % 2],
            pair_send.at[quarter],
            pair_recv.at[quarter],
            partner,
        )

    def take(quarter):
        low, high = 2 * quarter, 2 * quarter + 1
        for chunk in (low, high):
            for step in range(1, NY):
                y_copy(chunk, step).wait_recv()
        part, half = quarter // 2, quarter % 2

        def both(index):
            index = index & (ROWS - 1)
            return jnp.concatenate([y_recv[low][index], y_recv[high][index]], axis=0)

        def lay(r, carry):
            first = pl.multiple_of(r * 8, 8)
            for side in range(2):
                k = r * 2 + side
                lanes_of = slice(side * PW, side * PW + PW)
                win[core, part, half, pl.ds(first, 8), lanes_of] = both(slot[0, core * CELLS + k])
                other[part, half, pl.ds(first, 8), lanes_of] = both(slot[0, (1 - core) * CELLS + k])
            return carry

        lax.fori_loop(0, W // PR, lay, 0)

    def run(events):
        for event in events:
            if event[0] == "s":
                ring_send(*event[1:])
            elif event[0] == "x":
                along_x(event[1])
            elif event[0] == "y":
                along_y(event[1])
            else:
                take(event[1])
                pair_copy(event[1]).start()

    run(FETCH[first_x:first_y])

    for step in range(1, NX):
        mark_copy(0, step).wait()
    counts = marks_x[:, 0, :].astype(F32)
    starts = marks_x[:, 1, :].astype(F32)
    four = iota((NX, 128), 1)
    wide = four.astype(F32)
    giver = iota((NX, 128), 0).astype(F32)
    onward = []
    back = jnp.zeros((NX, 128), F32)
    for to in range(NY):
        mine = four == to * 32 + z * 4 + x
        many = jnp.sum(jnp.where(mine, counts, 0.0), axis=1, keepdims=True)
        low = jnp.sum(jnp.where(mine, starts, 0.0), axis=1, keepdims=True)
        first = exclusive(many)
        inside = (wide >= first) & (wide < first + many)
        onward.append(
            jnp.sum(
                jnp.where(inside, giver * PLACES + low + wide - first, 0.0),
                axis=0,
                keepdims=True,
            )
        )
        inside = (wide >= low) & (wide < low + many)
        back = back + jnp.where(inside, to * PLACES + first + wide - low, 0.0)
    tables[last] = jnp.concatenate(onward + [jnp.zeros((4, 128), F32)], axis=0).astype(I32)
    table_copy(last, turn).start()
    tab[8:12, :] = back.astype(I32)
    table_copy(last + 1, places).start()
    mark[1] = jnp.broadcast_to(
        jnp.max(marks_x[:, 2, :].astype(F32), axis=0, keepdims=True), (8, 128)
    ).astype(I32)
    marks_y[y] = mark[1]
    for step in range(1, NY):
        mark_copy(1, step).start()
    table_copy(last, turn).wait()
    table_copy(last + 1, places).wait()

    next_y = [i for i, event in enumerate(FETCH) if event[0] == "y"]
    run(FETCH[first_y : next_y[2]])
    for step in range(1, NY):
        mark_copy(1, step).wait()
    mark[2] = jnp.max(marks_y[...].astype(F32), axis=0).astype(I32)
    marks_z[z] = mark[2]
    for step in range(1, NZ):
        mark_copy(2, step).start()
    run(FETCH[next_y[2] : next_y[5]])
    for step in range(1, NZ):
        mark_copy(2, step).wait()
    mark[0] = jnp.max(marks_z[...].astype(F32), axis=0).astype(I32)
    crowded = pltpu.make_async_copy(mark.at[0], turned, local_sem.at[0])
    crowded.start()
    run(FETCH[next_y[5] :])
    for chunk in range(CHUNKS):
        for direction in (1, -1):
            for hop in range(1, hops(chunk, direction) + 1):
                ring_copy(chunk, direction, hop).wait_send()
        for step in range(1, NX):
            x_copy(chunk, step).wait_send()
            y_copy(chunk, step).wait_send()
    crowded.wait()
    flag[0, 0] = turned[0, 0]
    for quarter in range(4):
        pair_copy(quarter).wait()


def parts(value):
    high = value.astype(BF16)
    return high, (value - high.astype(F32)).astype(BF16)


def from_left(real, imag, table, sign):
    high, low = parts(jnp.concatenate([real, imag], axis=1))
    out = jnp.dot(
        table[...], jnp.concatenate([high, high], axis=0), preferred_element_type=F32
    ) + jnp.dot(table[:, :W], low, preferred_element_type=F32)
    return out[:W, :W] - sign * out[W:, W:], out[:W, W:] + sign * out[W:, :W]


def from_right(real, imag, table, sign):
    high, low = parts(jnp.concatenate([real, imag], axis=0))
    across = (((1,), (1,)), ((), ()))
    out = lax.dot_general(
        jnp.concatenate([high, high], axis=1), table[...], across, preferred_element_type=F32
    ) + lax.dot_general(low, table[:, :W], across, preferred_element_type=F32)
    return out[:W, :W] - sign * out[W:, W:], sign * out[:W, W:] + out[W:, :W]


def both_sides(real, imag, table, sign):
    real, imag = from_left(real, imag, table, sign)
    return from_right(real, imag, table, sign)


def window(win, index):
    if len(win.shape) == 4:
        return win[index, 0], win[index, 1]
    return tuple(
        jnp.concatenate(
            [
                win[index, part, half, r * 8 : r * 8 + 8]
                for r in range(W // PR)
                for half in range(2)
            ],
            axis=0,
        )
        for part in range(2)
    )


def position(win, probe, measured, dft, move, lay):
    pr, pi = probe[0], probe[1]
    ar, ai = window(win, 0)
    wave_r, wave_i = both_sides(pr * ar - pi * ai, pr * ai + pi * ar, move, 1.0)
    br, bi = window(win, 1)
    far_r, far_i = both_sides(
        wave_r * br - wave_i * bi, wave_r * bi + wave_i * br, dft, 1.0
    )
    gap = far_r * far_r + far_i * far_i - measured[...]
    back_r, back_i = both_sides(gap * far_r, gap * far_i, dft, -1.0)
    lay(1, wave_r * back_r + wave_i * back_i, wave_r * back_i - wave_i * back_r)
    br, bi = window(win, 1)
    low_r, low_i = both_sides(
        br * back_r + bi * back_i, br * back_i - bi * back_r, move, -1.0
    )
    pr, pi = probe[0], probe[1]
    lay(0, pr * low_r + pi * low_i, pr * low_i - pi * low_r)


def lay_cells(grad):
    def lay(index, real, imag):
        for k in range(CELLS):
            rows = slice(k // 2 * PR, k // 2 * PR + PR)
            lanes = slice(k % 2 * PW, k % 2 * PW + PW)
            for part, value in enumerate((real, imag)):
                value = value[rows, lanes]
                for strip in range(4):
                    grad[index, k, part * 4 + strip] = value[strip * TALL : strip * TALL + TALL]

    return lay


def position_kernel(win, probe, measured, dft, move, grad):
    core = lax.axis_index("section")
    position(win, probe, measured.at[core], dft, move, lay_cells(grad))


def position_gradients(windows, probe_wave, intensities, dft, move):
    vmem = pl.BlockSpec(memory_space=pltpu.VMEM)
    return pl.pallas_call(
        position_kernel,
        out_shape=jax.ShapeDtypeStruct((2, CELLS, CHUNKS, TALL, PW), F32),
        in_specs=[vmem] * 5,
        out_specs=vmem,
        name="position_gradients",
    )(windows, probe_wave, intensities, dft, move)


def give_back(
    grad,
    places,
    tab,
    out,
    cells,
    y_pack,
    y_recv,
    x_pack,
    x_recv,
    total,
    ring,
    mix,
    pair_send,
    pair_recv,
    y_send,
    y_sem,
    x_send,
    x_sem,
    rs_send,
    rs_recv,
):
    core, y, z, x = place()
    partner = device(1 - core, y, z, x)

    def ring_device(step):
        return device(core, y, (z + step) % NZ, x)

    def x_device(step):
        return device(core, y, z, (x + step) % NX)

    def y_device(step):
        return device(core, (y + step) % NY, z, x)

    def pair_copy(chunk):
        return send_to(
            grad.at[1 - core, :, chunk],
            cells[chunk].at[pl.ds(core * CELLS, CELLS)],
            pair_send.at[chunk],
            pair_recv.at[chunk],
            partner,
        )

    for chunk in range(CHUNKS):
        cells[chunk][pl.ds(core * CELLS, CELLS)] = grad[core, :, chunk]
    for chunk in range(CHUNKS):
        pair_copy(chunk).start()

    mix[...] = jnp.where(
        jnp.broadcast_to(tab[1:2, :], (COLUMN, ROWS)) == iota((COLUMN, ROWS), 0) + 1, 1.0, 0.0
    ).astype(BF16)

    def y_copy(chunk, step):
        return send_to(
            y_pack.at[chunk, pl.ds(((y + step) % NY) * PLACES, PLACES)],
            y_recv[chunk].at[pl.ds(y * PLACES, PLACES)],
            y_send.at[chunk, step],
            y_sem.at[chunk, step],
            y_device(step),
        )

    def x_copy(chunk, step):
        return send_to(
            x_pack.at[chunk, pl.ds(((x + step) % NX) * (PLACES * TALL), PLACES * TALL)],
            x_recv.at[chunk, pl.ds(x * (PLACES * TALL), PLACES * TALL)],
            x_send.at[chunk, step],
            x_sem.at[chunk, step],
            x_device(step),
        )

    for chunk in range(CHUNKS):
        pair_copy(chunk).wait_recv()

        def fill_y(row):
            index = places[0, row] & (MB * CELLS - 1)
            y_pack[chunk, row] = cells[chunk][index]

        fill_rows(ROWS, fill_y)
        for step in range(1, NY):
            y_copy(chunk, step).start()
        own = pl.ds(y * PLACES, PLACES)
        y_recv[chunk][own] = y_pack[chunk, own]

    def along_x(chunk):
        for step in range(1, NY):
            y_copy(chunk, step).wait_recv()

        def fill_x(pair):
            to, k = pair // (PLACES // 2), pair % (PLACES // 2) * 2
            two = [places[8 + to, k + i] & (ROWS - 1) for i in range(2)]
            spot = pl.ds(pl.multiple_of(pair * 2 * TALL, 8), 2 * TALL)
            x_pack[chunk, spot] = jnp.concatenate([y_recv[chunk][i] for i in two], axis=0)

        fill_rows(ROWS // 2, fill_x)
        for step in range(1, NX):
            x_copy(chunk, step).start()
        own = pl.ds(x * (PLACES * TALL), PLACES * TALL)
        x_recv[chunk, own] = x_pack[chunk, own]

    def block(zz):
        return pl.ds(((zz + 2 * NZ) % NZ) * (OWN * TALL), OWN * TALL)

    def ring_copy(chunk, direction, step):
        side = 0 if direction > 0 else 1
        reach = hops(chunk, direction)
        return send_to(
            total.at[chunk, block(z + direction * reach)]
            if step == 1
            else ring.at[chunk, side, step - 2],
            ring.at[chunk, side, step - 1],
            rs_send.at[chunk, side, step - 1],
            rs_recv.at[chunk, side, step - 1],
            ring_device(direction + NZ),
        )

    def sum_cells(chunk):
        for step in range(1, NX):
            x_copy(chunk, step).wait_recv()

        def add(r, carry):
            high, low = parts(x_recv[chunk, pl.ds(r, ROWS, stride=TALL), :])
            both = jnp.dot(
                mix[...], jnp.concatenate([high, low], axis=1), preferred_element_type=F32
            )
            total[chunk, pl.ds(r, COLUMN, stride=TALL), :] = both[:, :128] + both[:, 128:]
            return carry

        lax.fori_loop(0, TALL, add, 0)
        for direction in (1, -1):
            ring_copy(chunk, direction, 1).start()

    def pass_on(chunk, direction, step):
        reach = hops(chunk, direction)
        side = 0 if direction > 0 else 1
        ring_copy(chunk, direction, step - 1).wait_recv()
        ring[chunk, side, step - 2] += total[chunk, block(z + direction * (reach - step + 1))]
        ring_copy(chunk, direction, step).start()

    def last(chunk):
        value = total[chunk, block(z)]
        for direction in (1, -1):
            reach = hops(chunk, direction)
            side = 0 if direction > 0 else 1
            ring_copy(chunk, direction, reach).wait_recv()
            value = value + ring[chunk, side, reach - 1]
        return value

    def finish(quarter):
        low, high = last(2 * quarter), last(2 * quarter + 1)
        for p in range(OWN):
            rows = slice(p * TALL, p * TALL + TALL)
            spot = p * CHUNKS * TALL + quarter * 8
            out[spot : spot + 8] = jnp.concatenate([low[rows], high[rows]], axis=0)

    ended = set()
    for event in RETURN:
        if event[0] == "x":
            along_x(event[1])
        elif event[0] == "a":
            sum_cells(event[1])
        elif event[0] == "p":
            pass_on(*event[1:])
        else:
            ended.add(event[1])
            if event[1] ^ 1 in ended:
                finish(event[1] // 2)

    for chunk in range(CHUNKS):
        pair_copy(chunk).wait_send()
        for direction in (1, -1):
            for step in range(1, hops(chunk, direction) + 1):
                ring_copy(chunk, direction, step).wait_send()
        for step in range(1, NX):
            x_copy(chunk, step).wait_send()
            y_copy(chunk, step).wait_send()


def whole_kernel(obj, meta, cells, probe, measured, dft, move, out, flag, *scratch):
    fetching, giving, (grad, probe_in, measured_in, dft_in, move_in, load_sem) = scratch
    win, tab, places = fetching["win"], fetching["tab"], fetching["places"]
    core = lax.axis_index("section")
    loads = [
        pltpu.make_async_copy(source, target, load_sem.at[index])
        for index, (source, target) in enumerate(
            (
                (probe, probe_in),
                (measured.at[core], measured_in),
                (dft, dft_in),
                (move, move_in),
            )
        )
    ]
    fetch(obj, meta, cells, flag=flag, loads=loads, **fetching)
    for load in loads:
        load.wait()
    position(win, probe_in, measured_in, dft_in, move_in, lay_cells(grad))
    del win
    give_back(grad, places, tab, out, **giving)


def object_sums(owned, meta, cells, probe_wave, intensities, dft, move):
    vmem = pl.BlockSpec(memory_space=pltpu.VMEM)
    anywhere = pl.BlockSpec(memory_space=pltpu.HBM)
    tile, strip = (8, PW), (TALL, PW)
    dma = pltpu.SemaphoreType.DMA
    many, one = pltpu.VMEM((CHUNKS, ROWS) + strip, F32), pltpu.VMEM((ROWS,) + strip, F32)
    fetching = dict(
        win=pltpu.VMEM((2, 2, 2, W // 2, W), F32),
        tab=pltpu.VMEM((16, 128), I32),
        ag=[pltpu.VMEM((COLUMN,) + strip, F32)] * CHUNKS,
        metas=pltpu.VMEM(tile, I32),
        metain=pltpu.VMEM((NZ,) + tile, I32),
        tables=pltpu.VMEM((2 + PLACES // 8,) + tile, I32),
        pick=pltpu.SMEM((PLACES // 8,) + tile, I32),
        turn=pltpu.SMEM(tile, I32),
        turned=pltpu.SMEM(tile, I32),
        slot=pltpu.SMEM(tile, I32),
        places=pltpu.SMEM((16, 128), I32),
        x_pack=many,
        x_recv=[one] * CHUNKS,
        y_pack=many,
        y_recv=[one] * CHUNKS,
        mark=pltpu.VMEM((3,) + tile, I32),
        marks_x=pltpu.VMEM((NX,) + tile, I32),
        marks_y=pltpu.VMEM((NY,) + tile, I32),
        marks_z=pltpu.VMEM((NZ,) + tile, I32),
        other=pltpu.VMEM((2, 2, W // 2, W), F32),
        ag_send=dma((CHUNKS, 2, 4)),
        ag_recv=dma((CHUNKS, 2, 4)),
        meta_send=dma((NZ,)),
        meta_recv=dma((NZ,)),
        mark_send=dma((3, NZ)),
        mark_recv=dma((3, NZ)),
        x_send=dma((CHUNKS, NX)),
        x_sem=dma((CHUNKS, NX)),
        y_send=dma((CHUNKS, NY)),
        y_sem=dma((CHUNKS, NY)),
        pair_send=dma((4,)),
        pair_recv=dma((4,)),
        local_sem=dma((3 + PLACES // 8,)),
    )
    giving = dict(
        cells=[pltpu.VMEM((MB * CELLS,) + strip, F32)] * CHUNKS,
        y_pack=many,
        y_recv=[one] * CHUNKS,
        x_pack=pltpu.VMEM((CHUNKS, ROWS * TALL, PW), F32),
        x_recv=pltpu.VMEM((CHUNKS, ROWS * TALL, PW), F32),
        total=pltpu.VMEM((CHUNKS, COLUMN * TALL, PW), F32),
        ring=pltpu.VMEM((CHUNKS, 2, 4, OWN * TALL, PW), F32),
        mix=pltpu.VMEM((COLUMN, ROWS), BF16),
        pair_send=dma((CHUNKS,)),
        pair_recv=dma((CHUNKS,)),
        y_send=dma((CHUNKS, NY)),
        y_sem=dma((CHUNKS, NY)),
        x_send=dma((CHUNKS, NX)),
        x_sem=dma((CHUNKS, NX)),
        rs_send=dma((CHUNKS, 2, 4)),
        rs_recv=dma((CHUNKS, 2, 4)),
    )
    rest = [
        pltpu.VMEM((2, CELLS, CHUNKS) + strip, F32),
        pltpu.VMEM((2, W, W), F32),
        pltpu.VMEM((W, W), F32),
        pltpu.VMEM((2 * W, 2 * W), BF16),
        pltpu.VMEM((2 * W, 2 * W), BF16),
        dma((4,)),
    ]
    return pl.pallas_call(
        whole_kernel,
        out_shape=(
            jax.ShapeDtypeStruct((OWN * CHUNKS * TALL, PW), F32),
            jax.ShapeDtypeStruct((1, 1), I32),
        ),
        in_specs=[vmem] * 3 + [anywhere] * 4,
        out_specs=(vmem, pl.BlockSpec(memory_space=pltpu.SMEM)),
        scratch_shapes=[fetching, giving, rest],
        compiler_params=pltpu.CompilerParams(
            collective_id=0, has_side_effects=True, vmem_limit_bytes=46 << 20
        ),
        name="object_sums",
    )(owned, meta, cells, probe_wave, intensities, dft, move)


def swapped(block):
    return lax.ppermute(block, "section", [(0, 1), (1, 0)])


def place_in_all(cell_slot):
    batch = iota(cell_slot.shape, 0)
    return ((cell_slot >> 1) * (2 * MB) + batch * 2 + (cell_slot & 1)).reshape(-1)


def full_windows(owned, send_plan, cell_slot):
    core = lax.axis_index("section")
    outbound = jnp.swapaxes(send_plan, 0, 1)
    patches = owned[jnp.maximum(outbound, 0)]
    arrived = lax.all_to_all(patches, "tile", split_axis=0, concat_axis=0, tiled=True)
    picked = arrived.reshape((-1, 2, PR, PW))[place_in_all(cell_slot)]
    picked = picked.reshape(MB, W // PR, W // PW, 2, PR, PW)
    windows = jnp.transpose(picked, (0, 3, 1, 4, 2, 5)).reshape(MB, 2, W, W)
    passed = swapped(lax.dynamic_index_in_dim(windows, 1 - core, 0, keepdims=False))
    kept = lax.dynamic_index_in_dim(windows, core, 0, keepdims=False)
    first = core == 0
    return jnp.stack([jnp.where(first, kept, passed), jnp.where(first, passed, kept)])


def full_sums(gradients, send_plan, cell_slot):
    core = lax.axis_index("section")
    passed = swapped(lax.dynamic_index_in_dim(gradients, 1 - core, 0, keepdims=False))
    kept = lax.dynamic_index_in_dim(gradients, core, 0, keepdims=False)
    first = core == 0
    batches = jnp.stack([jnp.where(first, kept, passed), jnp.where(first, passed, kept)])
    owners = NX * NY * NZ
    placed = (
        jnp.zeros((owners * MB * 2, 2, PR, PW), F32)
        .at[place_in_all(cell_slot)]
        .set(batches.reshape(-1, 2, PR, PW))
    )
    returned = lax.all_to_all(
        placed.reshape(owners, MB, 2, 2, PR, PW), "tile", split_axis=0, concat_axis=0, tiled=True
    )
    outbound = jnp.swapaxes(send_plan, 0, 1)
    target = jnp.where(outbound < 0, OWN, outbound).reshape(-1)
    sums = jax.ops.segment_sum(
        returned.reshape((-1, 2, PR, PW)), target, num_segments=OWN + 1
    )
    return sums[:OWN]


def body(dft, move, object_slices, probe_wave, intensities, send_list, cell_slot):
    owned = object_slices[0]
    send_plan = send_list[0]
    meta = jnp.transpose(send_plan, (0, 2, 1)).reshape(MB * 2, NX * NY * NZ)
    meta = lax.optimization_barrier(meta)
    sums, flag = object_sums(
        owned.reshape(OWN, CHUNKS, TALL, PW),
        meta,
        cell_slot,
        probe_wave,
        intensities,
        dft,
        move,
    )

    def full():
        plan = jnp.transpose(meta.reshape(MB, 2, NX * NY * NZ), (0, 2, 1))
        windows = full_windows(owned, plan, cell_slot)
        gradients = position_gradients(windows, probe_wave, intensities, dft, move)
        return full_sums(gradients.reshape(2, CELLS, 2, PR, PW), plan, cell_slot)

    sums = lax.cond(flag[0, 0] > 0, full, lambda: sums.reshape(OWN, 2, PR, PW))
    return sums[None]


def solution(mesh):
    dft, move = matrix_tables()
    in_specs = (
        P("section", "tile", None, None, None),
        P(),
        P("tile", None, None),
        P("tile", None, None, None),
        P("tile", None),
    )
    out_specs = P("section", "tile", None, None, None)
    step = functools.partial(body, jnp.asarray(dft), jnp.asarray(move))
    return jax.shard_map(step, mesh=mesh, in_specs=in_specs, out_specs=out_specs, check_vma=False)
```

```python
import functools

import jax
import jax.numpy as jnp
import ml_dtypes
import numpy as np
from jax import lax
from jax.experimental import pallas as pl
from jax.experimental.pallas import tpu as pltpu
from jax.sharding import PartitionSpec as P

W = 256
PW = 128
PR = 16
MB = 2
CELLS = 32
NX, NY, NZ = 4, 4, 8
PLANE = NX * NY
OWN = 32
COLUMN = NZ * OWN
PLACES = 32
ROWS = 4 * PLACES
CHUNKS = 8
TALL = 4
PHASE_SCALE = 20.0
MESH = pl.DeviceIdType.MESH
F32 = jnp.float32
I32 = jnp.int32
BF16 = jnp.bfloat16


FETCH = (
    ("s", 0, -1, 1),
    ("s", 0, 1, 1),
    ("s", 1, -1, 1),
    ("s", 1, 1, 1),
    ("s", 2, -1, 1),
    ("s", 2, 1, 1),
    ("s", 3, -1, 1),
    ("s", 3, 1, 1),
    ("s", 4, -1, 1),
    ("s", 4, 1, 1),
    ("s", 0, -1, 2),
    ("s", 0, 1, 2),
    ("s", 1, -1, 2),
    ("s", 1, 1, 2),
    ("s", 2, -1, 2),
    ("s", 2, 1, 2),
    ("s", 3, -1, 2),
    ("s", 3, 1, 2),
    ("s", 4, -1, 2),
    ("s", 4, 1, 2),
    ("s", 0, -1, 3),
    ("s", 0, 1, 3),
    ("s", 1, -1, 3),
    ("s", 1, 1, 3),
    ("s", 2, -1, 3),
    ("s", 2, 1, 3),
    ("s", 3, -1, 3),
    ("s", 3, 1, 3),
    ("s", 4, -1, 3),
    ("s", 4, 1, 3),
    ("s", 0, 1, 4),
    ("s", 5, -1, 1),
    ("s", 1, -1, 4),
    ("s", 5, 1, 1),
    ("s", 2, 1, 4),
    ("s", 6, -1, 1),
    ("s", 3, -1, 4),
    ("s", 6, 1, 1),
    ("s", 4, 1, 4),
    ("s", 7, -1, 1),
    ("s", 5, -1, 2),
    ("x", 0),
    ("s", 7, 1, 1),
    ("x", 1),
    ("s", 5, 1, 2),
    ("s", 6, -1, 2),
    ("x", 2),
    ("x", 3),
    ("s", 6, 1, 2),
    ("s", 7, -1, 2),
    ("x", 4),
    ("y", 0),
    ("s", 5, -1, 3),
    ("s", 7, 1, 2),
    ("s", 6, -1, 3),
    ("s", 5, 1, 3),
    ("y", 1),
    ("s", 6, 1, 3),
    ("s", 7, -1, 3),
    ("s", 5, -1, 4),
    ("s", 7, 1, 3),
    ("y", 2),
    ("s", 6, 1, 4),
    ("s", 7, -1, 4),
    ("y", 3),
    ("t", 0),
    ("x", 5),
    ("y", 4),
    ("x", 6),
    ("x", 7),
    ("t", 1),
    ("y", 5),
    ("y", 6),
    ("y", 7),
    ("t", 2),
    ("t", 3),
)
RETURN = (
    ("x", 0),
    ("x", 1),
    ("x", 2),
    ("a", 0),
    ("x", 3),
    ("a", 1),
    ("x", 4),
    ("p", 0, -1, 2),
    ("p", 0, 1, 2),
    ("a", 2),
    ("x", 5),
    ("p", 1, -1, 2),
    ("p", 1, 1, 2),
    ("a", 3),
    ("p", 0, -1, 3),
    ("p", 0, 1, 3),
    ("x", 6),
    ("a", 4),
    ("p", 2, -1, 2),
    ("p", 2, 1, 2),
    ("p", 1, -1, 3),
    ("p", 1, 1, 3),
    ("x", 7),
    ("a", 5),
    ("p", 3, -1, 2),
    ("p", 3, 1, 2),
    ("p", 0, 1, 4),
    ("p", 4, -1, 2),
    ("p", 4, 1, 2),
    ("a", 6),
    ("p", 2, -1, 3),
    ("p", 2, 1, 3),
    ("p", 1, -1, 4),
    ("a", 7),
    ("p", 5, -1, 2),
    ("p", 5, 1, 2),
    ("p", 3, -1, 3),
    ("p", 3, 1, 3),
    ("p", 4, -1, 3),
    ("f", 0),
    ("p", 6, -1, 2),
    ("p", 4, 1, 3),
    ("p", 6, 1, 2),
    ("f", 1),
    ("p", 2, 1, 4),
    ("p", 7, -1, 2),
    ("p", 7, 1, 2),
    ("p", 5, -1, 3),
    ("p", 5, 1, 3),
    ("p", 3, -1, 4),
    ("p", 4, 1, 4),
    ("p", 6, -1, 3),
    ("p", 6, 1, 3),
    ("p", 7, -1, 3),
    ("f", 2),
    ("p", 5, -1, 4),
    ("p", 7, 1, 3),
    ("f", 3),
    ("f", 4),
    ("p", 7, -1, 4),
    ("p", 6, 1, 4),
    ("f", 5),
    ("f", 7),
    ("f", 6),
)


def stacked_parts(matrix):
    rows = np.concatenate([matrix.real, matrix.imag], axis=0).astype(np.float32)
    high = rows.astype(ml_dtypes.bfloat16)
    low = (rows - high.astype(np.float32)).astype(ml_dtypes.bfloat16)
    return np.concatenate([high, low], axis=1)


def matrix_tables():
    index = np.arange(W)
    product = np.outer(index, index) % W
    dft = np.exp(-2j * np.pi * product / W) / np.sqrt(W)
    frequency = np.where(index < W // 2, index, index - W).astype(np.float64)
    diagonal = np.exp(-1j * PHASE_SCALE * frequency**2 / (W * W))
    move = np.conj(dft) @ (diagonal[:, None] * dft)
    move = (move + move.T) / 2
    return stacked_parts(dft), stacked_parts(move)


def place():
    tile = lax.axis_index("tile")
    core = lax.axis_index("section")
    y = tile // (NZ * NX)
    z = (tile // NX) % NZ
    x = tile % NX
    return core, y, z, x


def device(core, y, z, x):
    return (core, y * (NZ * NX) + z * NX + x)


def iota(shape, axis):
    return lax.broadcasted_iota(I32, shape, axis)


def to_column(row):
    n = row.shape[1]
    wide = jnp.broadcast_to(row, (n, n))
    return jnp.sum(jnp.where(iota((n, n), 0) == iota((n, n), 1), wide, 0.0), axis=1, keepdims=True)


def exclusive(column):
    rows = [jnp.zeros_like(column[0:1])]
    for step in range(column.shape[0] - 1):
        rows.append(rows[-1] + column[step : step + 1])
    return jnp.concatenate(rows, axis=0)


def send_to(src, dst, send_sem, recv_sem, target):
    return pltpu.make_async_remote_copy(
        src_ref=src,
        dst_ref=dst,
        send_sem=send_sem,
        recv_sem=recv_sem,
        device_id=target,
        device_id_type=MESH,
    )


def greet(barrier, targets):
    for target in targets:
        pl.semaphore_signal(barrier, inc=1, device_id=target, device_id_type=MESH)
    pl.semaphore_wait(barrier, len(targets))


def hops(chunk, direction):
    return 4 if (chunk % 2 == 0) == (direction > 0) else 3


def fill_rows(count, move):
    def some(part, carry):
        for k in range(8):
            move(part * 8 + k)
        return carry

    lax.fori_loop(0, count // 8, some, 0)


def fetch(
    obj,
    meta,
    cells,
    win,
    tab,
    flag,
    ag,
    metas,
    metain,
    tables,
    pick,
    turn,
    turned,
    slot,
    places,
    x_pack,
    x_recv,
    y_pack,
    y_recv,
    mark,
    marks_x,
    marks_y,
    marks_z,
    other,
    ag_send,
    ag_recv,
    meta_send,
    meta_recv,
    mark_send,
    mark_recv,
    x_send,
    x_sem,
    y_send,
    y_sem,
    pair_send,
    pair_recv,
    local_sem,
    loads,
    mix,
):
    core, y, z, x = place()
    partner = device(1 - core, y, z, x)

    def ring_device(step):
        return device(core, y, (z + step) % NZ, x)

    def x_device(step):
        return device(core, y, z, (x + step) % NX)

    def y_device(step):
        return device(core, (y + step) % NY, z, x)

    greet(
        pltpu.get_barrier_semaphore(),
        [ring_device(step) for step in range(1, NZ)]
        + [x_device(step) for step in range(1, NX)]
        + [y_device(step) for step in range(1, NY)]
        + [partner],
    )

    def block(chunk, zz):
        return ag[chunk].at[pl.ds(((zz + 2 * NZ) % NZ) * OWN, OWN)]

    def ring_copy(chunk, direction, hop):
        side = 0 if direction > 0 else 1
        held = block(chunk, z - direction * (hop - 1))
        return send_to(
            obj.at[:, chunk] if hop == 1 else held,
            held,
            ag_send.at[chunk, side, hop - 1],
            ag_recv.at[chunk, side, hop - 1],
            ring_device(direction + NZ),
        )

    def ring_arrival(chunk, direction, hop):
        side = 0 if direction > 0 else 1
        held = block(chunk, z - direction * hop)
        send_to(
            held,
            held,
            ag_send.at[chunk, side, hop - 1],
            ag_recv.at[chunk, side, hop - 1],
            ring_device(direction + NZ),
        ).wait_recv()

    def ring_send(chunk, direction, hop):
        if hop > 1:
            ring_arrival(chunk, direction, hop - 1)
        ring_copy(chunk, direction, hop).start()

    first_wait = min(i for i, event in enumerate(FETCH) if event[0] != "s" or event[3] > 1)
    first_x = min(i for i, event in enumerate(FETCH) if event[0] == "x")
    first_y = min(i for i, event in enumerate(FETCH) if event[0] == "y")
    for event in FETCH[:first_wait]:
        ring_send(*event[1:])

    for load in loads:
        load.start()

    row = jnp.concatenate([cells[0:1, :], cells[1:2, :]], axis=1)
    owner = row >> 1
    entry = ((owner >> 2) & 7) * 4 + (iota(row.shape, 1) >> 5) * 2 + (row & 1)
    code_row = ((owner >> 5) * 128 + (owner & 3) * 32 + entry).astype(F32)
    y_row = (owner >> 5).astype(F32)
    code_col = to_column(code_row)
    y_col = to_column(y_row)
    ahead = (y_col == y_row) & (code_col < code_row)
    rank = jnp.sum(jnp.where(ahead, 1.0, 0.0), axis=0, keepdims=True)
    over = jnp.where(jnp.max(rank, axis=1, keepdims=True) >= PLACES, 1, 0)
    at = y_row * PLACES + jnp.minimum(rank, PLACES - 1.0)
    tables[0] = jnp.zeros((8, 128), I32)
    tables[0, 0:1, 0 : MB * CELLS] = at.astype(I32)
    at_col = to_column(jnp.where(rank < PLACES, at, -1.0))
    spread = jnp.broadcast_to(at_col, (MB * CELLS, ROWS)) == iota((MB * CELLS, ROWS), 1).astype(
        F32
    )
    number = iota((MB * CELLS, ROWS), 0).astype(F32)
    back_row = jnp.sum(jnp.where(spread, number, 0.0), axis=0, keepdims=True)

    metas[...] = jnp.concatenate(
        [meta[...], jnp.broadcast_to(over, (1, 128)), jnp.zeros((3, 128), I32)], axis=0
    )
    metain[z] = metas[...]

    def meta_copy(step):
        return send_to(
            metas,
            metain.at[z],
            meta_send.at[step],
            meta_recv.at[step],
            ring_device(step),
        )

    for step in range(1, NZ):
        meta_copy(step).start()

    last = 1 + PLACES // 8

    def table_copy(index, target):
        source = tab if index > last else tables.at[index]
        return pltpu.make_async_copy(source, target, local_sem.at[index])

    table_copy(0, slot).start()

    for chunk in range(CHUNKS):
        ag[chunk][pl.ds(z * OWN, OWN)] = obj[:, chunk]

    half_way = (first_wait + first_x) // 2
    for event in FETCH[first_wait:half_way]:
        ring_send(*event[1:])

    for step in range(1, NZ):
        meta_copy(step).wait()
    wanted = jnp.concatenate([metain[zz][0:4] for zz in range(NZ)], axis=0).astype(F32)
    lanes = iota((4 * NZ, 128), 1)
    valid = (wanted >= 0.0) & (((lanes >> 2) & 7) == z)
    held = jnp.where(valid, 1.0, 0.0)
    big_row, big_lane = iota((128, 128), 0), iota((128, 128), 1)
    one_x = (big_row & 31) == (big_lane & 31)
    column = jnp.where(one_x, 1.0, 0.0)
    above = jnp.where(one_x & ((big_row >> 5) < (big_lane >> 5)), 1.0, 0.0)
    earlier = jnp.where(iota((4 * NZ, 4 * NZ), 1) < iota((4 * NZ, 4 * NZ), 0), 1.0, 0.0)
    count = jnp.sum(held, axis=0, keepdims=True)
    sums = jnp.concatenate([count, jnp.zeros((7, 128), F32)], axis=0)
    start = jnp.dot(sums, above, preferred_element_type=F32)[0:1]
    whole = jnp.dot(sums, column, preferred_element_type=F32)[0:1]
    order = jnp.dot(earlier, held, preferred_element_type=F32) + start
    named = (iota((4 * NZ, 128), 0) >> 2).astype(F32) * OWN + wanted + 1.0
    picks = [
        jnp.sum(jnp.where(valid & (order == float(k)), named, 0.0), axis=0, keepdims=True)
        for k in range(PLACES)
    ]
    picks = jnp.dot(jnp.concatenate(picks, axis=0), column, preferred_element_type=F32)
    for part in range(PLACES // 8):
        tables[1 + part] = picks[part * 8 : part * 8 + 8].astype(I32) - 1
        table_copy(1 + part, pick.at[part]).start()
    over_x = jnp.where(jnp.max(whole, axis=1, keepdims=True) > PLACES, 1.0, 0.0)
    over_z = jnp.max(
        jnp.max(metain[:, 4, :].astype(F32), axis=1, keepdims=True), axis=0, keepdims=True
    )
    over = jnp.broadcast_to(jnp.maximum(over_x, over_z), (1, 128))
    mark[0] = jnp.concatenate([count, start, over, jnp.zeros((5, 128), F32)], axis=0).astype(I32)
    marks_x[x] = mark[0]

    def mark_copy(kind, step):
        targets = (x_device, y_device, ring_device)
        arrays = (marks_x, marks_y, marks_z)
        own = (x, y, z)
        return send_to(
            mark.at[kind],
            arrays[kind].at[own[kind]],
            mark_send.at[kind, step],
            mark_recv.at[kind, step],
            targets[kind](step),
        )

    for step in range(1, NX):
        mark_copy(0, step).start()
    target = iota((128, ROWS), 1)
    chosen = jnp.where(iota((128, ROWS), 0) == (target // PLACES) + z * 4, 1.0, 0.0)
    chosen = jnp.dot(picks, chosen, preferred_element_type=F32)
    here = iota((PLACES, ROWS), 0) == iota((PLACES, ROWS), 1) % PLACES
    sums_row = jnp.sum(jnp.where(here, chosen, 0.0), axis=0, keepdims=True)
    tab[...] = jnp.zeros(tab.shape, I32)
    tab[0:1, :] = back_row.astype(I32)
    tab[1:2, :] = sums_row.astype(I32)

    table_copy(0, slot).wait()
    for part in range(PLACES // 8):
        table_copy(1 + part, pick.at[part]).wait()

    for event in FETCH[half_way:first_x]:
        ring_send(*event[1:])

    def x_copy(chunk, step):
        return send_to(
            x_pack.at[chunk, pl.ds(((x + step) % NX) * PLACES, PLACES)],
            x_recv[chunk].at[pl.ds(x * PLACES, PLACES)],
            x_send.at[chunk, step],
            x_sem.at[chunk, step],
            x_device(step),
        )

    def y_copy(chunk, step):
        return send_to(
            y_pack.at[chunk, pl.ds(((y + step) % NY) * PLACES, PLACES)],
            y_recv[chunk].at[pl.ds(y * PLACES, PLACES)],
            y_send.at[chunk, step],
            y_sem.at[chunk, step],
            y_device(step),
        )

    def along_x(chunk):
        for direction in (1, -1):
            ring_arrival(chunk, direction, hops(chunk, direction))

        def fill(part, carry):
            for k in range(8):
                for to in range(NX):
                    index = pick[part, k, z * 4 + to] & (COLUMN - 1)
                    x_pack[chunk, to * PLACES + part * 8 + k] = ag[chunk][index]
            return carry

        lax.fori_loop(0, PLACES // 8, fill, 0)
        for step in range(1, NX):
            x_copy(chunk, step).start()
        own = pl.ds(x * PLACES, PLACES)
        x_recv[chunk][own] = x_pack[chunk, own]

    def along_y(chunk):
        for step in range(1, NX):
            x_copy(chunk, step).wait_recv()

        def fill(part, carry):
            for k in range(8):
                for to in range(NY):
                    index = turn[to, part * 8 + k] & (ROWS - 1)
                    y_pack[chunk, to * PLACES + part * 8 + k] = x_recv[chunk][index]
            return carry

        lax.fori_loop(0, PLACES // 8, fill, 0)
        for step in range(1, NY):
            y_copy(chunk, step).start()
        own = pl.ds(y * PLACES, PLACES)
        y_recv[chunk][own] = y_pack[chunk, own]

    def pair_copy(quarter):
        return send_to(
            other.at[quarter // 2, quarter % 2],
            win.at[core, quarter // 2, quarter % 2],
            pair_send.at[quarter],
            pair_recv.at[quarter],
            partner,
        )

    def take(quarter):
        low, high = 2 * quarter, 2 * quarter + 1
        for chunk in (low, high):
            for step in range(1, NY):
                y_copy(chunk, step).wait_recv()
        part, half = quarter // 2, quarter % 2

        def both(index):
            index = index & (ROWS - 1)
            return jnp.concatenate([y_recv[low][index], y_recv[high][index]], axis=0)

        def lay(r, carry):
            first = pl.multiple_of(r * 8, 8)
            for side in range(2):
                k = r * 2 + side
                lanes_of = slice(side * PW, side * PW + PW)
                win[core, part, half, pl.ds(first, 8), lanes_of] = both(slot[0, core * CELLS + k])
                other[part, half, pl.ds(first, 8), lanes_of] = both(slot[0, (1 - core) * CELLS + k])
            return carry

        lax.fori_loop(0, W // PR, lay, 0)

    def run(events):
        for event in events:
            if event[0] == "s":
                ring_send(*event[1:])
            elif event[0] == "x":
                along_x(event[1])
            elif event[0] == "y":
                along_y(event[1])
            else:
                take(event[1])
                pair_copy(event[1]).start()

    run(FETCH[first_x:first_y])

    for step in range(1, NX):
        mark_copy(0, step).wait()
    counts = marks_x[:, 0, :].astype(F32)
    starts = marks_x[:, 1, :].astype(F32)
    four = iota((NX, 128), 1)
    wide = four.astype(F32)
    giver = iota((NX, 128), 0).astype(F32)
    onward = []
    back = jnp.zeros((NX, 128), F32)
    for to in range(NY):
        mine = four == to * 32 + z * 4 + x
        many = jnp.sum(jnp.where(mine, counts, 0.0), axis=1, keepdims=True)
        low = jnp.sum(jnp.where(mine, starts, 0.0), axis=1, keepdims=True)
        first = exclusive(many)
        inside = (wide >= first) & (wide < first + many)
        onward.append(
            jnp.sum(
                jnp.where(inside, giver * PLACES + low + wide - first, 0.0),
                axis=0,
                keepdims=True,
            )
        )
        inside = (wide >= low) & (wide < low + many)
        back = back + jnp.where(inside, to * PLACES + first + wide - low, 0.0)
    tables[last] = jnp.concatenate(onward + [jnp.zeros((4, 128), F32)], axis=0).astype(I32)
    table_copy(last, turn).start()
    tab[8:12, :] = back.astype(I32)
    table_copy(last + 1, places).start()
    mark[1] = jnp.broadcast_to(
        jnp.max(marks_x[:, 2, :].astype(F32), axis=0, keepdims=True), (8, 128)
    ).astype(I32)
    marks_y[y] = mark[1]
    for step in range(1, NY):
        mark_copy(1, step).start()
    table_copy(last, turn).wait()
    table_copy(last + 1, places).wait()

    next_y = [i for i, event in enumerate(FETCH) if event[0] == "y"]
    run(FETCH[first_y : next_y[2]])
    for step in range(1, NY):
        mark_copy(1, step).wait()
    mark[2] = jnp.max(marks_y[...].astype(F32), axis=0).astype(I32)
    marks_z[z] = mark[2]
    for step in range(1, NZ):
        mark_copy(2, step).start()
    run(FETCH[next_y[2] : next_y[5]])
    for step in range(1, NZ):
        mark_copy(2, step).wait()
    mark[0] = jnp.max(marks_z[...].astype(F32), axis=0).astype(I32)
    crowded = pltpu.make_async_copy(mark.at[0], turned, local_sem.at[0])
    crowded.start()
    run(FETCH[next_y[5] :])
    for chunk in range(CHUNKS):
        for direction in (1, -1):
            for hop in range(1, hops(chunk, direction) + 1):
                ring_copy(chunk, direction, hop).wait_send()
        for step in range(1, NX):
            x_copy(chunk, step).wait_send()
            y_copy(chunk, step).wait_send()
    mix[...] = jnp.where(
        jnp.broadcast_to(tab[1:2, :], (COLUMN, ROWS)) == iota((COLUMN, ROWS), 0) + 1, 1.0, 0.0
    ).astype(BF16)
    crowded.wait()
    flag[0, 0] = turned[0, 0]
    for quarter in range(4):
        pair_copy(quarter).wait()


def parts(value):
    high = value.astype(BF16)
    return high, (value - high.astype(F32)).astype(BF16)


def from_left(real, imag, table, sign):
    high, low = parts(jnp.concatenate([real, imag], axis=1))
    out = jnp.dot(
        table[...], jnp.concatenate([high, high], axis=0), preferred_element_type=F32
    ) + jnp.dot(table[:, :W], low, preferred_element_type=F32)
    return out[:W, :W] - sign * out[W:, W:], out[:W, W:] + sign * out[W:, :W]


def from_right(real, imag, table, sign):
    high, low = parts(jnp.concatenate([real, imag], axis=0))
    across = (((1,), (1,)), ((), ()))
    out = lax.dot_general(
        jnp.concatenate([high, high], axis=1), table[...], across, preferred_element_type=F32
    ) + lax.dot_general(low, table[:, :W], across, preferred_element_type=F32)
    return out[:W, :W] - sign * out[W:, W:], sign * out[:W, W:] + out[W:, :W]


def both_sides(real, imag, table, sign):
    real, imag = from_left(real, imag, table, sign)
    return from_right(real, imag, table, sign)


def window(win, index):
    if len(win.shape) == 4:
        return win[index, 0], win[index, 1]
    return tuple(
        jnp.concatenate(
            [
                win[index, part, half, r * 8 : r * 8 + 8]
                for r in range(W // PR)
                for half in range(2)
            ],
            axis=0,
        )
        for part in range(2)
    )


def position(win, probe, measured, dft, move, lay):
    pr, pi = probe[0], probe[1]
    ar, ai = window(win, 0)
    wave_r, wave_i = both_sides(pr * ar - pi * ai, pr * ai + pi * ar, move, 1.0)
    br, bi = window(win, 1)
    far_r, far_i = both_sides(
        wave_r * br - wave_i * bi, wave_r * bi + wave_i * br, dft, 1.0
    )
    gap = far_r * far_r + far_i * far_i - measured[...]
    back_r, back_i = both_sides(gap * far_r, gap * far_i, dft, -1.0)
    lay(1, wave_r * back_r + wave_i * back_i, wave_r * back_i - wave_i * back_r)
    br, bi = window(win, 1)
    low_r, low_i = both_sides(
        br * back_r + bi * back_i, br * back_i - bi * back_r, move, -1.0
    )
    pr, pi = probe[0], probe[1]
    lay(0, pr * low_r + pi * low_i, pr * low_i - pi * low_r)


def lay_cells(grad):
    def lay(index, real, imag):
        for k in range(CELLS):
            rows = slice(k // 2 * PR, k // 2 * PR + PR)
            lanes = slice(k % 2 * PW, k % 2 * PW + PW)
            for part, value in enumerate((real, imag)):
                value = value[rows, lanes]
                for strip in range(4):
                    grad[index, k, part * 4 + strip] = value[strip * TALL : strip * TALL + TALL]

    return lay


def position_kernel(win, probe, measured, dft, move, grad):
    core = lax.axis_index("section")
    position(win, probe, measured.at[core], dft, move, lay_cells(grad))


def position_gradients(windows, probe_wave, intensities, dft, move):
    vmem = pl.BlockSpec(memory_space=pltpu.VMEM)
    return pl.pallas_call(
        position_kernel,
        out_shape=jax.ShapeDtypeStruct((2, CELLS, CHUNKS, TALL, PW), F32),
        in_specs=[vmem] * 5,
        out_specs=vmem,
        name="position_gradients",
    )(windows, probe_wave, intensities, dft, move)


def give_back(
    grad,
    places,
    tab,
    out,
    cells,
    y_pack,
    y_recv,
    x_pack,
    x_recv,
    total,
    ring,
    mix,
    pair_send,
    pair_recv,
    y_send,
    y_sem,
    x_send,
    x_sem,
    rs_send,
    rs_recv,
):
    core, y, z, x = place()
    partner = device(1 - core, y, z, x)

    def ring_device(step):
        return device(core, y, (z + step) % NZ, x)

    def x_device(step):
        return device(core, y, z, (x + step) % NX)

    def y_device(step):
        return device(core, (y + step) % NY, z, x)

    def pair_copy(chunk):
        return send_to(
            grad.at[1 - core, :, chunk],
            cells[chunk].at[pl.ds(core * CELLS, CELLS)],
            pair_send.at[chunk],
            pair_recv.at[chunk],
            partner,
        )

    for chunk in range(CHUNKS):
        cells[chunk][pl.ds(core * CELLS, CELLS)] = grad[core, :, chunk]
        pair_copy(chunk).start()

    def y_copy(chunk, step):
        return send_to(
            y_pack.at[chunk, pl.ds(((y + step) % NY) * PLACES, PLACES)],
            y_recv[chunk].at[pl.ds(y * PLACES, PLACES)],
            y_send.at[chunk, step],
            y_sem.at[chunk, step],
            y_device(step),
        )

    def x_copy(chunk, step):
        return send_to(
            x_pack.at[chunk, pl.ds(((x + step) % NX) * (PLACES * TALL), PLACES * TALL)],
            x_recv.at[chunk, pl.ds(x * (PLACES * TALL), PLACES * TALL)],
            x_send.at[chunk, step],
            x_sem.at[chunk, step],
            x_device(step),
        )

    for chunk in range(CHUNKS):
        pair_copy(chunk).wait_recv()

        def fill_y(row):
            index = places[0, row] & (MB * CELLS - 1)
            y_pack[chunk, row] = cells[chunk][index]

        fill_rows(ROWS, fill_y)
        for step in range(1, NY):
            y_copy(chunk, step).start()
        own = pl.ds(y * PLACES, PLACES)
        y_recv[chunk][own] = y_pack[chunk, own]

    def along_x(chunk):
        for step in range(1, NY):
            y_copy(chunk, step).wait_recv()

        def fill_x(pair):
            to, k = pair // (PLACES // 2), pair % (PLACES // 2) * 2
            two = [places[8 + to, k + i] & (ROWS - 1) for i in range(2)]
            spot = pl.ds(pl.multiple_of(pair * 2 * TALL, 8), 2 * TALL)
            x_pack[chunk, spot] = jnp.concatenate([y_recv[chunk][i] for i in two], axis=0)

        fill_rows(ROWS // 2, fill_x)
        for step in range(1, NX):
            x_copy(chunk, step).start()
        own = pl.ds(x * (PLACES * TALL), PLACES * TALL)
        x_recv[chunk, own] = x_pack[chunk, own]

    def block(zz):
        return pl.ds(((zz + 2 * NZ) % NZ) * (OWN * TALL), OWN * TALL)

    def ring_copy(chunk, direction, step):
        side = 0 if direction > 0 else 1
        reach = hops(chunk, direction)
        return send_to(
            total.at[chunk, block(z + direction * reach)]
            if step == 1
            else ring.at[chunk, side, step - 2],
            ring.at[chunk, side, step - 1],
            rs_send.at[chunk, side, step - 1],
            rs_recv.at[chunk, side, step - 1],
            ring_device(direction + NZ),
        )

    def sum_cells(chunk):
        for step in range(1, NX):
            x_copy(chunk, step).wait_recv()

        def add(r, carry):
            high, low = parts(x_recv[chunk, pl.ds(r, ROWS, stride=TALL), :])
            both = jnp.dot(
                mix[...], jnp.concatenate([high, low], axis=1), preferred_element_type=F32
            )
            total[chunk, pl.ds(r, COLUMN, stride=TALL), :] = both[:, :128] + both[:, 128:]
            return carry

        lax.fori_loop(0, TALL, add, 0)
        for direction in (1, -1):
            ring_copy(chunk, direction, 1).start()

    def pass_on(chunk, direction, step):
        reach = hops(chunk, direction)
        side = 0 if direction > 0 else 1
        ring_copy(chunk, direction, step - 1).wait_recv()
        ring[chunk, side, step - 2] += total[chunk, block(z + direction * (reach - step + 1))]
        ring_copy(chunk, direction, step).start()

    def last(chunk):
        value = total[chunk, block(z)]
        for direction in (1, -1):
            reach = hops(chunk, direction)
            side = 0 if direction > 0 else 1
            ring_copy(chunk, direction, reach).wait_recv()
            value = value + ring[chunk, side, reach - 1]
        return value

    def finish(quarter):
        low, high = last(2 * quarter), last(2 * quarter + 1)
        for p in range(OWN):
            rows = slice(p * TALL, p * TALL + TALL)
            spot = p * CHUNKS * TALL + quarter * 8
            out[spot : spot + 8] = jnp.concatenate([low[rows], high[rows]], axis=0)

    ended = set()
    for event in RETURN:
        if event[0] == "x":
            along_x(event[1])
        elif event[0] == "a":
            sum_cells(event[1])
        elif event[0] == "p":
            pass_on(*event[1:])
        else:
            ended.add(event[1])
            if event[1] ^ 1 in ended:
                finish(event[1] // 2)

    for chunk in range(CHUNKS):
        pair_copy(chunk).wait_send()
        for direction in (1, -1):
            for step in range(1, hops(chunk, direction) + 1):
                ring_copy(chunk, direction, step).wait_send()
        for step in range(1, NX):
            x_copy(chunk, step).wait_send()
            y_copy(chunk, step).wait_send()


def whole_kernel(obj, meta, cells, probe, measured, dft, move, out, flag, *scratch):
    fetching, giving, (grad, probe_in, measured_in, dft_in, move_in, load_sem) = scratch
    win, tab, places = fetching["win"], fetching["tab"], fetching["places"]
    core = lax.axis_index("section")
    loads = [
        pltpu.make_async_copy(source, target, load_sem.at[index])
        for index, (source, target) in enumerate(
            (
                (probe, probe_in),
                (measured.at[core], measured_in),
                (dft, dft_in),
                (move, move_in),
            )
        )
    ]
    fetch(obj, meta, cells, flag=flag, loads=loads, mix=giving["mix"], **fetching)
    for load in loads:
        load.wait()
    position(win, probe_in, measured_in, dft_in, move_in, lay_cells(grad))
    del win
    give_back(grad, places, tab, out, **giving)


def object_sums(owned, meta, cells, probe_wave, intensities, dft, move):
    vmem = pl.BlockSpec(memory_space=pltpu.VMEM)
    anywhere = pl.BlockSpec(memory_space=pltpu.HBM)
    tile, strip = (8, PW), (TALL, PW)
    dma = pltpu.SemaphoreType.DMA
    many, one = pltpu.VMEM((CHUNKS, ROWS) + strip, F32), pltpu.VMEM((ROWS,) + strip, F32)
    fetching = dict(
        win=pltpu.VMEM((2, 2, 2, W // 2, W), F32),
        tab=pltpu.VMEM((16, 128), I32),
        ag=[pltpu.VMEM((COLUMN,) + strip, F32)] * CHUNKS,
        metas=pltpu.VMEM(tile, I32),
        metain=pltpu.VMEM((NZ,) + tile, I32),
        tables=pltpu.VMEM((2 + PLACES // 8,) + tile, I32),
        pick=pltpu.SMEM((PLACES // 8,) + tile, I32),
        turn=pltpu.SMEM(tile, I32),
        turned=pltpu.SMEM(tile, I32),
        slot=pltpu.SMEM(tile, I32),
        places=pltpu.SMEM((16, 128), I32),
        x_pack=many,
        x_recv=[one] * CHUNKS,
        y_pack=many,
        y_recv=[one] * CHUNKS,
        mark=pltpu.VMEM((3,) + tile, I32),
        marks_x=pltpu.VMEM((NX,) + tile, I32),
        marks_y=pltpu.VMEM((NY,) + tile, I32),
        marks_z=pltpu.VMEM((NZ,) + tile, I32),
        other=pltpu.VMEM((2, 2, W // 2, W), F32),
        ag_send=dma((CHUNKS, 2, 4)),
        ag_recv=dma((CHUNKS, 2, 4)),
        meta_send=dma((NZ,)),
        meta_recv=dma((NZ,)),
        mark_send=dma((3, NZ)),
        mark_recv=dma((3, NZ)),
        x_send=dma((CHUNKS, NX)),
        x_sem=dma((CHUNKS, NX)),
        y_send=dma((CHUNKS, NY)),
        y_sem=dma((CHUNKS, NY)),
        pair_send=dma((4,)),
        pair_recv=dma((4,)),
        local_sem=dma((3 + PLACES // 8,)),
    )
    giving = dict(
        cells=[pltpu.VMEM((MB * CELLS,) + strip, F32)] * CHUNKS,
        y_pack=many,
        y_recv=[one] * CHUNKS,
        x_pack=pltpu.VMEM((CHUNKS, ROWS * TALL, PW), F32),
        x_recv=pltpu.VMEM((CHUNKS, ROWS * TALL, PW), F32),
        total=pltpu.VMEM((CHUNKS, COLUMN * TALL, PW), F32),
        ring=pltpu.VMEM((CHUNKS, 2, 4, OWN * TALL, PW), F32),
        mix=pltpu.VMEM((COLUMN, ROWS), BF16),
        pair_send=dma((CHUNKS,)),
        pair_recv=dma((CHUNKS,)),
        y_send=dma((CHUNKS, NY)),
        y_sem=dma((CHUNKS, NY)),
        x_send=dma((CHUNKS, NX)),
        x_sem=dma((CHUNKS, NX)),
        rs_send=dma((CHUNKS, 2, 4)),
        rs_recv=dma((CHUNKS, 2, 4)),
    )
    rest = [
        pltpu.VMEM((2, CELLS, CHUNKS) + strip, F32),
        pltpu.VMEM((2, W, W), F32),
        pltpu.VMEM((W, W), F32),
        pltpu.VMEM((2 * W, 2 * W), BF16),
        pltpu.VMEM((2 * W, 2 * W), BF16),
        dma((4,)),
    ]
    return pl.pallas_call(
        whole_kernel,
        out_shape=(
            jax.ShapeDtypeStruct((OWN * CHUNKS * TALL, PW), F32),
            jax.ShapeDtypeStruct((1, 1), I32),
        ),
        in_specs=[vmem] * 3 + [anywhere] * 4,
        out_specs=(vmem, pl.BlockSpec(memory_space=pltpu.SMEM)),
        scratch_shapes=[fetching, giving, rest],
        compiler_params=pltpu.CompilerParams(
            collective_id=0, has_side_effects=True, vmem_limit_bytes=46 << 20
        ),
        name="object_sums",
    )(owned, meta, cells, probe_wave, intensities, dft, move)


def swapped(block):
    return lax.ppermute(block, "section", [(0, 1), (1, 0)])


def place_in_all(cell_slot):
    batch = iota(cell_slot.shape, 0)
    return ((cell_slot >> 1) * (2 * MB) + batch * 2 + (cell_slot & 1)).reshape(-1)


def full_windows(owned, send_plan, cell_slot):
    core = lax.axis_index("section")
    outbound = jnp.swapaxes(send_plan, 0, 1)
    patches = owned[jnp.maximum(outbound, 0)]
    arrived = lax.all_to_all(patches, "tile", split_axis=0, concat_axis=0, tiled=True)
    picked = arrived.reshape((-1, 2, PR, PW))[place_in_all(cell_slot)]
    picked = picked.reshape(MB, W // PR, W // PW, 2, PR, PW)
    windows = jnp.transpose(picked, (0, 3, 1, 4, 2, 5)).reshape(MB, 2, W, W)
    passed = swapped(lax.dynamic_index_in_dim(windows, 1 - core, 0, keepdims=False))
    kept = lax.dynamic_index_in_dim(windows, core, 0, keepdims=False)
    first = core == 0
    return jnp.stack([jnp.where(first, kept, passed), jnp.where(first, passed, kept)])


def full_sums(gradients, send_plan, cell_slot):
    core = lax.axis_index("section")
    passed = swapped(lax.dynamic_index_in_dim(gradients, 1 - core, 0, keepdims=False))
    kept = lax.dynamic_index_in_dim(gradients, core, 0, keepdims=False)
    first = core == 0
    batches = jnp.stack([jnp.where(first, kept, passed), jnp.where(first, passed, kept)])
    owners = NX * NY * NZ
    placed = (
        jnp.zeros((owners * MB * 2, 2, PR, PW), F32)
        .at[place_in_all(cell_slot)]
        .set(batches.reshape(-1, 2, PR, PW))
    )
    returned = lax.all_to_all(
        placed.reshape(owners, MB, 2, 2, PR, PW), "tile", split_axis=0, concat_axis=0, tiled=True
    )
    outbound = jnp.swapaxes(send_plan, 0, 1)
    target = jnp.where(outbound < 0, OWN, outbound).reshape(-1)
    sums = jax.ops.segment_sum(
        returned.reshape((-1, 2, PR, PW)), target, num_segments=OWN + 1
    )
    return sums[:OWN]


def body(dft, move, object_slices, probe_wave, intensities, send_list, cell_slot):
    owned = object_slices[0]
    send_plan = send_list[0]
    meta = jnp.transpose(send_plan, (0, 2, 1)).reshape(MB * 2, NX * NY * NZ)
    meta = lax.optimization_barrier(meta)
    sums, flag = object_sums(
        owned.reshape(OWN, CHUNKS, TALL, PW),
        meta,
        cell_slot,
        probe_wave,
        intensities,
        dft,
        move,
    )

    def full():
        plan = jnp.transpose(meta.reshape(MB, 2, NX * NY * NZ), (0, 2, 1))
        windows = full_windows(owned, plan, cell_slot)
        gradients = position_gradients(windows, probe_wave, intensities, dft, move)
        return full_sums(gradients.reshape(2, CELLS, 2, PR, PW), plan, cell_slot)

    sums = lax.cond(flag[0, 0] > 0, full, lambda: sums.reshape(OWN, 2, PR, PW))
    return sums[None]


def solution(mesh):
    dft, move = matrix_tables()
    in_specs = (
        P("section", "tile", None, None, None),
        P(),
        P("tile", None, None),
        P("tile", None, None, None),
        P("tile", None),
    )
    out_specs = P("section", "tile", None, None, None)
    step = functools.partial(body, jnp.asarray(dft), jnp.asarray(move))
    return jax.shard_map(step, mesh=mesh, in_specs=in_specs, out_specs=out_specs, check_vma=False)
```
